128 devices in a mesh: prow: 4 (over y_hi, core), pcol: 32 (over x, y_lo, z).
Axes of the slice: x: 4, y: 4 (y_hi: 2, y_lo: 2; y = y_hi * 2 + y_lo), z: 4, core: 2. Of those that a mesh axis runs over, the one named last changes fastest.
Arguments:
- vectors: bfloat16 [2048, 120064], P('pcol', 'prow'), may hold values from -6 to 6
- reflectors: bfloat16 [2, 256, 120064], P(None, 'pcol', 'prow'), may hold values from -6 to 6
- panel_factor: float32 [2, 256, 256], replicated, as said below
Outputs:
- band_vectors: bfloat16 [32, 64, 120064], P('pcol', 'prow')
The draws below stay inside these ranges and needn't reach their ends.
Inputs may be any that keep to these rules, and one draw needn't show every extreme that they name: `panel_factor`: upper triangular: zero below the diagonal; diagonal entries between 1 / 120064 and 3 / 120064.
All inputs are finite; a program needn't handle non-finite values.
Results may differ from the reference program's by a relative error of at most 0.0095.
Values may be sent and summed in bfloat16 or wider, within the bound.
A program may use at most 192 MiB of HBM per device.

```python
import jax
import jax.numpy as jnp
from jax import lax

ORDER = 120064
PANEL = 256
PANELS = 2
COLS_DEV = 64
NEV = 2048
N_PCOL = 32


def draw_panel_factor(key, part):
    first_key, second_key = jax.random.split(jax.random.fold_in(key, 7))
    shape = (PANELS, PANEL, PANEL)
    upper_part = jax.random.normal(first_key, shape, jnp.float32) * (0.6 / ORDER)
    diag_part = jax.random.uniform(second_key, (PANELS, PANEL), jnp.float32, 1.0, 3.0) / ORDER
    row_ids = lax.broadcasted_iota(jnp.int32, shape, 1)
    col_ids = lax.broadcasted_iota(jnp.int32, shape, 2)
    result = jnp.where(col_ids > row_ids, upper_part, 0.0)
    result = result + jnp.where(col_ids == row_ids, diag_part[:, :, None], 0.0)
    return result.astype(jnp.float32)


def shard_levels(own_key, dims, pieces, low, top_value):
    factor_of = 1.0
    for position, blocks in pieces:
        steps = jax.random.uniform(jax.random.fold_in(jax.random.fold_in(own_key, 6), position), (blocks,), jnp.float32, low / len(pieces), top_value / len(pieces))
        factor_of = factor_of * jnp.repeat(jnp.exp(steps), dims[position] // blocks).reshape((-1,) + (1,) * (len(dims) - 1 - position))
    return factor_of


def scatter_about(rng, shape, deviation, most, cuts=(), dtype=jnp.bfloat16):
    entries = deviation * jax.random.normal(rng, shape, jnp.float32)
    if cuts:
        entries = entries * shard_levels(rng, shape, cuts, -0.22, 0.18)
    return jnp.clip(entries, -most, most).astype(dtype)


def setup_inputs(seed: int = 0) -> dict:
    streams_of = jax.random.split(jax.random.key(seed), 4)
    vectors = scatter_about(streams_of[0], (NEV, ORDER), 1.0, 6.0, ((0, 32), (1, 4)))
    reflectors = scatter_about(streams_of[1], (PANELS, PANEL, ORDER), 1.0, 6.0, ((1, 32), (2, 4)))
    panel_factor = draw_panel_factor(jax.random.fold_in(streams_of[3], 71), 0)
    return dict(vectors=vectors, reflectors=reflectors, panel_factor=panel_factor)


def apply_panel(current, panel, factor):
    projected = lax.dot_general(current, panel, (((1,), (1,)), ((), ())), preferred_element_type=jnp.float32)
    scaled = lax.dot_general(projected, factor, (((1,), (1,)), ((), ())), precision=lax.Precision.HIGHEST, preferred_element_type=jnp.float32).astype(jnp.bfloat16)
    updated = current.astype(jnp.float32) - jnp.dot(scaled, panel, preferred_element_type=jnp.float32)
    return updated.astype(jnp.bfloat16)


def reference(vectors, reflectors, panel_factor):
    current = vectors
    for number in range(PANELS):
        current = apply_panel(current, reflectors[number], panel_factor[number])
    return current.reshape(N_PCOL, COLS_DEV, ORDER)
```

```python
import functools

import jax
import jax.numpy as jnp
from jax import lax
from jax.experimental import pallas as pl
from jax.experimental.pallas import tpu as pltpu
from jax.sharding import PartitionSpec as P

X, YL, Z, R = 4, 2, 4, 4
Q = YL * Z
GROUP = Q * R
BF16, F32 = jnp.bfloat16, jnp.float32


def kernel(
    dims,
    v_hbm, r_hbm, v_tail, r_tail, factor,
    out,
    v_loc, r_loc, v_all, r_all, p_send, p_recv, g_send, g_recv, g_own, g_all, s_own, s_all,
    ld_sem, own_sem, r_ssem, r_rsem, x_ssem, v_ssem, v_rsem,
    gs_ssem, gs_rsem, ga_ssem, ga_rsem, ps_ssem, ps_rsem, sa_ssem, sa_rsem, o_ssem, o_rsem, o_own,
):
    rows, panel, whole, valid, chunk, step = dims
    per = rows // R
    share = panel // (X * Q)
    prow, pcol = lax.axis_index("prow"), lax.axis_index("pcol")
    x, yl, z = pcol // Q, lax.rem(pcol // Z, YL), lax.rem(pcol, Z)
    h, k = prow // 2, lax.rem(prow, 2)

    def place(dx, dy, dz, dr):
        far = lax.rem(x + dx, X) * Q + lax.rem(yl + dy, YL) * Z + lax.rem(z + dz, Z)
        across = lax.rem(h + dr // 2, 2) * 2 + lax.rem(k + dr % 2, 2)
        return across, far

    def place_of(d):
        dy, dz, dr = d // 16, lax.rem(d // 4, 4), lax.rem(d, 4)
        far = x * Q + lax.rem(yl + dy, YL) * Z + lax.rem(z + dz, Z)
        across = lax.rem(h + dr // 2, 2) * 2 + lax.rem(k + lax.rem(dr, 2), 2)
        return across, far

    def mirror(d):
        dy, dz, dr = d // 16, lax.rem(d // 4, 4), lax.rem(d, 4)
        return dy * 16 + lax.rem(4 - dz, 4) * 4 + dr

    def send(src, dst, ssem, rsem, to):
        return pltpu.make_async_remote_copy(
            src_ref=src, dst_ref=dst, send_sem=ssem, recv_sem=rsem,
            device_id=to, device_id_type=pl.DeviceIdType.MESH,
        )

    def arrived(ref, sem):
        pltpu.make_async_copy(ref, ref, sem).wait()

    load_r = pltpu.make_async_copy(r_hbm.at[:, :, pl.ds(0, whole)], r_loc.at[:, :, pl.ds(0, whole)], ld_sem.at[0])
    load_v = pltpu.make_async_copy(v_hbm.at[:, pl.ds(0, whole)], v_loc.at[:, pl.ds(0, whole)], ld_sem.at[1])
    load_r.start()
    load_v.start()

    barrier = pltpu.get_barrier_semaphore()

    @pl.loop(1, GROUP)
    def _(d):
        pl.semaphore_signal(barrier, inc=1, device_id=place_of(d), device_id_type=pl.DeviceIdType.MESH)

    for dx in range(1, X):
        pl.semaphore_signal(barrier, inc=1, device_id=place(dx, 0, 0, 0), device_id_type=pl.DeviceIdType.MESH)

    edge = v_loc.shape[1] - whole
    lane = lax.broadcasted_iota(jnp.int32, (rows, 128), 1)
    v_loc[:, whole:] = jnp.zeros((rows, edge), BF16)
    v_loc[:, whole:whole + 128] = jnp.where(lane < valid, v_tail[...].astype(F32), 0.0).astype(BF16)
    lane8 = lax.broadcasted_iota(jnp.int32, (share, 128), 1)
    for p in range(2):
        r_loc[p, :, whole:] = jnp.zeros((share, edge), BF16)
        r_loc[p, :, whole:whole + 128] = jnp.where(lane8 < valid, r_tail[p].astype(F32), 0.0).astype(BF16)

    pl.semaphore_wait(barrier, GROUP - 1 + X - 1)

    offsets = [(dy, dz) for dz in (1, 3, 2, 0) for dy in (0, 1) if (dy, dz) != (0, 0)]
    mine = pl.ds(pl.multiple_of(pcol * share, share), share)

    def columns(dy, dz):
        q = lax.rem(yl + dy, YL) * Z + lax.rem(z + dz, Z)
        return pl.ds(pl.multiple_of(q * chunk, 128), chunk)

    load_r.wait()
    r_out = []
    for dy, dz in offsets:
        back = dy * 4 + (4 - dz) % 4
        copy = send(r_loc.at[:, :, columns(dy, dz)], r_all.at[:, mine, :], r_ssem.at[dy * 4 + dz],
                    r_rsem.at[back], place(0, dy, dz, 0))
        copy.start()
        r_out.append(copy)
    own_r = pltpu.make_async_copy(r_loc.at[:, :, columns(0, 0)], r_all.at[:, mine, :], own_sem.at[0])
    own_r.start()
    load_v.wait()
    v_out = []
    for dy, dz in offsets:
        back = dy * 4 + (4 - dz) % 4
        copy = send(v_loc.at[:, columns(dy, dz)], v_all.at[pl.ds(rows * back, rows), :], v_ssem.at[dy * 4 + dz],
                    v_rsem.at[back], place(0, dy, dz, 0))
        copy.start()
        v_out.append(copy)
    own_v = pltpu.make_async_copy(v_loc.at[:, columns(0, 0)], v_all.at[pl.ds(0, rows), :], own_sem.at[1])
    own_v.start()

    def held(dx, dy, dz):
        source = place(dx, dy, dz, 0)[1]
        return r_all.at[:, pl.ds(pl.multiple_of(source * share, share), share), :]

    x_out = []
    for dy, dz in [(0, 0)] + [(dy, (4 - dz) % 4) for dy, dz in offsets]:
        slot = dy * 4 + dz
        piece = held(0, dy, dz)
        if slot == 0:
            own_r.wait()
        else:
            arrived(piece, r_rsem.at[slot])
        for dx in (1, 3, 2):
            at = (4 - dx) * Q + slot
            copy = send(piece, piece, x_ssem.at[dx * Q + slot], r_rsem.at[at], place(dx, 0, 0, 0))
            copy.start()
            x_out.append(copy)
    for dx in (1, 3, 2):
        for dy, dz in [(0, 0)] + [(dy, (4 - dz) % 4) for dy, dz in offsets]:
            arrived(held(dx, dy, dz), r_rsem.at[dx * Q + dy * 4 + dz])

    nt = (((1,), (1,)), ((), ()))

    g_send[...] = jnp.zeros_like(g_send)

    @pl.loop(0, chunk // step)
    def _(j):
        cols = pl.ds(pl.multiple_of(j * step, 128), step)
        g_send[...] += lax.dot_general(r_all[0, :, cols], r_all[1, :, cols], nt, preferred_element_type=F32)

    def order_of(d):
        across, far = place_of(d)
        return lax.rem(far, Q) * R + across

    def own_rows(d, count):
        return pl.ds(pl.multiple_of(order_of(d) * count, count), count)

    part = panel // GROUP

    def g_out(d):
        return send(g_send.at[own_rows(d, part), :], g_recv.at[mirror(d)], gs_ssem.at[d], gs_rsem.at[mirror(d)], place_of(d))

    @pl.loop(1, GROUP)
    def _(d):
        g_out(d).start()

    def block(dy, dz):
        slot = dy * 4 + dz
        for p in range(2):
            def body(j, total):
                cols = pl.ds(pl.multiple_of(j * step, 128), step)
                return total + lax.dot_general(
                    v_all[pl.ds(slot * rows, rows), cols], r_all[p, :, cols], nt, preferred_element_type=F32)
            total = lax.fori_loop(0, chunk // step, body, jnp.zeros((rows, panel), F32))
            p_send[pl.ds(slot * rows, rows), p * panel:(p + 1) * panel] = total.astype(BF16)

    def block_rows(d):
        across, _ = place_of(d)
        return pl.ds(pl.multiple_of((d // R) * rows + across * per, per), per)

    def p_out(d):
        return send(p_send.at[block_rows(d), :], p_recv.at[mirror(d)], ps_ssem.at[d], ps_rsem.at[mirror(d)], place_of(d))

    def p_start(dy, dz):
        slot = dy * 4 + dz
        for dr in range(R):
            if slot * R + dr:
                p_out(slot * R + dr).start()

    own_v.wait()
    block(0, 0)
    p_start(0, 0)

    def g_finish():
        @pl.loop(1, GROUP)
        def _(d):
            arrived(g_recv.at[d], gs_rsem.at[d])
        g_own[...] = jnp.sum(g_recv[1:], axis=0) + g_send[own_rows(0, part), :]

        @pl.loop(1, GROUP)
        def _(d):
            send(g_own, g_all.at[own_rows(0, part), :], ga_ssem.at[d], ga_rsem.at[mirror(d)], place_of(d)).start()
        g_all[own_rows(0, part), :] = g_own[...]

    for number, (dy, dz) in enumerate([(dy, (4 - dz) % 4) for dy, dz in offsets]):
        slot = dy * 4 + dz
        arrived(v_all.at[pl.ds(slot * rows, rows), :], v_rsem.at[slot])
        block(dy, dz)
        p_start(dy, dz)
        if number == 3:
            g_finish()

    @pl.loop(1, GROUP)
    def _(d):
        arrived(p_recv.at[d], ps_rsem.at[d])

    product = p_send[block_rows(0), :].astype(F32)
    product = product + jnp.sum(p_recv[1:].astype(F32), axis=0)

    def exact(a, b, dims):
        return lax.dot_general(a, b, dims, precision=lax.Precision.HIGHEST, preferred_element_type=F32)

    first = exact(product[:, :panel], factor[0], nt).astype(BF16)

    @pl.loop(1, GROUP)
    def _(d):
        arrived(g_all.at[own_rows(d, part), :], ga_rsem.at[d])
    rest = product[:, panel:] - exact(first.astype(F32), g_all[...], (((1,), (0,)), ((), ())))
    second = exact(rest, factor[1], nt).astype(BF16)
    s_own[:, :panel] = first
    s_own[:, panel:] = second

    def s_slot(d, across):
        return pl.ds(pl.multiple_of((d // R) * rows + across * per, per), per)

    def s_out(d):
        return send(s_own, s_all.at[s_slot(mirror(d), prow), :], sa_ssem.at[d], sa_rsem.at[mirror(d)], place_of(d))

    @pl.loop(1, GROUP)
    def _(d):
        s_out(d).start()
    s_all[s_slot(0, prow), :] = s_own[...]

    @pl.loop(1, GROUP)
    def _(d):
        arrived(s_all.at[s_slot(d, place_of(d)[0]), :], sa_rsem.at[d])

    base = lax.rem(pcol, Q) * chunk

    def put(d, j):
        there = pl.ds(pl.multiple_of(base + j * step, 128), step)
        here = pl.ds(pl.multiple_of(j * step, 128), step)
        return send(v_all.at[block_rows(d), here], out.at[prow, :, there], o_ssem.at[d], o_rsem.at[mirror(d)], place_of(d))

    def keep(j):
        there = pl.ds(pl.multiple_of(base + j * step, 128), step)
        here = pl.ds(pl.multiple_of(j * step, 128), step)
        return pltpu.make_async_copy(v_all.at[block_rows(0), here], out.at[prow, :, there], o_own.at[0])

    @pl.loop(0, chunk // step)
    def _(j):
        cols = pl.ds(pl.multiple_of(j * step, 128), step)
        change = jnp.dot(s_all[:, :panel], r_all[0, :, cols], preferred_element_type=F32)
        change = change + jnp.dot(s_all[:, panel:], r_all[1, :, cols], preferred_element_type=F32)
        v_all[:, cols] = (v_all[:, cols].astype(F32) - change).astype(BF16)

        @pl.loop(1, GROUP)
        def _(d):
            put(d, j).start()
        keep(j).start()

    for copy in r_out + v_out + x_out:
        copy.wait_send()
    whole_rows = out.at[0, :, pl.ds(0, chunk)]
    arrived(whole_rows, o_own.at[0])

    @pl.loop(1, GROUP)
    def _(d):
        arrived(g_recv.at[0], gs_ssem.at[d])
        arrived(g_own, ga_ssem.at[d])
        arrived(p_recv.at[0], ps_ssem.at[d])
        arrived(s_own, sa_ssem.at[d])
        arrived(whole_rows, o_ssem.at[d])
        across, far = place_of(d)
        there = pl.ds(pl.multiple_of(lax.rem(far, Q) * chunk, 128), chunk)
        arrived(out.at[across, :, there], o_rsem.at[d])


def body(vectors, reflectors, panel_factor):
    rows, width = vectors.shape
    panel = panel_factor.shape[1]
    share = reflectors.shape[1]
    tiles = pl.cdiv(width, 128)
    chunk = pl.cdiv(tiles, Q) * 128
    whole = (tiles - 1) * 128
    step = chunk // 6
    dims = (rows, panel, whole, width - whole, chunk, step)
    per = rows // R
    any_spec = pl.BlockSpec(memory_space=pl.ANY)
    dma = pltpu.SemaphoreType.DMA
    gathered = pl.pallas_call(
        functools.partial(kernel, dims),
        grid=(1,),
        out_shape=jax.ShapeDtypeStruct((R, per, chunk * Q), BF16),
        in_specs=[
            any_spec, any_spec,
            pl.BlockSpec((rows, 128), lambda i: (0, tiles - 1)),
            pl.BlockSpec((2, share, 128), lambda i: (0, 0, tiles - 1)),
            pl.BlockSpec((2, panel, panel), lambda i: (0, 0, 0)),
        ],
        out_specs=any_spec,
        scratch_shapes=[
            pltpu.VMEM((rows, chunk * Q), BF16),
            pltpu.VMEM((2, share, chunk * Q), BF16),
            pltpu.VMEM((rows * Q, chunk), BF16),
            pltpu.VMEM((2, panel, chunk), BF16),
            pltpu.VMEM((rows * Q, 2 * panel), BF16),
            pltpu.VMEM((GROUP, per, 2 * panel), BF16),
            pltpu.VMEM((panel, panel), F32),
            pltpu.VMEM((GROUP, panel // GROUP, panel), F32),
            pltpu.VMEM((panel // GROUP, panel), F32),
            pltpu.VMEM((panel, panel), F32),
            pltpu.VMEM((per, 2 * panel), BF16),
            pltpu.VMEM((rows * Q, 2 * panel), BF16),
            dma((2,)), dma((2,)), dma((Q,)), dma((X * Q,)), dma((X * Q,)), dma((Q,)), dma((Q,)),
            dma((GROUP,)), dma((GROUP,)), dma((GROUP,)), dma((GROUP,)), dma((GROUP,)), dma((GROUP,)),
            dma((GROUP,)), dma((GROUP,)), dma((GROUP,)), dma((GROUP,)), dma((1,)),
        ],
        compiler_params=pltpu.CompilerParams(
            collective_id=0, has_side_effects=True, vmem_limit_bytes=48 * 1024 * 1024
        ),
        name="back_transform",
    )(vectors, reflectors, vectors, reflectors, panel_factor)
    return jnp.concatenate([gathered[r, :, :width] for r in range(R)], axis=1)[None]


def solution(mesh):
    placed = (P("pcol", "prow"), P(None, "pcol", "prow"), P())
    return jax.shard_map(
        body, mesh=mesh, in_specs=placed, out_specs=P("pcol", "prow", None), check_vma=False
    )
```

```python
import functools

import jax
import jax.numpy as jnp
from jax import lax
from jax.experimental import pallas as pl
from jax.experimental.pallas import tpu as pltpu
from jax.sharding import PartitionSpec as P

X, YL, Z, R = 4, 2, 4, 4
Q = YL * Z
GROUP = Q * R
BF16, F32 = jnp.bfloat16, jnp.float32


def kernel(
    dims,
    v_hbm, r_hbm, v_tail, r_tail, factor,
    out,
    v_loc, r_loc, v_all, r_all, p_send, p_recv, g_send, g_recv, g_own, g_all, s_own, s_all,
    ld_sem, own_sem, r_ssem, r_rsem, x_ssem, v_ssem, v_rsem,
    gs_ssem, gs_rsem, ga_ssem, ga_rsem, ps_ssem, ps_rsem, sa_ssem, sa_rsem, o_ssem, o_rsem, o_own,
):
    rows, panel, whole, valid, chunk, step = dims
    per = rows // R
    share = panel // (X * Q)
    prow, pcol = lax.axis_index("prow"), lax.axis_index("pcol")
    x, yl, z = pcol // Q, lax.rem(pcol // Z, YL), lax.rem(pcol, Z)
    h, k = prow // 2, lax.rem(prow, 2)

    def place(dx, dy, dz, dr):
        far = lax.rem(x + dx, X) * Q + lax.rem(yl + dy, YL) * Z + lax.rem(z + dz, Z)
        across = lax.rem(h + dr // 2, 2) * 2 + lax.rem(k + dr % 2, 2)
        return across, far

    def place_of(d):
        dy, dz, dr = d // 16, lax.rem(d // 4, 4), lax.rem(d, 4)
        far = x * Q + lax.rem(yl + dy, YL) * Z + lax.rem(z + dz, Z)
        across = lax.rem(h + dr // 2, 2) * 2 + lax.rem(k + lax.rem(dr, 2), 2)
        return across, far

    def mirror(d):
        dy, dz, dr = d // 16, lax.rem(d // 4, 4), lax.rem(d, 4)
        return dy * 16 + lax.rem(4 - dz, 4) * 4 + dr

    def send(src, dst, ssem, rsem, to):
        return pltpu.make_async_remote_copy(
            src_ref=src, dst_ref=dst, send_sem=ssem, recv_sem=rsem,
            device_id=to, device_id_type=pl.DeviceIdType.MESH,
        )

    def arrived(ref, sem):
        pltpu.make_async_copy(ref, ref, sem).wait()

    load_r = pltpu.make_async_copy(r_hbm.at[:, :, pl.ds(0, whole)], r_loc.at[:, :, pl.ds(0, whole)], ld_sem.at[0])
    load_v = pltpu.make_async_copy(v_hbm.at[:, pl.ds(0, whole)], v_loc.at[:, pl.ds(0, whole)], ld_sem.at[1])
    load_r.start()
    load_v.start()

    barrier = pltpu.get_barrier_semaphore()

    @pl.loop(1, GROUP)
    def _(d):
        pl.semaphore_signal(barrier, inc=1, device_id=place_of(d), device_id_type=pl.DeviceIdType.MESH)

    for dx in range(1, X):
        pl.semaphore_signal(barrier, inc=1, device_id=place(dx, 0, 0, 0), device_id_type=pl.DeviceIdType.MESH)

    edge = v_loc.shape[1] - whole
    lane = lax.broadcasted_iota(jnp.int32, (rows, 128), 1)
    v_loc[:, whole:] = jnp.zeros((rows, edge), BF16)
    v_loc[:, whole:whole + 128] = jnp.where(lane < valid, v_tail[...].astype(F32), 0.0).astype(BF16)
    lane8 = lax.broadcasted_iota(jnp.int32, (share, 128), 1)
    for p in range(2):
        r_loc[p, :, whole:] = jnp.zeros((share, edge), BF16)
        r_loc[p, :, whole:whole + 128] = jnp.where(lane8 < valid, r_tail[p].astype(F32), 0.0).astype(BF16)

    pl.semaphore_wait(barrier, GROUP - 1 + X - 1)

    offsets = [(dy, dz) for dz in (1, 3, 2, 0) for dy in (0, 1) if (dy, dz) != (0, 0)]
    mine = pl.ds(pl.multiple_of(pcol * share, share), share)

    def columns(dy, dz):
        q = lax.rem(yl + dy, YL) * Z + lax.rem(z + dz, Z)
        return pl.ds(pl.multiple_of(q * chunk, 128), chunk)

    load_r.wait()
    r_out = []
    for dy, dz in offsets:
        back = dy * 4 + (4 - dz) % 4
        copy = send(r_loc.at[:, :, columns(dy, dz)], r_all.at[:, mine, :], r_ssem.at[dy * 4 + dz],
                    r_rsem.at[back], place(0, dy, dz, 0))
        copy.start()
        r_out.append(copy)
    own_r = pltpu.make_async_copy(r_loc.at[:, :, columns(0, 0)], r_all.at[:, mine, :], own_sem.at[0])
    own_r.start()
    load_v.wait()
    v_out = []
    for dy, dz in offsets:
        back = dy * 4 + (4 - dz) % 4
        copy = send(v_loc.at[:, columns(dy, dz)], v_all.at[pl.ds(rows * back, rows), :], v_ssem.at[dy * 4 + dz],
                    v_rsem.at[back], place(0, dy, dz, 0))
        copy.start()
        v_out.append(copy)
    own_v = pltpu.make_async_copy(v_loc.at[:, columns(0, 0)], v_all.at[pl.ds(0, rows), :], own_sem.at[1])
    own_v.start()

    def held(dx, dy, dz):
        source = place(dx, dy, dz, 0)[1]
        return r_all.at[:, pl.ds(pl.multiple_of(source * share, share), share), :]

    x_out = []
    for dy, dz in [(0, 0)] + [(dy, (4 - dz) % 4) for dy, dz in offsets]:
        slot = dy * 4 + dz
        piece = held(0, dy, dz)
        if slot == 0:
            own_r.wait()
        else:
            arrived(piece, r_rsem.at[slot])
        for dx in (1, 3, 2):
            at = (4 - dx) * Q + slot
            copy = send(piece, piece, x_ssem.at[dx * Q + slot], r_rsem.at[at], place(dx, 0, 0, 0))
            copy.start()
            x_out.append(copy)
    for dx in (1, 3, 2):
        for dy, dz in [(0, 0)] + [(dy, (4 - dz) % 4) for dy, dz in offsets]:
            arrived(held(dx, dy, dz), r_rsem.at[dx * Q + dy * 4 + dz])

    nt = (((1,), (1,)), ((), ()))

    g_send[...] = jnp.zeros_like(g_send)

    @pl.loop(0, chunk // step)
    def _(j):
        cols = pl.ds(pl.multiple_of(j * step, 128), step)
        g_send[...] += lax.dot_general(r_all[0, :, cols], r_all[1, :, cols], nt, preferred_element_type=F32)

    def order_of(d):
        across, far = place_of(d)
        return lax.rem(far, Q) * R + across

    def own_rows(d, count):
        return pl.ds(pl.multiple_of(order_of(d) * count, count), count)

    part = panel // GROUP

    def g_out(d):
        return send(g_send.at[own_rows(d, part), :], g_recv.at[mirror(d)], gs_ssem.at[d], gs_rsem.at[mirror(d)], place_of(d))

    @pl.loop(1, GROUP)
    def _(d):
        g_out(d).start()

    def block(dy, dz):
        slot = dy * 4 + dz
        for p in range(2):
            def body(j, total):
                cols = pl.ds(pl.multiple_of(j * step, 128), step)
                return total + lax.dot_general(
                    v_all[pl.ds(slot * rows, rows), cols], r_all[p, :, cols], nt, preferred_element_type=F32)
            total = lax.fori_loop(0, chunk // step, body, jnp.zeros((rows, panel), F32))
            p_send[pl.ds(slot * rows, rows), p * panel:(p + 1) * panel] = total.astype(BF16)

    def block_rows(d):
        across, _ = place_of(d)
        return pl.ds(pl.multiple_of((d // R) * rows + across * per, per), per)

    def p_out(d):
        return send(p_send.at[block_rows(d), :], p_recv.at[mirror(d)], ps_ssem.at[d], ps_rsem.at[mirror(d)], place_of(d))

    def p_start(dy, dz):
        slot = dy * 4 + dz
        for dr in range(R):
            if slot * R + dr:
                p_out(slot * R + dr).start()

    own_v.wait()
    block(0, 0)
    p_start(0, 0)

    def g_finish():
        @pl.loop(1, GROUP)
        def _(d):
            arrived(g_recv.at[d], gs_rsem.at[d])
        g_own[...] = jnp.sum(g_recv[1:], axis=0) + g_send[own_rows(0, part), :]

        @pl.loop(1, GROUP)
        def _(d):
            send(g_own, g_all.at[own_rows(0, part), :], ga_ssem.at[d], ga_rsem.at[mirror(d)], place_of(d)).start()
        g_all[own_rows(0, part), :] = g_own[...]

    for number, (dy, dz) in enumerate([(dy, (4 - dz) % 4) for dy, dz in offsets]):
        slot = dy * 4 + dz
        arrived(v_all.at[pl.ds(slot * rows, rows), :], v_rsem.at[slot])
        block(dy, dz)
        p_start(dy, dz)
        if number == 3:
            g_finish()

    @pl.loop(1, GROUP)
    def _(d):
        arrived(p_recv.at[d], ps_rsem.at[d])

    product = p_send[block_rows(0), :].astype(F32)
    product = product + jnp.sum(p_recv[1:].astype(F32), axis=0)

    def exact(a, b, dims):
        return lax.dot_general(a, b, dims, precision=lax.Precision.HIGHEST, preferred_element_type=F32)

    first = exact(product[:, :panel], factor[0], nt).astype(BF16)

    @pl.loop(1, GROUP)
    def _(d):
        arrived(g_all.at[own_rows(d, part), :], ga_rsem.at[d])
    rest = product[:, panel:] - exact(first.astype(F32), g_all[...], (((1,), (0,)), ((), ())))
    second = exact(rest, factor[1], nt).astype(BF16)
    s_own[:, :panel] = first
    s_own[:, panel:] = second

    def s_slot(d, across):
        return pl.ds(pl.multiple_of((d // R) * rows + across * per, per), per)

    def s_out(d):
        return send(s_own, s_all.at[s_slot(mirror(d), prow), :], sa_ssem.at[d], sa_rsem.at[mirror(d)], place_of(d))

    @pl.loop(1, GROUP)
    def _(d):
        s_out(d).start()
    s_all[s_slot(0, prow), :] = s_own[...]

    @pl.loop(1, GROUP)
    def _(d):
        arrived(s_all.at[s_slot(d, place_of(d)[0]), :], sa_rsem.at[d])

    base = lax.rem(pcol, Q) * chunk

    def put(d, j):
        there = pl.ds(pl.multiple_of(base + j * step, 128), step)
        here = pl.ds(pl.multiple_of(j * step, 128), step)
        return send(v_all.at[block_rows(d), here], out.at[prow, :, there], o_ssem.at[d], o_rsem.at[mirror(d)], place_of(d))

    def keep(j):
        there = pl.ds(pl.multiple_of(base + j * step, 128), step)
        here = pl.ds(pl.multiple_of(j * step, 128), step)
        return pltpu.make_async_copy(v_all.at[block_rows(0), here], out.at[prow, :, there], o_own.at[0])

    @pl.loop(0, chunk // step)
    def _(j):
        cols = pl.ds(pl.multiple_of(j * step, 128), step)
        change = jnp.dot(s_all[:, :panel], r_all[0, :, cols], preferred_element_type=F32)
        change = change + jnp.dot(s_all[:, panel:], r_all[1, :, cols], preferred_element_type=F32)
        v_all[:, cols] = (v_all[:, cols].astype(F32) - change).astype(BF16)

        @pl.loop(1, GROUP)
        def _(d):
            put(d, j).start()
        keep(j).start()

    for copy in r_out + v_out + x_out:
        copy.wait_send()
    whole_rows = out.at[0, :, pl.ds(0, chunk)]
    arrived(whole_rows, o_own.at[0])

    @pl.loop(1, GROUP)
    def _(d):
        arrived(g_recv.at[0], gs_ssem.at[d])
        arrived(g_own, ga_ssem.at[d])
        arrived(p_recv.at[0], ps_ssem.at[d])
        arrived(s_own, sa_ssem.at[d])
        arrived(whole_rows, o_ssem.at[d])
        across, far = place_of(d)
        there = pl.ds(pl.multiple_of(lax.rem(far, Q) * chunk, 128), chunk)
        arrived(out.at[across, :, there], o_rsem.at[d])


def joined(width, pieces, out, held, line, in_sem, out_sem):
    loads = [pltpu.make_async_copy(pieces.at[r], held.at[r], in_sem.at[r]) for r in range(R)]
    for load in loads:
        load.start()
    stores = []
    rows = held.shape[1]
    for r in range(R):
        loads[r].wait()
        first, shift = r * width // 128 * 128, r * width % 128
        end = (r + 1) * width // 128 * 128
        if shift == 0:
            source = held.at[r, :, pl.ds(0, end - first)]
        else:
            count = (end - first) // 128
            lane = lax.broadcasted_iota(jnp.int32, (rows, 128), 1)
            keep = held[r - 1, :, pl.ds(first - (r - 1) * width // 128 * 128, 128)].astype(F32)
            turned = pltpu.roll(held[r, :, :128].astype(F32), shift, 1)
            line[r // 2, :, :128] = jnp.where(lane < shift, keep, turned).astype(BF16)
            width_step = 13 * 128
            for a in range(128, count * 128, width_step):
                n = min(width_step, count * 128 - a)
                wide = held[r, :, a - 128:a + n].astype(F32)
                line[r // 2, :, a:a + n] = pltpu.roll(wide, shift, 1)[:, 128:].astype(BF16)
            source = line.at[r // 2]
        store = pltpu.make_async_copy(source, out.at[:, pl.ds(first, end - first)], out_sem.at[r])
        store.start()
        stores.append(store)
    for store in stores:
        store.wait()


def body(vectors, reflectors, panel_factor):
    rows, width = vectors.shape
    panel = panel_factor.shape[1]
    share = reflectors.shape[1]
    tiles = pl.cdiv(width, 128)
    chunk = pl.cdiv(tiles, Q) * 128
    whole = (tiles - 1) * 128
    step = chunk // 6
    dims = (rows, panel, whole, width - whole, chunk, step)
    per = rows // R
    any_spec = pl.BlockSpec(memory_space=pl.ANY)
    dma = pltpu.SemaphoreType.DMA
    gathered = pl.pallas_call(
        functools.partial(kernel, dims),
        grid=(1,),
        out_shape=jax.ShapeDtypeStruct((R, per, chunk * Q), BF16),
        in_specs=[
            any_spec, any_spec,
            pl.BlockSpec((rows, 128), lambda i: (0, tiles - 1)),
            pl.BlockSpec((2, share, 128), lambda i: (0, 0, tiles - 1)),
            pl.BlockSpec((2, panel, panel), lambda i: (0, 0, 0)),
        ],
        out_specs=any_spec,
        scratch_shapes=[
            pltpu.VMEM((rows, chunk * Q), BF16),
            pltpu.VMEM((2, share, chunk * Q), BF16),
            pltpu.VMEM((rows * Q, chunk), BF16),
            pltpu.VMEM((2, panel, chunk), BF16),
            pltpu.VMEM((rows * Q, 2 * panel), BF16),
            pltpu.VMEM((GROUP, per, 2 * panel), BF16),
            pltpu.VMEM((panel, panel), F32),
            pltpu.VMEM((GROUP, panel // GROUP, panel), F32),
            pltpu.VMEM((panel // GROUP, panel), F32),
            pltpu.VMEM((panel, panel), F32),
            pltpu.VMEM((per, 2 * panel), BF16),
            pltpu.VMEM((rows * Q, 2 * panel), BF16),
            dma((2,)), dma((2,)), dma((Q,)), dma((X * Q,)), dma((X * Q,)), dma((Q,)), dma((Q,)),
            dma((GROUP,)), dma((GROUP,)), dma((GROUP,)), dma((GROUP,)), dma((GROUP,)), dma((GROUP,)),
            dma((GROUP,)), dma((GROUP,)), dma((GROUP,)), dma((GROUP,)), dma((1,)),
        ],
        compiler_params=pltpu.CompilerParams(
            collective_id=0, has_side_effects=True, vmem_limit_bytes=61 * 1024 * 1024
        ),
        name="back_transform",
    )(vectors, reflectors, vectors, reflectors, panel_factor)
    line = R * width // 128 * 128 - 3 * width // 128 * 128
    rows_out = pl.pallas_call(
        functools.partial(joined, width),
        out_shape=jax.ShapeDtypeStruct((per, R * width), BF16),
        in_specs=[any_spec],
        out_specs=any_spec,
        scratch_shapes=[
            pltpu.VMEM((R, per, chunk * Q), BF16), pltpu.VMEM((2, per, line), BF16), dma((R,)), dma((R,)),
        ],
        compiler_params=pltpu.CompilerParams(vmem_limit_bytes=61 * 1024 * 1024),
        name="joined",
    )(gathered)
    return rows_out[None]


def solution(mesh):
    placed = (P("pcol", "prow"), P(None, "pcol", "prow"), P())
    return jax.shard_map(
        body, mesh=mesh, in_specs=placed, out_specs=P("pcol", "prow", None), check_vma=False
    )
```

```python
import functools

import jax
import jax.numpy as jnp
from jax import lax
from jax.experimental import pallas as pl
from jax.experimental.pallas import tpu as pltpu
from jax.sharding import PartitionSpec as P

X, YL, Z, R = 4, 2, 4, 4
Q = YL * Z
GROUP = Q * R
ORDER = ((0, 0), (0, 3), (0, 1), (1, 3), (1, 1), (0, 2), (1, 2), (1, 0))
SLOT = {pair: number for number, pair in enumerate(ORDER)}
OTHERS = range(1, GROUP)
HELD = 0
BF16, F32 = jnp.bfloat16, jnp.float32
NT = (((1,), (1,)), ((), ()))


def mirror(d):
    dy, dz = ORDER[d // R]
    return SLOT[dy, (4 - dz) % 4] * R + d % R


def halves(value):
    high = value.astype(BF16)
    return high, (value - high.astype(F32)).astype(BF16)


def times(value, high, low):
    a, b = halves(value)
    total = lax.dot_general(a, high, NT, preferred_element_type=F32)
    total = total + lax.dot_general(b, high, NT, preferred_element_type=F32)
    return total + lax.dot_general(a, low, NT, preferred_element_type=F32)


def kernel(
    dims,
    v_hbm, r_hbm, v_tail, r_tail, factor,
    out,
    v_loc, r_loc, v_all, r_all, p_send, p_recv, g_send, g_recv, g_own, g_all, s_own, s_all, f_high, f_low,
    ld_sem, own_sem, r_ssem, r_rsem, x_ssem, v_ssem, v_rsem,
    gs_ssem, gs_rsem, ga_ssem, ga_rsem, ps_ssem, ps_rsem, sa_ssem, sa_rsem, o_ssem, o_rsem, o_own,
):
    rows, panel, whole, valid, chunk, step = dims
    per = rows // R
    share = panel // (X * Q)
    half = chunk // 2
    prow, pcol = lax.axis_index("prow"), lax.axis_index("pcol")
    x, yl, z = pcol // Q, lax.rem(pcol // Z, YL), lax.rem(pcol, Z)
    h, k = prow // 2, lax.rem(prow, 2)

    yls = [yl, 1 - yl]
    zs = [z] + [lax.rem(z + dz, Z) for dz in range(1, Z)]
    xs = [x] + [lax.rem(x + dx, X) for dx in range(1, X)]
    prows = [prow, h * 2 + 1 - k, (1 - h) * 2 + k, (1 - h) * 2 + 1 - k]

    def at(d, dx=0):
        dy, dz = ORDER[d // R]
        return prows[d % R], xs[dx] * Q + yls[dy] * Z + zs[dz]

    def send(src, dst, ssem, rsem, to):
        copy = pltpu.make_async_remote_copy(
            src_ref=src, dst_ref=dst, send_sem=ssem, recv_sem=rsem,
            device_id=to, device_id_type=pl.DeviceIdType.MESH,
        )
        copy.start()
        return copy

    def arrived(ref, sem):
        pltpu.make_async_copy(ref, ref, sem).wait()

    load_r = pltpu.make_async_copy(r_hbm.at[:, :, pl.ds(0, whole)], r_loc.at[:, :, pl.ds(0, whole)], ld_sem.at[0])
    load_v = pltpu.make_async_copy(v_hbm.at[:, pl.ds(0, whole)], v_loc.at[:, pl.ds(0, whole)], ld_sem.at[1])
    load_r.start()
    load_v.start()

    barrier = pltpu.get_barrier_semaphore()
    for d in OTHERS:
        pl.semaphore_signal(barrier, inc=1, device_id=at(d), device_id_type=pl.DeviceIdType.MESH)
    for dx in (1, 3):
        pl.semaphore_signal(barrier, inc=1, device_id=at(0, dx), device_id_type=pl.DeviceIdType.MESH)

    edge = v_loc.shape[1] - whole
    lane = lax.broadcasted_iota(jnp.int32, (rows, 128), 1)
    v_loc[:, whole:] = jnp.zeros((rows, edge), BF16)
    v_loc[:, whole:whole + 128] = jnp.where(lane < valid, v_tail[...].astype(F32), 0.0).astype(BF16)
    lane8 = lax.broadcasted_iota(jnp.int32, (share, 128), 1)
    for p in range(2):
        r_loc[p, :, whole:] = jnp.zeros((share, edge), BF16)
        r_loc[p, :, whole:whole + 128] = jnp.where(lane8 < valid, r_tail[p].astype(F32), 0.0).astype(BF16)

    pl.semaphore_wait(barrier, GROUP - 1 + 2)

    mine = pl.ds(pl.multiple_of(pcol * share, share), share)

    def columns(slot):
        q = lax.rem(at(slot * R)[1], Q)
        return pl.ds(pl.multiple_of(q * chunk, 128), chunk)

    def rows_at(slot, count=1):
        return pl.ds(slot * rows, count * rows)

    load_r.wait()
    own_r = pltpu.make_async_copy(r_loc.at[:, :, columns(0)], r_all.at[:, mine, :], own_sem.at[0])
    own_r.start()
    for slot in range(1, Q):
        d = mirror(slot * R)
        send(r_loc.at[:, :, columns(d // R)], r_all.at[:, mine, :], r_ssem.at[slot], r_rsem.at[slot], at(d))
    load_v.wait()
    own_v = pltpu.make_async_copy(v_loc.at[:, columns(0)], v_all.at[rows_at(0), :], own_sem.at[1])
    own_v.start()

    def v_out(slot):
        d = mirror(slot * R)
        send(v_loc.at[:, columns(d // R)], v_all.at[rows_at(slot), :], v_ssem.at[slot], v_rsem.at[slot], at(d))

    for slot in range(1, Q - HELD):
        v_out(slot)

    def piece(slot, dx, cols=None):
        source = pl.ds(pl.multiple_of(at(slot * R, dx)[1] * share, share), share)
        return r_all.at[:, source, :] if cols is None else r_all.at[:, source, cols]

    parts = (pl.ds(0, half), pl.ds(half, half))

    def spread(slot):
        if slot == 0:
            own_r.wait()
        else:
            arrived(piece(slot, 0), r_rsem.at[slot])
        for dx in (1, 3):
            send(piece(slot, 0), piece(slot, 0), x_ssem.at[dx * Q + slot], r_rsem.at[(4 - dx) * Q + slot], at(0, dx))

    def relay(slot):
        for number, dx in enumerate((1, 3)):
            arrived(piece(slot, dx), r_rsem.at[dx * Q + slot])
            part = piece(slot, dx, parts[number])
            send(part, part, x_ssem.at[2 * number * Q + slot], r_rsem.at[(2 + 2 * number) * Q + slot], at(0, 4 - dx))

    lag = 1
    for slot in range(Q + lag):
        if slot < Q:
            spread(slot)
        if slot >= lag:
            relay(slot - lag)

    f_high[...], f_low[...] = halves(factor[...])
    for slot in range(Q):
        for number in range(2):
            arrived(piece(slot, 2, parts[number]), r_rsem.at[(2 + 2 * number) * Q + slot])

    def summed(a, b, m):
        def one(j, total):
            cols = pl.ds(pl.multiple_of(j * step, 128), step)
            return total + lax.dot_general(a(cols), b(cols), NT, preferred_element_type=F32)
        return lax.fori_loop(0, chunk // step, one, jnp.zeros((m, panel), F32))

    part = panel // GROUP
    gram = summed(lambda cols: r_all[0, :, cols], lambda cols: r_all[1, :, cols], panel)
    g_send[...] = gram.reshape(GROUP, part, panel).astype(BF16)

    def owner(d):
        across, far = at(d)
        return lax.rem(far, Q) * R + across

    for d in OTHERS:
        send(g_send.at[owner(d)], g_recv.at[mirror(d)], gs_ssem.at[d], gs_rsem.at[mirror(d)], at(d))
    for slot in range(Q - HELD, Q):
        v_out(slot)

    def own_rows(slot, across):
        return pl.ds(pl.multiple_of(slot * rows + across * per, per), per)

    def products(first, count):
        for p in range(2):
            total = summed(lambda cols: v_all[rows_at(first, count), cols], lambda cols: r_all[p, :, cols], rows * count)
            p_send[rows_at(first, count), p * panel:(p + 1) * panel] = total.astype(BF16)
        for d in range(max(first * R, 1), (first + count) * R):
            send(p_send.at[own_rows(d // R, prows[d % R]), :], p_recv.at[mirror(d)], ps_ssem.at[d],
                 ps_rsem.at[mirror(d)], at(d))

    own_v.wait()
    for slot in range(1, 4):
        arrived(v_all.at[rows_at(slot), :], v_rsem.at[slot])
    products(0, 4)

    for d in OTHERS:
        arrived(g_recv.at[d], gs_rsem.at[d])
    g_own[...] = (jnp.sum(g_recv[1:].astype(F32), axis=0) + g_send[owner(0)].astype(F32)).astype(BF16)
    for d in OTHERS:
        send(g_own, g_all.at[owner(0)], ga_ssem.at[d], ga_rsem.at[mirror(d)], at(d))
    g_all[owner(0)] = g_own[...]

    for slot in range(4, Q):
        arrived(v_all.at[rows_at(slot), :], v_rsem.at[slot])
    products(4, 4)

    for d in OTHERS:
        arrived(g_all.at[owner(d)], ga_rsem.at[d])
    for d in OTHERS:
        arrived(p_recv.at[d], ps_rsem.at[d])

    product = p_send[own_rows(0, prow), :].astype(F32)
    product = product + jnp.sum(p_recv[1:].astype(F32), axis=0)
    first = times(product[:, :panel], f_high[0], f_low[0]).astype(BF16)
    second = times(product[:, panel:], f_high[1], f_low[1])
    gram = g_all[...].reshape(panel, panel)
    second = second - times(jnp.dot(first, gram, preferred_element_type=F32), f_high[1], f_low[1])
    s_own[:, :panel] = first
    s_own[:, panel:] = second.astype(BF16)

    for d in OTHERS:
        send(s_own, s_all.at[own_rows(mirror(d) // R, prow), :], sa_ssem.at[d], sa_rsem.at[mirror(d)], at(d))
    s_all[own_rows(0, prow), :] = s_own[...]
    for d in OTHERS:
        arrived(s_all.at[own_rows(d // R, prows[d % R]), :], sa_rsem.at[d])

    base = lax.rem(pcol, Q) * chunk
    width = chunk // 6

    @pl.loop(0, chunk // width)
    def _(j):
        there = pl.ds(pl.multiple_of(base + j * width, 128), width)
        here = pl.ds(pl.multiple_of(j * width, 128), width)
        change = jnp.dot(s_all[:, :panel], r_all[0, :, here], preferred_element_type=F32)
        change = change + jnp.dot(s_all[:, panel:], r_all[1, :, here], preferred_element_type=F32)
        v_all[:, here] = (v_all[:, here].astype(F32) - change).astype(BF16)
        for d in OTHERS:
            send(v_all.at[own_rows(d // R, prows[d % R]), here], out.at[prow, :, there], o_ssem.at[d],
                 o_rsem.at[mirror(d)], at(d))
        pltpu.make_async_copy(v_all.at[own_rows(0, prow), here], out.at[prow, :, there], o_own.at[0]).start()

    for slot in range(Q):
        if slot:
            arrived(piece(slot, 0), r_ssem.at[slot])
            arrived(v_all.at[rows_at(slot), :], v_ssem.at[slot])
        for dx in (1, 3):
            arrived(piece(slot, 0), x_ssem.at[dx * Q + slot])
        for number in range(2):
            arrived(piece(slot, 0, parts[number]), x_ssem.at[2 * number * Q + slot])
    piece_rows = out.at[0, :, pl.ds(0, chunk)]
    arrived(piece_rows, o_own.at[0])
    for d in OTHERS:
        arrived(g_own, gs_ssem.at[d])
        arrived(g_own, ga_ssem.at[d])
        arrived(p_recv.at[0], ps_ssem.at[d])
        arrived(s_own, sa_ssem.at[d])
        arrived(piece_rows, o_ssem.at[d])
    for d in OTHERS:
        across, far = at(d)
        there = pl.ds(pl.multiple_of(lax.rem(far, Q) * chunk, 128), chunk)
        arrived(out.at[across, :, there], o_rsem.at[d])


def joined(width, pieces, out, held, line, in_sem, out_sem):
    loads = [pltpu.make_async_copy(pieces.at[r], held.at[r], in_sem.at[r]) for r in range(R)]
    for load in loads:
        load.start()
    stores = []
    rows = held.shape[1]
    for r in range(R):
        loads[r].wait()
        first, shift = r * width // 128 * 128, r * width % 128
        end = (r + 1) * width // 128 * 128
        if shift == 0:
            source = held.at[r, :, pl.ds(0, end - first)]
        else:
            count = (end - first) // 128
            lane = lax.broadcasted_iota(jnp.int32, (rows, 128), 1)
            keep = held[r - 1, :, pl.ds(first - (r - 1) * width // 128 * 128, 128)].astype(F32)
            turned = pltpu.roll(held[r, :, :128].astype(F32), shift, 1)
            line[r // 2, :, :128] = jnp.where(lane < shift, keep, turned).astype(BF16)
            width_step = 13 * 128
            for a in range(128, count * 128, width_step):
                n = min(width_step, count * 128 - a)
                wide = held[r, :, a - 128:a + n].astype(F32)
                line[r // 2, :, a:a + n] = pltpu.roll(wide, shift, 1)[:, 128:].astype(BF16)
            source = line.at[r // 2]
        store = pltpu.make_async_copy(source, out.at[:, pl.ds(first, end - first)], out_sem.at[r])
        store.start()
        stores.append(store)
    for store in stores:
        store.wait()


def body(vectors, reflectors, panel_factor):
    rows, width = vectors.shape
    panel = panel_factor.shape[1]
    share = reflectors.shape[1]
    tiles = pl.cdiv(width, 128)
    chunk = pl.cdiv(tiles, Q) * 128
    whole = (tiles - 1) * 128
    dims = (rows, panel, whole, width - whole, chunk, chunk // 3)
    per = rows // R
    any_spec = pl.BlockSpec(memory_space=pl.ANY)
    dma = pltpu.SemaphoreType.DMA
    part = panel // GROUP
    gathered = pl.pallas_call(
        functools.partial(kernel, dims),
        grid=(1,),
        out_shape=jax.ShapeDtypeStruct((R, per, chunk * Q), BF16),
        in_specs=[
            any_spec, any_spec,
            pl.BlockSpec((rows, 128), lambda i: (0, tiles - 1)),
            pl.BlockSpec((2, share, 128), lambda i: (0, 0, tiles - 1)),
            pl.BlockSpec((2, panel, panel), lambda i: (0, 0, 0)),
        ],
        out_specs=any_spec,
        scratch_shapes=[
            pltpu.VMEM((rows, chunk * Q), BF16),
            pltpu.VMEM((2, share, chunk * Q), BF16),
            pltpu.VMEM((rows * Q, chunk), BF16),
            pltpu.VMEM((2, panel, chunk), BF16),
            pltpu.VMEM((rows * Q, 2 * panel), BF16),
            pltpu.VMEM((GROUP, per, 2 * panel), BF16),
            pltpu.VMEM((GROUP, part, panel), BF16),
            pltpu.VMEM((GROUP, part, panel), BF16),
            pltpu.VMEM((part, panel), BF16),
            pltpu.VMEM((GROUP, part, panel), BF16),
            pltpu.VMEM((per, 2 * panel), BF16),
            pltpu.VMEM((rows * Q, 2 * panel), BF16),
            pltpu.VMEM((2, panel, panel), BF16),
            pltpu.VMEM((2, panel, panel), BF16),
            dma((2,)), dma((2,)), dma((Q,)), dma(((X + 1) * Q,)), dma((X * Q,)), dma((Q,)), dma((Q,)),
            dma((GROUP,)), dma((GROUP,)), dma((GROUP,)), dma((GROUP,)), dma((GROUP,)), dma((GROUP,)),
            dma((GROUP,)), dma((GROUP,)), dma((GROUP,)), dma((GROUP,)), dma((1,)),
        ],
        compiler_params=pltpu.CompilerParams(
            collective_id=0, has_side_effects=True, vmem_limit_bytes=61 * 1024 * 1024
        ),
        name="back_transform",
    )(vectors, reflectors, vectors, reflectors, panel_factor)
    line = R * width // 128 * 128 - (R - 1) * width // 128 * 128
    rows_out = pl.pallas_call(
        functools.partial(joined, width),
        out_shape=jax.ShapeDtypeStruct((per, R * width), BF16),
        in_specs=[any_spec],
        out_specs=any_spec,
        scratch_shapes=[
            pltpu.VMEM((R, per, chunk * Q), BF16), pltpu.VMEM((2, per, line), BF16), dma((R,)), dma((R,)),
        ],
        compiler_params=pltpu.CompilerParams(vmem_limit_bytes=61 * 1024 * 1024),
        name="joined",
    )(gathered)
    return rows_out[None]


def solution(mesh):
    placed = (P("pcol", "prow"), P(None, "pcol", "prow"), P())
    return jax.shard_map(
        body, mesh=mesh, in_specs=placed, out_specs=P("pcol", "prow", None), check_vma=False
    )
```

```python
import functools

import jax
import jax.numpy as jnp
from jax import lax
from jax.experimental import pallas as pl
from jax.experimental.pallas import tpu as pltpu
from jax.sharding import PartitionSpec as P

X, YL, Z, R = 4, 2, 4, 4
Q = YL * Z
GROUP = Q * R
ORDER = ((0, 0), (1, 0), (1, 1), (1, 3), (0, 2), (1, 2), (0, 1), (0, 3))
SLOT = {pair: number for number, pair in enumerate(ORDER)}
LATE, THIRDS = Q // 2, 3


def hops(d):
    dy, dz = ORDER[d // R]
    return min(dz, Z - dz) + (1 if dy else d % R // 2 * 2)


OTHERS = sorted(range(1, GROUP), key=lambda d: -hops(d))

TURNS = (
    (
        ((0, 1, 2),),
        ((0, 1, 1), (0, 1, 3), (0, 0, 1), (0, 0, 3)),
        ((1, 0, 1), (1, 1, 3)),
        ((1, 0, 3), (1, 1, 1)),
        ((1, 0, 2), (1, 1, 2), (1, 0, 0), (1, 1, 0)),
        ((0, 1, 0), (0, 0, 2)),
    ),
    (
        ((1, 0, 0), (1, 1, 0), (1, 0, 2), (1, 1, 2)),
        ((1, 0, 1), (1, 1, 3)),
        ((1, 0, 3), (1, 1, 1)),
        ((0, 1, 2),),
        ((0, 1, 0), (0, 0, 2)),
        ((0, 1, 1), (0, 1, 3), (0, 0, 1), (0, 0, 3)),
    ),
)
LEAVING = [
    [SLOT[lo, dz] * R + hi * 2 + core for turn in turns for core in (0, 1) for lo, hi, dz in turn] + [1]
    for turns in TURNS
]
BF16, F32 = jnp.bfloat16, jnp.float32
NT = (((1,), (1,)), ((), ()))


def mirror(d):
    dy, dz = ORDER[d // R]
    return SLOT[dy, (4 - dz) % 4] * R + d % R


def halves(value):
    high = value.astype(BF16)
    return high, (value - high.astype(F32)).astype(BF16)


def times(value, high, low):
    a, b = halves(value)
    total = lax.dot_general(a, high, NT, preferred_element_type=F32)
    total = total + lax.dot_general(b, high, NT, preferred_element_type=F32)
    return total + lax.dot_general(a, low, NT, preferred_element_type=F32)


def kernel(
    dims,
    v_hbm, r_hbm, v_tail, r_tail, factor,
    out,
    v_loc, r_loc, v_all, r_all, p_sum, p_send, p_recv, g_send, g_recv, g_own, g_all, s_own, s_all, f_high, f_low,
    ld_sem, own_sem, r_ssem, r_rsem, x_ssem, v_ssem, v_rsem,
    gs_ssem, gs_rsem, ga_ssem, ga_rsem, ps_ssem, ps_rsem, sa_ssem, sa_rsem, o_ssem, o_rsem, o_own,
):
    rows, panel, whole, valid, chunk, step = dims
    per = rows // R
    share = panel // (X * Q)
    half = chunk // 2
    prow, pcol = lax.axis_index("prow"), lax.axis_index("pcol")
    x, yl, z = pcol // Q, lax.rem(pcol // Z, YL), lax.rem(pcol, Z)
    h, k = prow // 2, lax.rem(prow, 2)

    yls = [yl, 1 - yl]
    zs = [z] + [lax.rem(z + dz, Z) for dz in range(1, Z)]
    xs = [x] + [lax.rem(x + dx, X) for dx in range(1, X)]
    prows = [prow, h * 2 + 1 - k, (1 - h) * 2 + k, (1 - h) * 2 + 1 - k]

    def at(d, dx=0):
        dy, dz = ORDER[d // R]
        return prows[d % R], xs[dx] * Q + yls[dy] * Z + zs[dz]

    def send(src, dst, ssem, rsem, to):
        copy = pltpu.make_async_remote_copy(
            src_ref=src, dst_ref=dst, send_sem=ssem, recv_sem=rsem,
            device_id=to, device_id_type=pl.DeviceIdType.MESH,
        )
        copy.start()
        return copy

    def arrived(ref, sem):
        pltpu.make_async_copy(ref, ref, sem).wait()

    load_r = pltpu.make_async_copy(r_hbm.at[:, :, pl.ds(0, whole)], r_loc.at[:, :, pl.ds(0, whole)], ld_sem.at[0])
    load_v = pltpu.make_async_copy(v_hbm.at[:, pl.ds(0, whole)], v_loc.at[:, pl.ds(0, whole)], ld_sem.at[1])
    load_r.start()
    load_v.start()

    barrier = pltpu.get_barrier_semaphore()
    for d in OTHERS:
        pl.semaphore_signal(barrier, inc=1, device_id=at(d), device_id_type=pl.DeviceIdType.MESH)
    for dx in (1, 3):
        pl.semaphore_signal(barrier, inc=1, device_id=at(0, dx), device_id_type=pl.DeviceIdType.MESH)

    edge = v_loc.shape[1] - whole
    lane = lax.broadcasted_iota(jnp.int32, (rows, 128), 1)
    v_loc[:, whole:] = jnp.zeros((rows, edge), BF16)
    v_loc[:, whole:whole + 128] = jnp.where(lane < valid, v_tail[...].astype(F32), 0.0).astype(BF16)
    lane8 = lax.broadcasted_iota(jnp.int32, (share, 128), 1)
    for p in range(2):
        r_loc[p, :, whole:] = jnp.zeros((share, edge), BF16)
        r_loc[p, :, whole:whole + 128] = jnp.where(lane8 < valid, r_tail[p].astype(F32), 0.0).astype(BF16)

    pl.semaphore_wait(barrier, GROUP - 1 + 2)

    mine = pl.ds(pl.multiple_of(pcol * share, share), share)

    def columns(slot):
        q = lax.rem(at(slot * R)[1], Q)
        return pl.ds(pl.multiple_of(q * chunk, 128), chunk)

    def rows_at(slot, count=1):
        return pl.ds(slot * rows, count * rows)

    load_r.wait()
    own_r = pltpu.make_async_copy(r_loc.at[:, :, columns(0)], r_all.at[:, mine, :], own_sem.at[0])
    own_r.start()
    for slot in range(1, Q):
        d = mirror(slot * R)
        send(r_loc.at[:, :, columns(d // R)], r_all.at[:, mine, :], r_ssem.at[slot], r_rsem.at[slot], at(d))
    load_v.wait()
    own_v = pltpu.make_async_copy(v_loc.at[:, columns(0)], v_all.at[rows_at(0), :], own_sem.at[1])
    own_v.start()

    third = chunk // THIRDS

    def v_sem(slot, number):
        return slot if number is None else Q + slot * THIRDS + number

    def v_landing(slot, number=None):
        return v_all.at[rows_at(slot), pl.ds(0, chunk) if number is None else pl.ds(number * third, third)]

    def v_out(slot, number=None):
        d = mirror(slot * R)
        first = lax.rem(at(d)[1], Q) * chunk + (number or 0) * third
        source = v_loc.at[:, pl.ds(pl.multiple_of(first, 128), chunk if number is None else third)]
        sem = v_sem(slot, number)
        send(source, v_landing(slot, number), v_ssem.at[sem], v_rsem.at[sem], at(d))

    for slot in range(LATE, Q):
        v_out(slot)
    for number in range(THIRDS - 1):
        for slot in range(1, LATE):
            v_out(slot, number)

    def piece(slot, dx, cols=None):
        source = pl.ds(pl.multiple_of(at(slot * R, dx)[1] * share, share), share)
        return r_all.at[:, source, :] if cols is None else r_all.at[:, source, cols]

    parts = (pl.ds(0, half), pl.ds(half, half))

    def spread(slot):
        if slot == 0:
            own_r.wait()
        else:
            arrived(piece(slot, 0), r_rsem.at[slot])
        for dx in (1, 3):
            send(piece(slot, 0), piece(slot, 0), x_ssem.at[dx * Q + slot], r_rsem.at[(4 - dx) * Q + slot], at(0, dx))

    def relay(slot):
        for number, dx in enumerate((1, 3)):
            arrived(piece(slot, dx), r_rsem.at[dx * Q + slot])
            part = piece(slot, dx, parts[number])
            send(part, part, x_ssem.at[2 * number * Q + slot], r_rsem.at[(2 + 2 * number) * Q + slot], at(0, 4 - dx))

    lag = 1
    for slot in range(Q + lag):
        if slot < Q:
            spread(slot)
        if slot >= lag:
            relay(slot - lag)

    f_high[...], f_low[...] = halves(factor[...])
    for slot in range(Q):
        for number in range(2):
            arrived(piece(slot, 2, parts[number]), r_rsem.at[(2 + 2 * number) * Q + slot])

    def summed(a, b, m):
        def one(j, total):
            cols = pl.ds(pl.multiple_of(j * step, 128), step)
            return total + lax.dot_general(a(cols), b(cols), NT, preferred_element_type=F32)
        return lax.fori_loop(0, chunk // step, one, jnp.zeros((m, panel), F32))

    part = panel // GROUP
    gram = summed(lambda cols: r_all[0, :, cols], lambda cols: r_all[1, :, cols], panel)
    g_send[...] = gram.reshape(GROUP, part, panel).astype(BF16)

    def owner(d):
        across, far = at(d)
        return lax.rem(far, Q) * R + across

    for d in OTHERS:
        send(g_send.at[owner(d)], g_recv.at[mirror(d)], gs_ssem.at[d], gs_rsem.at[mirror(d)], at(d))
    for slot in range(1, LATE):
        v_out(slot, THIRDS - 1)

    def own_rows(slot, across):
        return pl.ds(pl.multiple_of(slot * rows + across * per, per), per)

    def p_out(first, count):
        for d in [d for d in OTHERS if first <= d // R < first + count]:
            send(p_send.at[own_rows(d // R, prows[d % R]), :], p_recv.at[mirror(d)], ps_ssem.at[d],
                 ps_rsem.at[mirror(d)], at(d))

    for slot in range(LATE, Q):
        arrived(v_landing(slot), v_rsem.at[slot])
    for p in range(2):
        total = summed(lambda cols: v_all[rows_at(LATE, Q - LATE), cols], lambda cols: r_all[p, :, cols], rows * (Q - LATE))
        p_send[rows_at(LATE, Q - LATE), p * panel:(p + 1) * panel] = total.astype(BF16)
    p_out(LATE, Q - LATE)
    own_v.wait()

    for number in range(THIRDS):
        if number == THIRDS - 1:
            for d in OTHERS:
                arrived(g_recv.at[d], gs_rsem.at[d])
            g_own[...] = (jnp.sum(g_recv[1:].astype(F32), axis=0) + g_send[owner(0)].astype(F32)).astype(BF16)
            for d in OTHERS:
                send(g_own, g_all.at[owner(0)], ga_ssem.at[d], ga_rsem.at[mirror(d)], at(d))
            g_all[owner(0)] = g_own[...]
        for slot in range(1, LATE):
            arrived(v_landing(slot, number), v_rsem.at[v_sem(slot, number)])
        cols = pl.ds(number * third, third)
        for p in range(2):
            here = slice(p * panel, (p + 1) * panel)
            total = lax.dot_general(
                v_all[rows_at(0, LATE), cols], r_all[p, :, cols], NT, preferred_element_type=F32)
            if number:
                total = total + p_sum[:, here]
            if number < THIRDS - 1:
                p_sum[:, here] = total
            else:
                p_send[rows_at(0, LATE), here] = total.astype(BF16)
    p_out(0, LATE)

    for d in OTHERS:
        arrived(g_all.at[owner(d)], ga_rsem.at[d])
    for d in OTHERS:
        arrived(p_recv.at[d], ps_rsem.at[d])

    product = p_send[own_rows(0, prow), :].astype(F32)
    product = product + jnp.sum(p_recv[1:].astype(F32), axis=0)
    first = times(product[:, :panel], f_high[0], f_low[0]).astype(BF16)
    second = times(product[:, panel:], f_high[1], f_low[1])
    gram = g_all[...].reshape(panel, panel)
    second = second - times(jnp.dot(first, gram, preferred_element_type=F32), f_high[1], f_low[1])
    s_own[:, :panel] = first
    s_own[:, panel:] = second.astype(BF16)

    def s_place(d):
        return s_all.at[own_rows(d // R, prows[d % R]), :]

    for d in [d for d in OTHERS if d % 2 == 0]:
        send(s_own, s_all.at[own_rows(mirror(d) // R, prow), :], sa_ssem.at[d], sa_rsem.at[mirror(d)], at(d))
    send(s_own, s_place(0), sa_ssem.at[1], sa_rsem.at[1], at(1))
    s_all[own_rows(0, prow), :] = s_own[...]
    for d in [d for d in OTHERS if d % 2 == 0]:
        arrived(s_place(d), sa_rsem.at[d])
        send(s_place(d), s_place(d), sa_ssem.at[d + 1], sa_rsem.at[d + 1], at(1))
    for d in range(1, GROUP, 2):
        arrived(s_place(d), sa_rsem.at[d])

    base = lax.rem(pcol, Q) * chunk
    width = chunk // 6

    @pl.loop(0, chunk // width)
    def _(j):
        there = pl.ds(pl.multiple_of(base + j * width, 128), width)
        here = pl.ds(pl.multiple_of(j * width, 128), width)
        change = jnp.dot(s_all[:, :panel], r_all[0, :, here], preferred_element_type=F32)
        change = change + jnp.dot(s_all[:, panel:], r_all[1, :, here], preferred_element_type=F32)
        v_all[:, here] = (v_all[:, here].astype(F32) - change).astype(BF16)
        for core in range(2):
            @pl.when(k == core)
            def _():
                for d in LEAVING[core]:
                    send(v_all.at[own_rows(d // R, prows[d % R]), here], out.at[prow, :, there], o_ssem.at[d],
                         o_rsem.at[mirror(d)], at(d))
        pltpu.make_async_copy(v_all.at[own_rows(0, prow), here], out.at[prow, :, there], o_own.at[0]).start()

    for slot in range(Q):
        if slot:
            arrived(piece(slot, 0), r_ssem.at[slot])
        for number in ((None,) if slot >= LATE else range(THIRDS) if slot else ()):
            arrived(v_landing(slot, number), v_ssem.at[v_sem(slot, number)])
        for dx in (1, 3):
            arrived(piece(slot, 0), x_ssem.at[dx * Q + slot])
        for number in range(2):
            arrived(piece(slot, 0, parts[number]), x_ssem.at[2 * number * Q + slot])
    piece_rows = out.at[0, :, pl.ds(0, chunk)]
    arrived(piece_rows, o_own.at[0])
    for d in OTHERS:
        arrived(g_own, gs_ssem.at[d])
        arrived(g_own, ga_ssem.at[d])
        arrived(p_recv.at[0], ps_ssem.at[d])
        arrived(s_own, sa_ssem.at[d])
        arrived(piece_rows, o_ssem.at[d])
    for d in OTHERS:
        across, far = at(d)
        there = pl.ds(pl.multiple_of(lax.rem(far, Q) * chunk, 128), chunk)
        arrived(out.at[across, :, there], o_rsem.at[d])


def joined(width, pieces, out, held, line, in_sem, out_sem):
    loads = [pltpu.make_async_copy(pieces.at[r], held.at[r], in_sem.at[r]) for r in range(R)]
    for load in loads:
        load.start()
    stores = []
    rows = held.shape[1]
    for r in range(R):
        loads[r].wait()
        first, shift = r * width // 128 * 128, r * width % 128
        end = (r + 1) * width // 128 * 128
        if shift == 0:
            source = held.at[r, :, pl.ds(0, end - first)]
        else:
            count = (end - first) // 128
            lane = lax.broadcasted_iota(jnp.int32, (rows, 128), 1)
            keep = held[r - 1, :, pl.ds(first - (r - 1) * width // 128 * 128, 128)].astype(F32)
            turned = pltpu.roll(held[r, :, :128].astype(F32), shift, 1)
            line[r // 2, :, :128] = jnp.where(lane < shift, keep, turned).astype(BF16)
            width_step = 13 * 128
            for a in range(128, count * 128, width_step):
                n = min(width_step, count * 128 - a)
                wide = held[r, :, a - 128:a + n].astype(F32)
                line[r // 2, :, a:a + n] = pltpu.roll(wide, shift, 1)[:, 128:].astype(BF16)
            source = line.at[r // 2]
        store = pltpu.make_async_copy(source, out.at[:, pl.ds(first, end - first)], out_sem.at[r])
        store.start()
        stores.append(store)
    for store in stores:
        store.wait()


def body(vectors, reflectors, panel_factor):
    rows, width = vectors.shape
    panel = panel_factor.shape[1]
    share = reflectors.shape[1]
    tiles = pl.cdiv(width, 128)
    chunk = pl.cdiv(tiles, Q) * 128
    whole = (tiles - 1) * 128
    dims = (rows, panel, whole, width - whole, chunk, chunk // 3)
    per = rows // R
    any_spec = pl.BlockSpec(memory_space=pl.ANY)
    dma = pltpu.SemaphoreType.DMA
    part = panel // GROUP
    gathered = pl.pallas_call(
        functools.partial(kernel, dims),
        grid=(1,),
        out_shape=jax.ShapeDtypeStruct((R, per, chunk * Q), BF16),
        in_specs=[
            any_spec, any_spec,
            pl.BlockSpec((rows, 128), lambda i: (0, tiles - 1)),
            pl.BlockSpec((2, share, 128), lambda i: (0, 0, tiles - 1)),
            pl.BlockSpec((2, panel, panel), lambda i: (0, 0, 0)),
        ],
        out_specs=any_spec,
        scratch_shapes=[
            pltpu.VMEM((rows, chunk * Q), BF16),
            pltpu.VMEM((2, share, chunk * Q), BF16),
            pltpu.VMEM((rows * Q, chunk), BF16),
            pltpu.VMEM((2, panel, chunk), BF16),
            pltpu.VMEM((rows * LATE, 2 * panel), F32),
            pltpu.VMEM((rows * Q, 2 * panel), BF16),
            pltpu.VMEM((GROUP, per, 2 * panel), BF16),
            pltpu.VMEM((GROUP, part, panel), BF16),
            pltpu.VMEM((GROUP, part, panel), BF16),
            pltpu.VMEM((part, panel), BF16),
            pltpu.VMEM((GROUP, part, panel), BF16),
            pltpu.VMEM((per, 2 * panel), BF16),
            pltpu.VMEM((rows * Q, 2 * panel), BF16),
            pltpu.VMEM((2, panel, panel), BF16),
            pltpu.VMEM((2, panel, panel), BF16),
            dma((2,)), dma((2,)), dma((Q,)), dma(((X + 1) * Q,)), dma((X * Q,)), dma((Q + LATE * THIRDS,)), dma((Q + LATE * THIRDS,)),
            dma((GROUP,)), dma((GROUP,)), dma((GROUP,)), dma((GROUP,)), dma((GROUP,)), dma((GROUP,)),
            dma((GROUP,)), dma((GROUP,)), dma((GROUP,)), dma((GROUP,)), dma((1,)),
        ],
        compiler_params=pltpu.CompilerParams(
            collective_id=0, has_side_effects=True, vmem_limit_bytes=61 * 1024 * 1024
        ),
        name="back_transform",
    )(vectors, reflectors, vectors, reflectors, panel_factor)
    line = R * width // 128 * 128 - (R - 1) * width // 128 * 128
    rows_out = pl.pallas_call(
        functools.partial(joined, width),
        out_shape=jax.ShapeDtypeStruct((per, R * width), BF16),
        in_specs=[any_spec],
        out_specs=any_spec,
        scratch_shapes=[
            pltpu.VMEM((R, per, chunk * Q), BF16), pltpu.VMEM((2, per, line), BF16), dma((R,)), dma((R,)),
        ],
        compiler_params=pltpu.CompilerParams(vmem_limit_bytes=61 * 1024 * 1024),
        name="joined",
    )(gathered)
    return rows_out[None]


def solution(mesh):
    placed = (P("pcol", "prow"), P(None, "pcol", "prow"), P())
    return jax.shard_map(
        body, mesh=mesh, in_specs=placed, out_specs=P("pcol", "prow", None), check_vma=False
    )
```

```python
import functools

import jax
import jax.numpy as jnp
from jax import lax
from jax.experimental import pallas as pl
from jax.experimental.pallas import tpu as pltpu
from jax.sharding import PartitionSpec as P

X, YL, Z, R = 4, 2, 4, 4
Q = YL * Z
GROUP = Q * R
ORDER = ((0, 0), (1, 0), (1, 1), (1, 3), (0, 2), (1, 2), (0, 1), (0, 3))
SLOT = {pair: number for number, pair in enumerate(ORDER)}
PAIRS = [(slot, flip) for slot in range(Q) for flip in range(2)]
PIECES, AHEAD = 5, (2, 3, 4, 5)
GOING = ((1, 2), (1, 0), (0, 2), (1, 1), (0, 3), (1, 3), (0, 1))


def hops(d):
    dy, dz = ORDER[d // R]
    return min(dz, Z - dz) + (1 if dy else d % R // 2 * 2)


OTHERS = sorted(range(1, GROUP), key=lambda d: -hops(d))

TURNS = (
    (
        ((0, 1, 2),),
        ((0, 1, 1), (0, 1, 3), (0, 0, 1), (0, 0, 3)),
        ((1, 0, 1), (1, 1, 3)),
        ((1, 0, 3), (1, 1, 1)),
        ((1, 0, 2), (1, 1, 2), (1, 0, 0), (1, 1, 0)),
        ((0, 1, 0), (0, 0, 2)),
    ),
    (
        ((1, 0, 0), (1, 1, 0), (1, 0, 2), (1, 1, 2)),
        ((1, 0, 1), (1, 1, 3)),
        ((1, 0, 3), (1, 1, 1)),
        ((0, 1, 2),),
        ((0, 1, 0), (0, 0, 2)),
        ((0, 1, 1), (0, 1, 3), (0, 0, 1), (0, 0, 3)),
    ),
)
LEAVING = [[(SLOT[lo, dz], hi) for turn in turns for lo, hi, dz in turn] for turns in TURNS]
FAR = sorted(PAIRS[1:], key=lambda pair: -hops(pair[0] * R + pair[1] * 2))
BF16, F32 = jnp.bfloat16, jnp.float32
NT = (((1,), (1,)), ((), ()))


def mirror(d):
    dy, dz = ORDER[d // R]
    return SLOT[dy, (4 - dz) % 4] * R + d % R


def halves(value):
    high = value.astype(BF16)
    return high, (value - high.astype(F32)).astype(BF16)


def times(value, high, low):
    a, b = halves(value)
    total = lax.dot_general(a, high, NT, preferred_element_type=F32)
    total = total + lax.dot_general(b, high, NT, preferred_element_type=F32)
    return total + lax.dot_general(a, low, NT, preferred_element_type=F32)


def kernel(
    dims,
    v_hbm, r_hbm, v_tail, r_tail, factor,
    out,
    v_loc, r_loc, v_all, r_all, p_sum, p_send, p_recv, g_send, g_recv, g_own, g_all, s_own, s_all, f_high, f_low,
    ld_sem, own_sem, r_ssem, r_rsem, x_ssem, v_ssem, v_rsem,
    gs_ssem, gs_rsem, ga_ssem, ga_rsem, ps_ssem, ps_rsem, sa_ssem, sa_rsem, o_ssem, o_rsem, o_own,
):
    rows, panel, whole, valid, chunk, step = dims
    per = rows // R
    share = panel // (X * Q)
    half = chunk // 2
    prow, pcol = lax.axis_index("prow"), lax.axis_index("pcol")
    x, yl, z = pcol // Q, lax.rem(pcol // Z, YL), lax.rem(pcol, Z)
    h, k = prow // 2, lax.rem(prow, 2)

    yls = [yl, 1 - yl]
    zs = [z] + [lax.rem(z + dz, Z) for dz in range(1, Z)]
    xs = [x] + [lax.rem(x + dx, X) for dx in range(1, X)]
    prows = [prow, h * 2 + 1 - k, (1 - h) * 2 + k, (1 - h) * 2 + 1 - k]

    def at(d, dx=0):
        dy, dz = ORDER[d // R]
        return prows[d % R], xs[dx] * Q + yls[dy] * Z + zs[dz]

    def send(src, dst, ssem, rsem, to):
        copy = pltpu.make_async_remote_copy(
            src_ref=src, dst_ref=dst, send_sem=ssem, recv_sem=rsem,
            device_id=to, device_id_type=pl.DeviceIdType.MESH,
        )
        copy.start()
        return copy

    def arrived(ref, sem):
        pltpu.make_async_copy(ref, ref, sem).wait()

    load_r = pltpu.make_async_copy(r_hbm.at[:, :, pl.ds(0, whole)], r_loc.at[:, :, pl.ds(0, whole)], ld_sem.at[0])
    load_v = [
        pltpu.make_async_copy(
            v_hbm.at[pl.ds(r * per, per), pl.ds(0, whole)], v_loc.at[r // 2, r % 2, :, pl.ds(0, whole)], ld_sem.at[1 + r])
        for r in (0, 2, 1, 3)
    ]
    load_r.start()
    for load in load_v:
        load.start()

    barrier = pltpu.get_barrier_semaphore()
    for d in OTHERS:
        pl.semaphore_signal(barrier, inc=1, device_id=at(d), device_id_type=pl.DeviceIdType.MESH)
    for dx in (1, 3):
        pl.semaphore_signal(barrier, inc=1, device_id=at(0, dx), device_id_type=pl.DeviceIdType.MESH)

    edge = v_loc.shape[3] - whole
    lane = lax.broadcasted_iota(jnp.int32, (rows, 128), 1)
    tail = jnp.where(lane < valid, v_tail[...].astype(F32), 0.0).astype(BF16)
    for r in range(R):
        v_loc[r // 2, r % 2, :, whole:] = jnp.zeros((per, edge), BF16)
        v_loc[r // 2, r % 2, :, whole:whole + 128] = tail[r * per:(r + 1) * per]
    lane8 = lax.broadcasted_iota(jnp.int32, (share, 128), 1)
    for p in range(2):
        r_loc[p, :, whole:] = jnp.zeros((share, edge), BF16)
        r_loc[p, :, whole:whole + 128] = jnp.where(lane8 < valid, r_tail[p].astype(F32), 0.0).astype(BF16)

    pl.semaphore_wait(barrier, GROUP - 1 + 2)

    mine = pl.ds(pl.multiple_of(pcol * share, share), share)

    def columns(slot):
        q = lax.rem(at(slot * R)[1], Q)
        return pl.ds(pl.multiple_of(q * chunk, 128), chunk)

    load_r.wait()
    own_r = pltpu.make_async_copy(r_loc.at[:, :, columns(0)], r_all.at[:, mine, :], own_sem.at[0])
    own_r.start()
    for slot in range(1, Q):
        d = mirror(slot * R)
        send(r_loc.at[:, :, columns(d // R)], r_all.at[:, mine, :], r_ssem.at[slot], r_rsem.at[slot], at(d))
    part_width = chunk // PIECES

    def v_sem(slot, number):
        return slot if number is None else Q + slot * PIECES + number

    def v_landing(slot, number=None):
        if number is None:
            return v_all.at[0, slot]
        return v_all.at[1, slot, :, :, pl.ds(number * part_width, part_width)]

    def v_source(slot, number):
        first = lax.rem(at(slot * R)[1], Q) * chunk + (number or 0) * part_width
        width = chunk if number is None else part_width
        return v_loc.at[:, 0 if number is None else 1, :, pl.ds(pl.multiple_of(first, 128), width)]

    def v_out(numbers):
        for number in numbers:
            for pair in GOING:
                d = SLOT[pair] * R
                slot = mirror(d) // R
                sem = v_sem(slot, number)
                send(v_source(d // R, number), v_landing(slot, number), v_ssem.at[sem], v_rsem.at[sem], at(d))

    load_v[0].wait()
    load_v[1].wait()
    v_out([None])
    own_first = pltpu.make_async_copy(v_source(0, None), v_landing(0), own_sem.at[1])
    own_first.start()
    load_v[2].wait()
    load_v[3].wait()
    v_out(range(AHEAD[0]))
    own_second = pltpu.make_async_copy(v_loc.at[:, 1, :, columns(0)], v_all.at[1, 0], own_sem.at[2])
    own_second.start()

    def piece(slot, dx, cols=None):
        source = pl.ds(pl.multiple_of(at(slot * R, dx)[1] * share, share), share)
        return r_all.at[:, source, :] if cols is None else r_all.at[:, source, cols]

    parts = (pl.ds(0, half), pl.ds(half, half))

    def spread(slot):
        if slot == 0:
            own_r.wait()
        else:
            arrived(piece(slot, 0), r_rsem.at[slot])
        for dx in (1, 3):
            send(piece(slot, 0), piece(slot, 0), x_ssem.at[dx * Q + slot], r_rsem.at[(4 - dx) * Q + slot], at(0, dx))

    def relay(slot):
        for number, dx in enumerate((1, 3)):
            arrived(piece(slot, dx), r_rsem.at[dx * Q + slot])
            part = piece(slot, dx, parts[number])
            send(part, part, x_ssem.at[2 * number * Q + slot], r_rsem.at[(2 + 2 * number) * Q + slot], at(0, 4 - dx))

    lag = 1
    for slot in range(Q + lag):
        if slot < Q:
            spread(slot)
        if slot >= lag:
            relay(slot - lag)

    f_high[...], f_low[...] = halves(factor[...])
    for slot in range(Q):
        for number in range(2):
            arrived(piece(slot, 2, parts[number]), r_rsem.at[(2 + 2 * number) * Q + slot])

    def summed(a, b, m):
        def one(j, total):
            cols = pl.ds(pl.multiple_of(j * step, 128), step)
            return total + lax.dot_general(a(cols), b(cols), NT, preferred_element_type=F32)
        return lax.fori_loop(0, chunk // step, one, jnp.zeros((m, panel), F32))

    part = panel // GROUP
    gram = summed(lambda cols: r_all[0, :, cols], lambda cols: r_all[1, :, cols], panel)
    g_send[...] = gram.reshape(GROUP, part, panel).astype(BF16)

    def owner(d):
        across, far = at(d)
        return lax.rem(far, Q) * R + across

    for d in OTHERS:
        send(g_send.at[owner(d)], g_recv.at[mirror(d)], gs_ssem.at[d], gs_rsem.at[mirror(d)], at(d))
    v_out(range(AHEAD[0], AHEAD[1]))

    sides = (h, 1 - h)

    def place(slot, flip, core):
        return sides[flip] * 2 + core, at(slot * R)[1]

    def turned(slot):
        return mirror(slot * R) // R

    def tall(ref):
        value = ref[...]
        return value.reshape(2 * Q * per, value.shape[-1])

    def p_out(core):
        for slot, flip in FAR:
            send(p_send.at[core, slot, sides[flip]], p_recv.at[(turned(slot) * 2 + flip) * 2 + k],
                 ps_ssem.at[(slot * 2 + flip) * 2 + core], ps_rsem.at[(turned(slot) * 2 + flip) * 2 + k], place(slot, flip, core))

        @pl.when(k != core)
        def _():
            send(p_send.at[core, 0, h], p_recv.at[k], ps_ssem.at[core], ps_rsem.at[k], place(0, 0, core))

        @pl.when(k == core)
        def _():
            p_recv[k] = p_send[core, 0, h]

    for slot in range(1, Q):
        arrived(v_landing(slot), v_rsem.at[slot])
    own_first.wait()
    for p in range(2):
        total = summed(lambda cols: tall(v_all.at[0, :, :, :, cols]), lambda cols: r_all[p, :, cols], 2 * Q * per)
        p_send[0, :, :, :, p * panel:(p + 1) * panel] = total.astype(BF16).reshape(Q, 2, per, panel)
    p_out(0)
    v_out(range(AHEAD[1], AHEAD[2]))

    for d in OTHERS:
        arrived(g_recv.at[d], gs_rsem.at[d])
    g_own[...] = (jnp.sum(g_recv[1:].astype(F32), axis=0) + g_send[owner(0)].astype(F32)).astype(BF16)
    for d in OTHERS:
        send(g_own, g_all.at[owner(0)], ga_ssem.at[d], ga_rsem.at[mirror(d)], at(d))
    g_all[owner(0)] = g_own[...]
    v_out(range(AHEAD[2], AHEAD[3]))

    def second_half(numbers):
        for number in numbers:
            for slot in range(1, Q):
                arrived(v_landing(slot, number), v_rsem.at[v_sem(slot, number)])
            cols = pl.ds(number * part_width, part_width)
            for p in range(2):
                here = slice(p * panel, (p + 1) * panel)
                total = lax.dot_general(
                    tall(v_all.at[1, :, :, :, cols]), r_all[p, :, cols], NT, preferred_element_type=F32)
                if number:
                    total = total + p_sum[:, here]
                if number < PIECES - 1:
                    p_sum[:, here] = total
                else:
                    p_send[1, :, :, :, here] = total.astype(BF16).reshape(Q, 2, per, panel)

    own_second.wait()
    second_half(range(AHEAD[1]))

    def s_place(core, slot, flip):
        return s_all.at[core, slot, sides[flip]]

    def s_out(core):
        @pl.when(k == core)
        def _():
            for slot, flip in FAR:
                for sender in range(2):
                    spot = (slot * 2 + flip) * 2 + sender
                    arrived(p_recv.at[spot], ps_rsem.at[spot])
            arrived(p_recv.at[1 - k], ps_rsem.at[1 - k])
            product = jnp.sum(p_recv[...].astype(F32), axis=0)
            first = times(product[:, :panel], f_high[0], f_low[0]).astype(BF16)
            second = times(product[:, panel:], f_high[1], f_low[1])
            for d in OTHERS:
                arrived(g_all.at[owner(d)], ga_rsem.at[d])
            gram = g_all[...].reshape(panel, panel)
            second = second - times(jnp.dot(first, gram, preferred_element_type=F32), f_high[1], f_low[1])
            s_own[:, :panel] = first
            s_own[:, panel:] = second.astype(BF16)
            for slot, flip in FAR:
                spot = (turned(slot) * 2 + flip) * 2 + core
                send(s_own, s_all.at[core, turned(slot), h], sa_ssem.at[(slot * 2 + flip) * 2], sa_rsem.at[spot],
                     place(slot, flip, core))
            send(s_own, s_place(core, 0, 0), sa_ssem.at[1], sa_rsem.at[core], place(0, 0, 1 - core))
            s_all[core, 0, h] = s_own[...]

    def s_shared(core):
        @pl.when(k == core)
        def _():
            for slot, flip in FAR:
                spot = (slot * 2 + flip) * 2 + core
                arrived(s_place(core, slot, flip), sa_rsem.at[spot])
                send(s_place(core, slot, flip), s_place(core, slot, flip), sa_ssem.at[(slot * 2 + flip) * 2 + 1],
                     sa_rsem.at[spot], place(0, 0, 1 - core))

        @pl.when(k != core)
        def _():
            for slot, flip in FAR + [(0, 0)]:
                arrived(s_place(core, slot, flip), sa_rsem.at[(slot * 2 + flip) * 2 + core])

    base = lax.rem(pcol, Q) * chunk
    width = chunk // 6

    def results(core, first, count):
        @pl.loop(first, first + count)
        def _(j):
            there = pl.ds(pl.multiple_of(base + j * width, 128), width)
            here = pl.ds(pl.multiple_of(j * width, 128), width)
            change = jnp.dot(tall(s_all.at[core, :, :, :, pl.ds(0, panel)]), r_all[0, :, here], preferred_element_type=F32)
            change = change + jnp.dot(
                tall(s_all.at[core, :, :, :, pl.ds(panel, panel)]), r_all[1, :, here], preferred_element_type=F32)
            fresh = (tall(v_all.at[core, :, :, :, here]).astype(F32) - change).astype(BF16)
            v_all[core, :, :, :, here] = fresh.reshape(Q, 2, per, width)
            for sender in range(2):
                @pl.when(k == sender)
                def _():
                    for slot, flip in LEAVING[sender]:
                        send(v_all.at[core, slot, sides[flip], :, here], out.at[prow, :, there],
                             o_ssem.at[(slot * 2 + flip) * 2 + core],
                             o_rsem.at[(turned(slot) * 2 + flip) * 2 + sender], place(slot, flip, core))
                    if sender == core:
                        pltpu.make_async_copy(
                            v_all.at[core, 0, h, :, here], out.at[prow, :, there], o_own.at[0]).start()
                    else:
                        send(v_all.at[core, 0, h, :, here], out.at[prow, :, there], o_ssem.at[core],
                             o_rsem.at[sender], place(0, 0, core))

    s_out(0)
    second_half(range(AHEAD[1], PIECES))
    p_out(1)
    s_shared(0)
    results(0, 0, 3)
    s_out(1)
    results(0, 3, 3)
    s_shared(1)
    results(1, 0, 6)

    for slot in range(Q):
        if slot:
            arrived(piece(slot, 0), r_ssem.at[slot])
        for number in (None, *range(PIECES)) if slot else ():
            arrived(v_landing(slot, number), v_ssem.at[v_sem(slot, number)])
        for dx in (1, 3):
            arrived(piece(slot, 0), x_ssem.at[dx * Q + slot])
        for number in range(2):
            arrived(piece(slot, 0, parts[number]), x_ssem.at[2 * number * Q + slot])
    piece_rows = out.at[0, :, pl.ds(0, chunk)]
    arrived(piece_rows, o_own.at[0])
    for d in OTHERS:
        arrived(g_own, gs_ssem.at[d])
        arrived(g_own, ga_ssem.at[d])
        arrived(s_own, sa_ssem.at[d])

    def ended(spot):
        arrived(s_own, ps_ssem.at[spot])
        arrived(piece_rows, o_ssem.at[spot])

    def landed(slot, flip, core):
        across, far = place(slot, flip, core)
        there = pl.ds(pl.multiple_of(lax.rem(far, Q) * chunk, 128), chunk)
        arrived(out.at[across, :, there], o_rsem.at[(slot * 2 + flip) * 2 + core])

    ended(1 - k)
    landed(0, 0, 1 - k)
    for slot, flip in FAR:
        for core in range(2):
            ended((slot * 2 + flip) * 2 + core)
            landed(slot, flip, core)


def joined(width, pieces, out, held, line, in_sem, out_sem):
    loads = [pltpu.make_async_copy(pieces.at[r], held.at[r], in_sem.at[r]) for r in range(R)]
    for load in loads:
        load.start()
    stores = []
    rows = held.shape[1]
    for r in range(R):
        loads[r].wait()
        first, shift = r * width // 128 * 128, r * width % 128
        end = (r + 1) * width // 128 * 128
        if shift == 0:
            source = held.at[r, :, pl.ds(0, end - first)]
        else:
            count = (end - first) // 128
            lane = lax.broadcasted_iota(jnp.int32, (rows, 128), 1)
            keep = held[r - 1, :, pl.ds(first - (r - 1) * width // 128 * 128, 128)].astype(F32)
            turned = pltpu.roll(held[r, :, :128].astype(F32), shift, 1)
            line[r // 2, :, :128] = jnp.where(lane < shift, keep, turned).astype(BF16)
            width_step = 13 * 128
            for a in range(128, count * 128, width_step):
                n = min(width_step, count * 128 - a)
                wide = held[r, :, a - 128:a + n].astype(F32)
                line[r // 2, :, a:a + n] = pltpu.roll(wide, shift, 1)[:, 128:].astype(BF16)
            source = line.at[r // 2]
        store = pltpu.make_async_copy(source, out.at[:, pl.ds(first, end - first)], out_sem.at[r])
        store.start()
        stores.append(store)
    for store in stores:
        store.wait()


def body(vectors, reflectors, panel_factor):
    rows, width = vectors.shape
    panel = panel_factor.shape[1]
    share = reflectors.shape[1]
    tiles = pl.cdiv(width, 128)
    chunk = pl.cdiv(tiles, Q) * 128
    whole = (tiles - 1) * 128
    dims = (rows, panel, whole, width - whole, chunk, chunk // 3)
    per = rows // R
    any_spec = pl.BlockSpec(memory_space=pl.ANY)
    dma = pltpu.SemaphoreType.DMA
    part = panel // GROUP
    gathered = pl.pallas_call(
        functools.partial(kernel, dims),
        grid=(1,),
        out_shape=jax.ShapeDtypeStruct((R, per, chunk * Q), BF16),
        in_specs=[
            any_spec, any_spec,
            pl.BlockSpec((rows, 128), lambda i: (0, tiles - 1)),
            pl.BlockSpec((2, share, 128), lambda i: (0, 0, tiles - 1)),
            pl.BlockSpec((2, panel, panel), lambda i: (0, 0, 0)),
        ],
        out_specs=any_spec,
        scratch_shapes=[
            pltpu.VMEM((2, 2, per, chunk * Q), BF16),
            pltpu.VMEM((2, share, chunk * Q), BF16),
            pltpu.VMEM((2, Q, 2, per, chunk), BF16),
            pltpu.VMEM((2, panel, chunk), BF16),
            pltpu.VMEM((rows * Q // 2, 2 * panel), F32),
            pltpu.VMEM((2, Q, 2, per, 2 * panel), BF16),
            pltpu.VMEM((GROUP, per, 2 * panel), BF16),
            pltpu.VMEM((GROUP, part, panel), BF16),
            pltpu.VMEM((GROUP, part, panel), BF16),
            pltpu.VMEM((part, panel), BF16),
            pltpu.VMEM((GROUP, part, panel), BF16),
            pltpu.VMEM((per, 2 * panel), BF16),
            pltpu.VMEM((2, Q, 2, per, 2 * panel), BF16),
            pltpu.VMEM((2, panel, panel), BF16),
            pltpu.VMEM((2, panel, panel), BF16),
            dma((1 + R,)), dma((3,)), dma((Q,)), dma(((X + 1) * Q,)), dma((X * Q,)), dma((Q + Q * PIECES,)), dma((Q + Q * PIECES,)),
            dma((GROUP,)), dma((GROUP,)), dma((GROUP,)), dma((GROUP,)), dma((GROUP,)), dma((GROUP,)),
            dma((GROUP,)), dma((GROUP,)), dma((GROUP,)), dma((GROUP,)), dma((1,)),
        ],
        compiler_params=pltpu.CompilerParams(
            collective_id=0, has_side_effects=True, vmem_limit_bytes=61 * 1024 * 1024
        ),
        name="back_transform",
    )(vectors, reflectors, vectors, reflectors, panel_factor)
    line = R * width // 128 * 128 - (R - 1) * width // 128 * 128
    rows_out = pl.pallas_call(
        functools.partial(joined, width),
        out_shape=jax.ShapeDtypeStruct((per, R * width), BF16),
        in_specs=[any_spec],
        out_specs=any_spec,
        scratch_shapes=[
            pltpu.VMEM((R, per, chunk * Q), BF16), pltpu.VMEM((2, per, line), BF16), dma((R,)), dma((R,)),
        ],
        compiler_params=pltpu.CompilerParams(vmem_limit_bytes=61 * 1024 * 1024),
        name="joined",
    )(gathered)
    return rows_out[None]


def solution(mesh):
    placed = (P("pcol", "prow"), P(None, "pcol", "prow"), P())
    return jax.shard_map(
        body, mesh=mesh, in_specs=placed, out_specs=P("pcol", "prow", None), check_vma=False
    )
```

```python
import functools

import jax
import jax.numpy as jnp
from jax import lax
from jax.experimental import pallas as pl
from jax.experimental.pallas import tpu as pltpu
from jax.sharding import PartitionSpec as P

X, YL, Z, R = 4, 2, 4, 4
Q = YL * Z
GROUP = Q * R
ORDER = ((0, 0), (1, 0), (1, 1), (1, 3), (0, 2), (1, 2), (0, 1), (0, 3))
SLOT = {pair: number for number, pair in enumerate(ORDER)}
PAIRS = [(slot, flip) for slot in range(Q) for flip in range(2)]
PIECES, AHEAD = 5, (2, 2, 3, 5)
GOING = ((1, 2), (1, 0), (0, 2), (1, 1), (0, 3), (1, 3), (0, 1))


def hops(d):
    dy, dz = ORDER[d // R]
    return min(dz, Z - dz) + (1 if dy else d % R // 2 * 2)


OTHERS = sorted(range(1, GROUP), key=lambda d: -hops(d))

FAR = sorted(PAIRS[1:], key=lambda pair: -hops(pair[0] * R + pair[1] * 2))
BF16, F32 = jnp.bfloat16, jnp.float32
NT = (((1,), (1,)), ((), ()))


def mirror(d):
    dy, dz = ORDER[d // R]
    return SLOT[dy, (4 - dz) % 4] * R + d % R


def halves(value):
    high = value.astype(BF16)
    return high, (value - high.astype(F32)).astype(BF16)


def times(value, high, low):
    a, b = halves(value)
    total = lax.dot_general(a, high, NT, preferred_element_type=F32)
    total = total + lax.dot_general(b, high, NT, preferred_element_type=F32)
    return total + lax.dot_general(a, low, NT, preferred_element_type=F32)


def kernel(
    dims,
    v_hbm, r_hbm, f_hbm,
    out,
    v_loc, r_loc, v_all, r_all, p_sum, p_send, p_recv, g_send, g_recv, g_own, g_all, s_own, s_all, v_tail, r_tail, factor, f_high, f_low,
    ld_sem, own_sem, r_ssem, r_rsem, x_ssem, v_ssem, v_rsem,
    gs_ssem, gs_rsem, ga_ssem, ga_rsem, ps_ssem, ps_rsem, sa_ssem, sa_rsem, o_ssem, o_rsem, o_own,
):
    rows, panel, whole, valid, chunk, step = dims
    per = rows // R
    share = panel // (X * Q)
    half = chunk // 2
    prow, pcol = lax.axis_index("prow"), lax.axis_index("pcol")
    x, yl, z = pcol // Q, lax.rem(pcol // Z, YL), lax.rem(pcol, Z)
    h, k = prow // 2, lax.rem(prow, 2)

    yls = [yl, 1 - yl]
    zs = [z] + [lax.rem(z + dz, Z) for dz in range(1, Z)]
    xs = [x] + [lax.rem(x + dx, X) for dx in range(1, X)]
    prows = [prow, h * 2 + 1 - k, (1 - h) * 2 + k, (1 - h) * 2 + 1 - k]

    def at(d, dx=0):
        dy, dz = ORDER[d // R]
        return prows[d % R], xs[dx] * Q + yls[dy] * Z + zs[dz]

    def send(src, dst, ssem, rsem, to):
        copy = pltpu.make_async_remote_copy(
            src_ref=src, dst_ref=dst, send_sem=ssem, recv_sem=rsem,
            device_id=to, device_id_type=pl.DeviceIdType.MESH,
        )
        copy.start()
        return copy

    def arrived(ref, sem):
        pltpu.make_async_copy(ref, ref, sem).wait()

    barrier = pltpu.get_barrier_semaphore()
    for d in OTHERS:
        pl.semaphore_signal(barrier, inc=1, device_id=at(d), device_id_type=pl.DeviceIdType.MESH)
    for dx in (1, 3):
        pl.semaphore_signal(barrier, inc=1, device_id=at(0, dx), device_id_type=pl.DeviceIdType.MESH)

    load_r = pltpu.make_async_copy(r_hbm.at[:, :, pl.ds(0, whole)], r_loc.at[:, :, pl.ds(0, whole)], ld_sem.at[0])
    load_v = [
        pltpu.make_async_copy(
            v_hbm.at[pl.ds(r * per, per), pl.ds(0, whole)], v_loc.at[r // 2, r % 2, :, pl.ds(0, whole)], ld_sem.at[1 + r])
        for r in (0, 2, 1, 3)
    ]
    load_r.start()
    for load in load_v:
        load.start()
    load_f = pltpu.make_async_copy(f_hbm, factor, ld_sem.at[1 + R])
    load_f.start()
    tails = [
        pltpu.make_async_copy(v_hbm.at[:, pl.ds(whole, valid)], v_tail, ld_sem.at[2 + R]),
        pltpu.make_async_copy(r_hbm.at[:, :, pl.ds(whole, valid)], r_tail, ld_sem.at[3 + R]),
    ]
    for load in tails:
        load.start()

    edge = v_loc.shape[3] - whole
    for load in tails:
        load.wait()
    for r in range(R):
        v_loc[r // 2, r % 2, :, whole:] = jnp.zeros((per, edge), BF16)
        v_loc[r // 2, r % 2, :, whole:whole + valid] = v_tail[r * per:(r + 1) * per, :]
    for p in range(2):
        r_loc[p, :, whole:] = jnp.zeros((share, edge), BF16)
        r_loc[p, :, whole:whole + valid] = r_tail[p]

    pl.semaphore_wait(barrier, GROUP - 1 + 2)

    mine = pl.ds(pl.multiple_of(pcol * share, share), share)

    def columns(slot):
        q = lax.rem(at(slot * R)[1], Q)
        return pl.ds(pl.multiple_of(q * chunk, 128), chunk)

    load_r.wait()
    own_r = pltpu.make_async_copy(r_loc.at[:, :, columns(0)], r_all.at[:, mine, :], own_sem.at[0])
    own_r.start()
    for slot in range(1, Q):
        d = mirror(slot * R)
        send(r_loc.at[:, :, columns(d // R)], r_all.at[:, mine, :], r_ssem.at[slot], r_rsem.at[slot], at(d))
    part_width = chunk // PIECES

    def v_sem(slot, number):
        return slot if number is None else Q + slot * PIECES + number

    def v_landing(slot, number=None):
        if number is None:
            return v_all.at[0, slot]
        return v_all.at[1, slot, :, :, pl.ds(number * part_width, part_width)]

    def v_source(slot, number):
        first = lax.rem(at(slot * R)[1], Q) * chunk + (number or 0) * part_width
        width = chunk if number is None else part_width
        return v_loc.at[:, 0 if number is None else 1, :, pl.ds(pl.multiple_of(first, 128), width)]

    def v_out(numbers):
        for number in numbers:
            for pair in GOING:
                d = SLOT[pair] * R
                slot = mirror(d) // R
                sem = v_sem(slot, number)
                send(v_source(d // R, number), v_landing(slot, number), v_ssem.at[sem], v_rsem.at[sem], at(d))

    load_v[0].wait()
    load_v[1].wait()
    v_out([None])
    own_first = pltpu.make_async_copy(v_source(0, None), v_landing(0), own_sem.at[1])
    own_first.start()
    load_v[2].wait()
    load_v[3].wait()
    v_out(range(AHEAD[0]))
    own_second = pltpu.make_async_copy(v_loc.at[:, 1, :, columns(0)], v_all.at[1, 0], own_sem.at[2])
    own_second.start()

    def piece(slot, dx, cols=None):
        source = pl.ds(pl.multiple_of(at(slot * R, dx)[1] * share, share), share)
        return r_all.at[:, source, :] if cols is None else r_all.at[:, source, cols]

    parts = (pl.ds(0, half), pl.ds(half, half))

    def spread(slot):
        if slot == 0:
            own_r.wait()
        else:
            arrived(piece(slot, 0), r_rsem.at[slot])
        for dx in (1, 3):
            send(piece(slot, 0), piece(slot, 0), x_ssem.at[dx * Q + slot], r_rsem.at[(4 - dx) * Q + slot], at(0, dx))

    def relay(slot):
        for number, dx in enumerate((1, 3)):
            arrived(piece(slot, dx), r_rsem.at[dx * Q + slot])
            part = piece(slot, dx, parts[number])
            send(part, part, x_ssem.at[2 * number * Q + slot], r_rsem.at[(2 + 2 * number) * Q + slot], at(0, 4 - dx))

    lag = 1
    for slot in range(Q + lag):
        if slot < Q:
            spread(slot)
        if slot >= lag:
            relay(slot - lag)

    load_f.wait()
    f_high[...], f_low[...] = halves(factor[...])
    for slot in range(Q):
        for number in range(2):
            arrived(piece(slot, 2, parts[number]), r_rsem.at[(2 + 2 * number) * Q + slot])

    def summed(a, b, m):
        def one(j, total):
            cols = pl.ds(pl.multiple_of(j * step, 128), step)
            return total + lax.dot_general(a(cols), b(cols), NT, preferred_element_type=F32)
        return lax.fori_loop(0, chunk // step, one, jnp.zeros((m, panel), F32))

    part = panel // GROUP
    gram = summed(lambda cols: r_all[0, :, cols], lambda cols: r_all[1, :, cols], panel)
    g_send[...] = gram.reshape(GROUP, part, panel).astype(BF16)

    def owner(d):
        across, far = at(d)
        return lax.rem(far, Q) * R + across

    for d in OTHERS:
        send(g_send.at[owner(d)], g_recv.at[mirror(d)], gs_ssem.at[d], gs_rsem.at[mirror(d)], at(d))
    v_out(range(AHEAD[0], AHEAD[1]))

    sides = (h, 1 - h)

    def place(slot, flip, core):
        return sides[flip] * 2 + core, at(slot * R)[1]

    def turned(slot):
        return mirror(slot * R) // R

    def tall(ref):
        value = ref[...]
        return value.reshape(2 * Q * per, value.shape[-1])

    def p_out(core):
        for slot, flip in FAR:
            send(p_send.at[core, slot, sides[flip]], p_recv.at[(turned(slot) * 2 + flip) * 2 + k],
                 ps_ssem.at[(slot * 2 + flip) * 2 + core], ps_rsem.at[(turned(slot) * 2 + flip) * 2 + k], place(slot, flip, core))

        @pl.when(k != core)
        def _():
            send(p_send.at[core, 0, h], p_recv.at[k], ps_ssem.at[core], ps_rsem.at[k], place(0, 0, core))

        @pl.when(k == core)
        def _():
            p_recv[k] = p_send[core, 0, h]

    for slot in range(1, Q):
        arrived(v_landing(slot), v_rsem.at[slot])
    own_first.wait()
    for p in range(2):
        total = summed(lambda cols: tall(v_all.at[0, :, :, :, cols]), lambda cols: r_all[p, :, cols], 2 * Q * per)
        p_send[0, :, :, :, p * panel:(p + 1) * panel] = total.astype(BF16).reshape(Q, 2, per, panel)
    p_out(0)
    v_out(range(AHEAD[1], AHEAD[2]))

    for d in OTHERS:
        arrived(g_recv.at[d], gs_rsem.at[d])
    g_own[...] = (jnp.sum(g_recv[1:].astype(F32), axis=0) + g_send[owner(0)].astype(F32)).astype(BF16)
    for d in OTHERS:
        send(g_own, g_all.at[owner(0)], ga_ssem.at[d], ga_rsem.at[mirror(d)], at(d))
    g_all[owner(0)] = g_own[...]
    v_out(range(AHEAD[2], AHEAD[3]))

    def second_half(numbers):
        for number in numbers:
            for slot in range(1, Q):
                arrived(v_landing(slot, number), v_rsem.at[v_sem(slot, number)])
            cols = pl.ds(number * part_width, part_width)
            for p in range(2):
                here = slice(p * panel, (p + 1) * panel)
                total = lax.dot_general(
                    tall(v_all.at[1, :, :, :, cols]), r_all[p, :, cols], NT, preferred_element_type=F32)
                if number:
                    total = total + p_sum[:, here]
                if number < PIECES - 1:
                    p_sum[:, here] = total
                else:
                    p_send[1, :, :, :, here] = total.astype(BF16).reshape(Q, 2, per, panel)

    own_second.wait()
    second_half(range(AHEAD[1]))

    def s_place(core, slot, flip):
        return s_all.at[core, slot, sides[flip]]

    def s_out(core):
        @pl.when(k == core)
        def _():
            for slot, flip in FAR:
                for sender in range(2):
                    spot = (slot * 2 + flip) * 2 + sender
                    arrived(p_recv.at[spot], ps_rsem.at[spot])
            arrived(p_recv.at[1 - k], ps_rsem.at[1 - k])
            product = jnp.sum(p_recv[...].astype(F32), axis=0)
            first = times(product[:, :panel], f_high[0], f_low[0]).astype(BF16)
            second = times(product[:, panel:], f_high[1], f_low[1])
            for d in OTHERS:
                arrived(g_all.at[owner(d)], ga_rsem.at[d])
            gram = g_all[...].reshape(panel, panel)
            second = second - times(jnp.dot(first, gram, preferred_element_type=F32), f_high[1], f_low[1])
            s_own[:, :panel] = first
            s_own[:, panel:] = second.astype(BF16)
            for slot, flip in FAR:
                spot = (turned(slot) * 2 + flip) * 2 + core
                send(s_own, s_all.at[core, turned(slot), h], sa_ssem.at[(slot * 2 + flip) * 2], sa_rsem.at[spot],
                     place(slot, flip, core))
            send(s_own, s_place(core, 0, 0), sa_ssem.at[1], sa_rsem.at[core], place(0, 0, 1 - core))
            s_all[core, 0, h] = s_own[...]

    def s_shared(core):
        @pl.when(k == core)
        def _():
            for slot, flip in FAR:
                spot = (slot * 2 + flip) * 2 + core
                arrived(s_place(core, slot, flip), sa_rsem.at[spot])
                send(s_place(core, slot, flip), s_place(core, slot, flip), sa_ssem.at[(slot * 2 + flip) * 2 + 1],
                     sa_rsem.at[spot], place(0, 0, 1 - core))

        @pl.when(k != core)
        def _():
            for slot, flip in FAR + [(0, 0)]:
                arrived(s_place(core, slot, flip), sa_rsem.at[(slot * 2 + flip) * 2 + core])

    base = lax.rem(pcol, Q) * chunk
    width = chunk // 6

    def results(core, first, count):
        @pl.loop(first, first + count)
        def _(j):
            there = pl.ds(pl.multiple_of(base + j * width, 128), width)
            here = pl.ds(pl.multiple_of(j * width, 128), width)
            change = jnp.dot(tall(s_all.at[core, :, :, :, pl.ds(0, panel)]), r_all[0, :, here], preferred_element_type=F32)
            change = change + jnp.dot(
                tall(s_all.at[core, :, :, :, pl.ds(panel, panel)]), r_all[1, :, here], preferred_element_type=F32)
            fresh = (tall(v_all.at[core, :, :, :, here]).astype(F32) - change).astype(BF16)
            v_all[core, :, :, :, here] = fresh.reshape(Q, 2, per, width)
            for slot, flip in FAR:
                send(v_all.at[core, slot, sides[flip], :, here], out.at[prow, :, there],
                     o_ssem.at[(slot * 2 + flip) * 2 + core], o_rsem.at[(turned(slot) * 2 + flip) * 2 + k],
                     place(slot, flip, core))

            @pl.when(k == core)
            def _():
                pltpu.make_async_copy(v_all.at[core, 0, h, :, here], out.at[prow, :, there], o_own.at[0]).start()

            @pl.when(k != core)
            def _():
                send(v_all.at[core, 0, h, :, here], out.at[prow, :, there], o_ssem.at[core], o_rsem.at[k],
                     place(0, 0, core))

    s_out(0)
    second_half(range(AHEAD[1], PIECES))
    p_out(1)
    s_shared(0)
    results(0, 0, 3)
    s_out(1)
    results(0, 3, 3)
    s_shared(1)
    results(1, 0, 6)

    for slot in range(Q):
        if slot:
            arrived(piece(slot, 0), r_ssem.at[slot])
        for number in (None, *range(PIECES)) if slot else ():
            arrived(v_landing(slot, number), v_ssem.at[v_sem(slot, number)])
        for dx in (1, 3):
            arrived(piece(slot, 0), x_ssem.at[dx * Q + slot])
        for number in range(2):
            arrived(piece(slot, 0, parts[number]), x_ssem.at[2 * number * Q + slot])
    piece_rows = out.at[0, :, pl.ds(0, chunk)]
    arrived(piece_rows, o_own.at[0])
    for d in OTHERS:
        arrived(g_own, gs_ssem.at[d])
        arrived(g_own, ga_ssem.at[d])
        arrived(s_own, sa_ssem.at[d])

    def ended(spot):
        arrived(s_own, ps_ssem.at[spot])
        arrived(piece_rows, o_ssem.at[spot])

    def landed(slot, flip, core):
        across, far = place(slot, flip, core)
        there = pl.ds(pl.multiple_of(lax.rem(far, Q) * chunk, 128), chunk)
        arrived(out.at[across, :, there], o_rsem.at[(slot * 2 + flip) * 2 + core])

    ended(1 - k)
    landed(0, 0, 1 - k)
    for slot, flip in FAR:
        for core in range(2):
            ended((slot * 2 + flip) * 2 + core)
            landed(slot, flip, core)


def joined(width, held, out, line, out_sem):
    stores = []
    rows = held.shape[1]
    for r in sorted(range(R), key=lambda r: r * width % 128):
        first, shift = r * width // 128 * 128, r * width % 128
        end = (r + 1) * width // 128 * 128
        if shift == 0:
            source = held.at[r, :, pl.ds(0, end - first)]
        else:
            count = (end - first) // 128
            lane = lax.broadcasted_iota(jnp.int32, (rows, 128), 1)
            keep = held[r - 1, :, pl.ds(first - (r - 1) * width // 128 * 128, 128)].astype(F32)
            turned = pltpu.roll(held[r, :, :128].astype(F32), shift, 1)
            line[r // 2, :, :128] = jnp.where(lane < shift, keep, turned).astype(BF16)
            width_step = 13 * 128
            for a in range(128, count * 128, width_step):
                n = min(width_step, count * 128 - a)
                wide = held[r, :, a - 128:a + n].astype(F32)
                line[r // 2, :, a:a + n] = pltpu.roll(wide, shift, 1)[:, 128:].astype(BF16)
            source = line.at[r // 2]
        store = pltpu.make_async_copy(source, out.at[:, pl.ds(first, end - first)], out_sem.at[r])
        store.start()
        stores.append(store)
    for store in stores:
        store.wait()


def body(vectors, reflectors, panel_factor):
    rows, width = vectors.shape
    panel = panel_factor.shape[1]
    share = reflectors.shape[1]
    tiles = pl.cdiv(width, 128)
    chunk = pl.cdiv(tiles, Q) * 128
    whole = (tiles - 1) * 128
    dims = (rows, panel, whole, width - whole, chunk, chunk // 3)
    per = rows // R
    any_spec = pl.BlockSpec(memory_space=pl.ANY)
    dma = pltpu.SemaphoreType.DMA
    part = panel // GROUP
    gathered = pl.pallas_call(
        functools.partial(kernel, dims),
        out_shape=pltpu.VMEM((R, per, chunk * Q), BF16),
        in_specs=[
            any_spec, any_spec,
            any_spec,
        ],
        out_specs=pl.BlockSpec(memory_space=pltpu.VMEM),
        scratch_shapes=[
            pltpu.VMEM((2, 2, per, chunk * Q), BF16),
            pltpu.VMEM((2, share, chunk * Q), BF16),
            pltpu.VMEM((2, Q, 2, per, chunk), BF16),
            pltpu.VMEM((2, panel, chunk), BF16),
            pltpu.VMEM((rows * Q // 2, 2 * panel), F32),
            pltpu.VMEM((2, Q, 2, per, 2 * panel), BF16),
            pltpu.VMEM((GROUP, per, 2 * panel), BF16),
            pltpu.VMEM((GROUP, part, panel), BF16),
            pltpu.VMEM((GROUP, part, panel), BF16),
            pltpu.VMEM((part, panel), BF16),
            pltpu.VMEM((GROUP, part, panel), BF16),
            pltpu.VMEM((per, 2 * panel), BF16),
            pltpu.VMEM((2, Q, 2, per, 2 * panel), BF16),
            pltpu.VMEM((rows, width - whole), BF16),
            pltpu.VMEM((2, share, width - whole), BF16),
            pltpu.VMEM((2, panel, panel), F32),
            pltpu.VMEM((2, panel, panel), BF16),
            pltpu.VMEM((2, panel, panel), BF16),
            dma((4 + R,)), dma((3,)), dma((Q,)), dma(((X + 1) * Q,)), dma((X * Q,)), dma((Q + Q * PIECES,)), dma((Q + Q * PIECES,)),
            dma((GROUP,)), dma((GROUP,)), dma((GROUP,)), dma((GROUP,)), dma((GROUP,)), dma((GROUP,)),
            dma((GROUP,)), dma((GROUP,)), dma((GROUP,)), dma((GROUP,)), dma((1,)),
        ],
        compiler_params=pltpu.CompilerParams(
            collective_id=0, has_side_effects=True, vmem_limit_bytes=62700000
        ),
        name="back_transform",
    )(vectors, reflectors, panel_factor)
    line = R * width // 128 * 128 - (R - 1) * width // 128 * 128
    rows_out = pl.pallas_call(
        functools.partial(joined, width),
        out_shape=jax.ShapeDtypeStruct((per, R * width), BF16),
        in_specs=[pl.BlockSpec(memory_space=pltpu.VMEM)],
        out_specs=any_spec,
        scratch_shapes=[pltpu.VMEM((2, per, line), BF16), dma((R,))],
        compiler_params=pltpu.CompilerParams(vmem_limit_bytes=16 * 1024 * 1024),
        name="joined",
    )(gathered)
    return rows_out[None]


def solution(mesh):
    placed = (P("pcol", "prow"), P(None, "pcol", "prow"), P())
    return jax.shard_map(
        body, mesh=mesh, in_specs=placed, out_specs=P("pcol", "prow", None), check_vma=False
    )
```

```python
import functools

import jax
import jax.numpy as jnp
from jax import lax
from jax.experimental import pallas as pl
from jax.experimental.pallas import tpu as pltpu
from jax.sharding import PartitionSpec as P

X, YL, Z, R = 4, 2, 4, 4
Q = YL * Z
GROUP = Q * R
ORDER = ((0, 0), (1, 0), (1, 1), (1, 3), (0, 2), (1, 2), (0, 1), (0, 3))
SLOT = {pair: number for number, pair in enumerate(ORDER)}
PAIRS = [(slot, flip) for slot in range(Q) for flip in range(2)]
PIECES, AHEAD = 5, (2, 2, 3, 5)
GOING = ((0, 1), (0, 3), (1, 1), (1, 3), (1, 0), (0, 2), (1, 2))


def hops(d):
    dy, dz = ORDER[d // R]
    return min(dz, Z - dz) + (1 if dy else d % R // 2 * 2)


OTHERS = sorted(range(1, GROUP), key=lambda d: -hops(d))

FAR = sorted(PAIRS[1:], key=lambda pair: -hops(pair[0] * R + pair[1] * 2))
BF16, F32 = jnp.bfloat16, jnp.float32
NT = (((1,), (1,)), ((), ()))


def mirror(d):
    dy, dz = ORDER[d // R]
    return SLOT[dy, (4 - dz) % 4] * R + d % R


def halves(value):
    high = value.astype(BF16)
    return high, (value - high.astype(F32)).astype(BF16)


def times(value, high, low):
    a, b = halves(value)
    total = lax.dot_general(a, high, NT, preferred_element_type=F32)
    total = total + lax.dot_general(b, high, NT, preferred_element_type=F32)
    return total + lax.dot_general(a, low, NT, preferred_element_type=F32)


def kernel(
    dims,
    v_hbm, r_hbm, f_hbm,
    out,
    v_loc, r_loc, v_all, r_all, p_sum, p_send, p_recv, g_send, g_recv, g_own, g_all, s_own, s_all, v_tail, r_tail, factor, f_high, f_low,
    ld_sem, own_sem, r_ssem, r_rsem, x_ssem, v_ssem, v_rsem,
    gs_ssem, gs_rsem, ga_ssem, ga_rsem, ps_ssem, ps_rsem, sa_ssem, sa_rsem, o_ssem, o_rsem, o_own,
):
    rows, panel, whole, valid, chunk, slim, extras, step = dims
    per = rows // R
    share = panel // (X * Q)
    half = chunk // 2
    prow, pcol = lax.axis_index("prow"), lax.axis_index("pcol")
    x, yl, z = pcol // Q, lax.rem(pcol // Z, YL), lax.rem(pcol, Z)
    h, k = prow // 2, lax.rem(prow, 2)

    yls = [yl, 1 - yl]
    zs = [z] + [lax.rem(z + dz, Z) for dz in range(1, Z)]
    xs = [x] + [lax.rem(x + dx, X) for dx in range(1, X)]
    prows = [prow, h * 2 + 1 - k, (1 - h) * 2 + k, (1 - h) * 2 + 1 - k]

    def at(d, dx=0):
        dy, dz = ORDER[d // R]
        return prows[d % R], xs[dx] * Q + yls[dy] * Z + zs[dz]

    def send(src, dst, ssem, rsem, to):
        copy = pltpu.make_async_remote_copy(
            src_ref=src, dst_ref=dst, send_sem=ssem, recv_sem=rsem,
            device_id=to, device_id_type=pl.DeviceIdType.MESH,
        )
        copy.start()
        return copy

    def arrived(ref, sem):
        pltpu.make_async_copy(ref, ref, sem).wait()

    def first_of(q):
        return (q * (slim // 128) + sum((q + (Q - 1 - e)) // Q for e in extras)) * 128

    def wide(q):
        return sum((q + (Q - e)) // Q - (q + (Q - 1 - e)) // Q for e in extras) == 1

    def place_q(slot):
        return yls[ORDER[slot][0]] * Z + zs[ORDER[slot][1]]

    def either(q, action, most=chunk):
        @pl.when(wide(q))
        def _():
            action(most)

        @pl.when(jnp.logical_not(wide(q)))
        def _():
            action(most - 128)

    @pl.when(jnp.logical_not(wide(place_q(0))))
    def _():
        v_all[:, :, :, :, slim:] = jnp.zeros((2, Q, 2, per, chunk - slim), BF16)
        r_all[:, :, slim:] = jnp.zeros((2, panel, chunk - slim), BF16)

    barrier = pltpu.get_barrier_semaphore()
    for d in OTHERS:
        pl.semaphore_signal(barrier, inc=1, device_id=at(d), device_id_type=pl.DeviceIdType.MESH)
    for dx in (1, 3):
        pl.semaphore_signal(barrier, inc=1, device_id=at(0, dx), device_id_type=pl.DeviceIdType.MESH)

    load_r = pltpu.make_async_copy(r_hbm.at[:, :, pl.ds(0, whole)], r_loc.at[:, :, pl.ds(0, whole)], ld_sem.at[0])
    load_v = [
        pltpu.make_async_copy(
            v_hbm.at[pl.ds(r * per, per), pl.ds(0, whole)], v_loc.at[r // 2, r % 2, :, pl.ds(0, whole)], ld_sem.at[1 + r])
        for r in (0, 2, 1, 3)
    ]
    load_r.start()
    for load in load_v:
        load.start()
    load_f = pltpu.make_async_copy(f_hbm, factor, ld_sem.at[1 + R])
    load_f.start()
    tails = [
        pltpu.make_async_copy(v_hbm.at[:, pl.ds(whole, valid)], v_tail, ld_sem.at[2 + R]),
        pltpu.make_async_copy(r_hbm.at[:, :, pl.ds(whole, valid)], r_tail, ld_sem.at[3 + R]),
    ]
    for load in tails:
        load.start()

    edge = v_loc.shape[3] - whole
    for load in tails:
        load.wait()
    for r in range(R):
        v_loc[r // 2, r % 2, :, whole:] = jnp.zeros((per, edge), BF16)
        v_loc[r // 2, r % 2, :, whole:whole + valid] = v_tail[r * per:(r + 1) * per, :]
    for p in range(2):
        r_loc[p, :, whole:] = jnp.zeros((share, edge), BF16)
        r_loc[p, :, whole:whole + valid] = r_tail[p]

    pl.semaphore_wait(barrier, GROUP - 1 + 2)

    mine = pl.ds(pl.multiple_of(pcol * share, share), share)

    def columns(slot, count, skip=0):
        return pl.ds(pl.multiple_of(first_of(place_q(slot)) + skip, 128), count)

    load_r.wait()
    def r_mine(count):
        return r_all.at[:, mine, pl.ds(0, count)]

    either(place_q(0), lambda n: pltpu.make_async_copy(r_loc.at[:, :, columns(0, n)], r_mine(n), own_sem.at[0]).start())
    for slot in range(1, Q):
        d = mirror(slot * R)
        either(place_q(d // R), lambda n: send(
            r_loc.at[:, :, columns(d // R, n)], r_mine(n), r_ssem.at[slot], r_rsem.at[slot], at(d)))
    part_width = chunk // PIECES

    def v_sem(slot, number):
        return slot if number is None else Q + slot * PIECES + number

    def v_landing(slot, number, count):
        return v_all.at[0 if number is None else 1, slot, :, :, pl.ds((number or 0) * part_width, count)]

    def v_source(slot, number, count):
        return v_loc.at[:, 0 if number is None else 1, :, columns(slot, count, (number or 0) * part_width)]

    def v_each(q, number, action):
        if number is None:
            either(q, action)
        elif number == PIECES - 1:
            either(q, action, part_width)
        else:
            action(part_width)

    def v_out(numbers):
        for number in numbers:
            for pair in GOING:
                d = SLOT[pair] * R
                slot = mirror(d) // R
                sem = v_sem(slot, number)
                v_each(place_q(d // R), number, lambda n: send(
                    v_source(d // R, number, n), v_landing(slot, number, n), v_ssem.at[sem], v_rsem.at[sem], at(d)))

    def v_arrived(slot, number):
        sem = v_rsem.at[v_sem(slot, number)]
        v_each(place_q(0), number, lambda n: arrived(v_landing(slot, number, n), sem))

    def own_copy(core):
        def start(n):
            pltpu.make_async_copy(
                v_loc.at[:, core, :, columns(0, n)], v_all.at[core, 0, :, :, pl.ds(0, n)], own_sem.at[1 + core]).start()
        either(place_q(0), start)

    def own_copied(core):
        either(place_q(0), lambda n: arrived(v_all.at[core, 0, :, :, pl.ds(0, n)], own_sem.at[1 + core]))

    load_v[0].wait()
    load_v[1].wait()
    v_out([None])
    own_copy(0)
    load_v[2].wait()
    load_v[3].wait()
    v_out(range(AHEAD[0]))
    own_copy(1)

    def piece(slot, dx, cols=None):
        source = pl.ds(pl.multiple_of(at(slot * R, dx)[1] * share, share), share)
        return r_all.at[:, source, :] if cols is None else r_all.at[:, source, cols]

    parts = (pl.ds(0, half), pl.ds(half, half))

    def spread(slot):
        came = r_rsem.at[slot] if slot else own_sem.at[0]
        either(place_q(0), lambda n: arrived(piece(slot, 0, pl.ds(0, n)), came))
        for dx in (1, 3):
            send(piece(slot, 0), piece(slot, 0), x_ssem.at[dx * Q + slot], r_rsem.at[(4 - dx) * Q + slot], at(0, dx))

    def relay(slot):
        for number, dx in enumerate((1, 3)):
            arrived(piece(slot, dx), r_rsem.at[dx * Q + slot])
            part = piece(slot, dx, parts[number])
            send(part, part, x_ssem.at[2 * number * Q + slot], r_rsem.at[(2 + 2 * number) * Q + slot], at(0, 4 - dx))

    lag = 1
    for slot in range(Q + lag):
        if slot < Q:
            spread(slot)
        if slot >= lag:
            relay(slot - lag)

    load_f.wait()
    f_high[...], f_low[...] = halves(factor[...])
    for slot in range(Q):
        for number in range(2):
            arrived(piece(slot, 2, parts[number]), r_rsem.at[(2 + 2 * number) * Q + slot])

    def summed(a, b, m):
        def one(j, total):
            cols = pl.ds(pl.multiple_of(j * step, 128), step)
            return total + lax.dot_general(a(cols), b(cols), NT, preferred_element_type=F32)
        return lax.fori_loop(0, chunk // step, one, jnp.zeros((m, panel), F32))

    part = panel // GROUP
    gram = summed(lambda cols: r_all[0, :, cols], lambda cols: r_all[1, :, cols], panel)
    g_send[...] = gram.reshape(GROUP, part, panel).astype(BF16)

    def owner(d):
        across, far = at(d)
        return lax.rem(far, Q) * R + across

    for d in OTHERS:
        send(g_send.at[owner(d)], g_recv.at[mirror(d)], gs_ssem.at[d], gs_rsem.at[mirror(d)], at(d))
    v_out(range(AHEAD[0], AHEAD[1]))

    sides = (h, 1 - h)

    def place(slot, flip, core):
        return sides[flip] * 2 + core, at(slot * R)[1]

    def turned(slot):
        return mirror(slot * R) // R

    def tall(ref):
        value = ref[...]
        return value.reshape(2 * Q * per, value.shape[-1])

    def p_out(core):
        for slot, flip in FAR:
            send(p_send.at[core, slot, sides[flip]], p_recv.at[(turned(slot) * 2 + flip) * 2 + k],
                 ps_ssem.at[(slot * 2 + flip) * 2 + core], ps_rsem.at[(turned(slot) * 2 + flip) * 2 + k], place(slot, flip, core))

        @pl.when(k != core)
        def _():
            send(p_send.at[core, 0, h], p_recv.at[k], ps_ssem.at[core], ps_rsem.at[k], place(0, 0, core))

        @pl.when(k == core)
        def _():
            p_recv[k] = p_send[core, 0, h]

    for slot in range(1, Q):
        v_arrived(slot, None)
    own_copied(0)
    for p in range(2):
        total = summed(lambda cols: tall(v_all.at[0, :, :, :, cols]), lambda cols: r_all[p, :, cols], 2 * Q * per)
        p_send[0, :, :, :, p * panel:(p + 1) * panel] = total.astype(BF16).reshape(Q, 2, per, panel)
    p_out(0)
    v_out(range(AHEAD[1], AHEAD[2]))

    for d in OTHERS:
        arrived(g_recv.at[d], gs_rsem.at[d])
    g_own[...] = (jnp.sum(g_recv[1:].astype(F32), axis=0) + g_send[owner(0)].astype(F32)).astype(BF16)
    for d in OTHERS:
        send(g_own, g_all.at[owner(0)], ga_ssem.at[d], ga_rsem.at[mirror(d)], at(d))
    g_all[owner(0)] = g_own[...]
    v_out(range(AHEAD[2], AHEAD[3]))

    def second_half(numbers):
        for number in numbers:
            for slot in range(1, Q):
                v_arrived(slot, number)
            cols = pl.ds(number * part_width, part_width)
            for p in range(2):
                here = slice(p * panel, (p + 1) * panel)
                total = lax.dot_general(
                    tall(v_all.at[1, :, :, :, cols]), r_all[p, :, cols], NT, preferred_element_type=F32)
                if number:
                    total = total + p_sum[:, here]
                if number < PIECES - 1:
                    p_sum[:, here] = total
                else:
                    p_send[1, :, :, :, here] = total.astype(BF16).reshape(Q, 2, per, panel)

    own_copied(1)
    second_half(range(AHEAD[1]))

    def s_place(core, slot, flip):
        return s_all.at[core, slot, sides[flip]]

    def s_out(core):
        @pl.when(k == core)
        def _():
            for slot, flip in FAR:
                for sender in range(2):
                    spot = (slot * 2 + flip) * 2 + sender
                    arrived(p_recv.at[spot], ps_rsem.at[spot])
            arrived(p_recv.at[1 - k], ps_rsem.at[1 - k])
            product = jnp.sum(p_recv[...].astype(F32), axis=0)
            first = times(product[:, :panel], f_high[0], f_low[0]).astype(BF16)
            second = times(product[:, panel:], f_high[1], f_low[1])
            for d in OTHERS:
                arrived(g_all.at[owner(d)], ga_rsem.at[d])
            gram = g_all[...].reshape(panel, panel)
            second = second - times(jnp.dot(first, gram, preferred_element_type=F32), f_high[1], f_low[1])
            s_own[:, :panel] = first
            s_own[:, panel:] = second.astype(BF16)
            for slot, flip in FAR:
                spot = (turned(slot) * 2 + flip) * 2 + core
                send(s_own, s_all.at[core, turned(slot), h], sa_ssem.at[(slot * 2 + flip) * 2], sa_rsem.at[spot],
                     place(slot, flip, core))
            send(s_own, s_place(core, 0, 0), sa_ssem.at[1], sa_rsem.at[core], place(0, 0, 1 - core))
            s_all[core, 0, h] = s_own[...]

    def s_shared(core):
        @pl.when(k == core)
        def _():
            for slot, flip in FAR:
                spot = (slot * 2 + flip) * 2 + core
                arrived(s_place(core, slot, flip), sa_rsem.at[spot])
                send(s_place(core, slot, flip), s_place(core, slot, flip), sa_ssem.at[(slot * 2 + flip) * 2 + 1],
                     sa_rsem.at[spot], place(0, 0, 1 - core))

        @pl.when(k != core)
        def _():
            for slot, flip in FAR + [(0, 0)]:
                arrived(s_place(core, slot, flip), sa_rsem.at[(slot * 2 + flip) * 2 + core])

    base = first_of(place_q(0))
    width = chunk // 6

    def results(core, first, stop):
        def update(j):
            here = pl.ds(pl.multiple_of(j * width, 128), width)
            change = jnp.dot(tall(s_all.at[core, :, :, :, pl.ds(0, panel)]), r_all[0, :, here], preferred_element_type=F32)
            change = change + jnp.dot(
                tall(s_all.at[core, :, :, :, pl.ds(panel, panel)]), r_all[1, :, here], preferred_element_type=F32)
            fresh = (tall(v_all.at[core, :, :, :, here]).astype(F32) - change).astype(BF16)
            v_all[core, :, :, :, here] = fresh.reshape(Q, 2, per, width)

        def leave(j, count):
            there = pl.ds(pl.multiple_of(base + j * width, 128), count)
            here = pl.ds(pl.multiple_of(j * width, 128), count)
            for slot, flip in FAR:
                send(v_all.at[core, slot, sides[flip], :, here], out.at[prow, :, there],
                     o_ssem.at[(slot * 2 + flip) * 2 + core], o_rsem.at[(turned(slot) * 2 + flip) * 2 + k],
                     place(slot, flip, core))

            @pl.when(k == core)
            def _():
                pltpu.make_async_copy(v_all.at[core, 0, h, :, here], out.at[prow, :, there], o_own.at[0]).start()

            @pl.when(k != core)
            def _():
                send(v_all.at[core, 0, h, :, here], out.at[prow, :, there], o_ssem.at[core], o_rsem.at[k],
                     place(0, 0, core))

        last = chunk // width - 1

        @pl.loop(first, min(stop, last))
        def _(j):
            update(j)
            leave(j, width)
        if stop > last:
            update(last)
            either(place_q(0), lambda n: leave(last, n), width)

    s_out(0)
    second_half(range(AHEAD[1], PIECES))
    p_out(1)
    s_shared(0)
    results(0, 0, 3)
    s_out(1)
    results(0, 3, 6)
    s_shared(1)
    results(1, 0, 6)

    for slot in range(Q):
        if slot:
            q = place_q(turned(slot))
            either(q, lambda n: arrived(piece(slot, 0, pl.ds(0, n)), r_ssem.at[slot]))
            for number in (None, *range(PIECES)):
                sem = v_ssem.at[v_sem(slot, number)]
                v_each(q, number, lambda n: arrived(v_landing(slot, number, n), sem))
        for dx in (1, 3):
            arrived(piece(slot, 0), x_ssem.at[dx * Q + slot])
        for number in range(2):
            arrived(piece(slot, 0, parts[number]), x_ssem.at[2 * number * Q + slot])
    def out_rows(n):
        return out.at[0, :, pl.ds(0, n)]

    either(place_q(0), lambda n: arrived(out_rows(n), o_own.at[0]))
    for d in OTHERS:
        arrived(g_own, gs_ssem.at[d])
        arrived(g_own, ga_ssem.at[d])
        arrived(s_own, sa_ssem.at[d])

    def ended(spot):
        arrived(s_own, ps_ssem.at[spot])
        either(place_q(0), lambda n: arrived(out_rows(n), o_ssem.at[spot]))

    def landed(slot, flip, core):
        q = place_q(slot)

        def wait(n):
            there = pl.ds(pl.multiple_of(first_of(q), 128), n)
            arrived(out.at[place(slot, flip, core)[0], :, there], o_rsem.at[(slot * 2 + flip) * 2 + core])
        either(q, wait)

    ended(1 - k)
    landed(0, 0, 1 - k)
    for slot, flip in FAR:
        for core in range(2):
            ended((slot * 2 + flip) * 2 + core)
            landed(slot, flip, core)


def joined(width, held, out, line, out_sem):
    stores = []
    rows = held.shape[1]
    for r in sorted(range(R), key=lambda r: r * width % 128):
        first, shift = r * width // 128 * 128, r * width % 128
        end = (r + 1) * width // 128 * 128
        if shift == 0:
            source = held.at[r, :, pl.ds(0, end - first)]
        else:
            count = (end - first) // 128
            lane = lax.broadcasted_iota(jnp.int32, (rows, 128), 1)
            keep = held[r - 1, :, pl.ds(first - (r - 1) * width // 128 * 128, 128)].astype(F32)
            turned = pltpu.roll(held[r, :, :128].astype(F32), shift, 1)
            line[r // 2, :, :128] = jnp.where(lane < shift, keep, turned).astype(BF16)
            width_step = 13 * 128
            for a in range(128, count * 128, width_step):
                n = min(width_step, count * 128 - a)
                wide = held[r, :, a - 128:a + n].astype(F32)
                line[r // 2, :, a:a + n] = pltpu.roll(wide, shift, 1)[:, 128:].astype(BF16)
            source = line.at[r // 2]
        store = pltpu.make_async_copy(source, out.at[:, pl.ds(first, end - first)], out_sem.at[r])
        store.start()
        stores.append(store)
    for store in stores:
        store.wait()


def body(vectors, reflectors, panel_factor):
    rows, width = vectors.shape
    panel = panel_factor.shape[1]
    share = reflectors.shape[1]
    tiles = pl.cdiv(width, 128)
    chunk = pl.cdiv(tiles, Q) * 128
    whole = (tiles - 1) * 128
    slim = tiles // Q * 128
    extras = tuple(number * Q // (tiles % Q) for number in range(tiles % Q))
    dims = (rows, panel, whole, width - whole, chunk, slim, extras, chunk // 3)
    per = rows // R
    any_spec = pl.BlockSpec(memory_space=pl.ANY)
    dma = pltpu.SemaphoreType.DMA
    part = panel // GROUP
    gathered = pl.pallas_call(
        functools.partial(kernel, dims),
        out_shape=pltpu.VMEM((R, per, tiles * 128), BF16),
        in_specs=[
            any_spec, any_spec,
            any_spec,
        ],
        out_specs=pl.BlockSpec(memory_space=pltpu.VMEM),
        scratch_shapes=[
            pltpu.VMEM((2, 2, per, tiles * 128), BF16),
            pltpu.VMEM((2, share, tiles * 128), BF16),
            pltpu.VMEM((2, Q, 2, per, chunk), BF16),
            pltpu.VMEM((2, panel, chunk), BF16),
            pltpu.VMEM((rows * Q // 2, 2 * panel), F32),
            pltpu.VMEM((2, Q, 2, per, 2 * panel), BF16),
            pltpu.VMEM((GROUP, per, 2 * panel), BF16),
            pltpu.VMEM((GROUP, part, panel), BF16),
            pltpu.VMEM((GROUP, part, panel), BF16),
            pltpu.VMEM((part, panel), BF16),
            pltpu.VMEM((GROUP, part, panel), BF16),
            pltpu.VMEM((per, 2 * panel), BF16),
            pltpu.VMEM((2, Q, 2, per, 2 * panel), BF16),
            pltpu.VMEM((rows, width - whole), BF16),
            pltpu.VMEM((2, share, width - whole), BF16),
            pltpu.VMEM((2, panel, panel), F32),
            pltpu.VMEM((2, panel, panel), BF16),
            pltpu.VMEM((2, panel, panel), BF16),
            dma((4 + R,)), dma((3,)), dma((Q,)), dma(((X + 1) * Q,)), dma((X * Q,)), dma((Q + Q * PIECES,)), dma((Q + Q * PIECES,)),
            dma((GROUP,)), dma((GROUP,)), dma((GROUP,)), dma((GROUP,)), dma((GROUP,)), dma((GROUP,)),
            dma((GROUP,)), dma((GROUP,)), dma((GROUP,)), dma((GROUP,)), dma((1,)),
        ],
        compiler_params=pltpu.CompilerParams(
            collective_id=0, has_side_effects=True, vmem_limit_bytes=62700000
        ),
        name="back_transform",
    )(vectors, reflectors, panel_factor)
    line = R * width // 128 * 128 - (R - 1) * width // 128 * 128
    rows_out = pl.pallas_call(
        functools.partial(joined, width),
        out_shape=jax.ShapeDtypeStruct((per, R * width), BF16),
        in_specs=[pl.BlockSpec(memory_space=pltpu.VMEM)],
        out_specs=any_spec,
        scratch_shapes=[pltpu.VMEM((2, per, line), BF16), dma((R,))],
        compiler_params=pltpu.CompilerParams(vmem_limit_bytes=16 * 1024 * 1024),
        name="joined",
    )(gathered)
    return rows_out[None]


def solution(mesh):
    placed = (P("pcol", "prow"), P(None, "pcol", "prow"), P())
    return jax.shard_map(
        body, mesh=mesh, in_specs=placed, out_specs=P("pcol", "prow", None), check_vma=False
    )
```

```python
import functools

import jax
import jax.numpy as jnp
from jax import lax
from jax.experimental import pallas as pl
from jax.experimental.pallas import tpu as pltpu
from jax.sharding import PartitionSpec as P

X, YL, Z, R = 4, 2, 4, 4
Q = YL * Z
GROUP = Q * R
ORDER = ((0, 0), (1, 0), (1, 1), (1, 3), (0, 2), (1, 2), (0, 1), (0, 3))
SLOT = {pair: number for number, pair in enumerate(ORDER)}
PAIRS = [(slot, flip) for slot in range(Q) for flip in range(2)]
PIECES, AHEAD = 5, (2, 3, 4, 5)
GOING = ((0, 1), (0, 3), (1, 1), (1, 3), (1, 0), (0, 2), (1, 2))


def hops(d):
    dy, dz = ORDER[d // R]
    return min(dz, Z - dz) + (1 if dy else d % R // 2 * 2)


OTHERS = sorted(range(1, GROUP), key=lambda d: -hops(d))

FAR = sorted(PAIRS[1:], key=lambda pair: -hops(pair[0] * R + pair[1] * 2))
DISTANT = sorted(range(1, Q), key=lambda slot: -hops(slot * R))
BF16, F32 = jnp.bfloat16, jnp.float32
NT = (((1,), (1,)), ((), ()))


def mirror(d):
    dy, dz = ORDER[d // R]
    return SLOT[dy, (4 - dz) % 4] * R + d % R


def halves(value):
    high = value.astype(BF16)
    return high, (value - high.astype(F32)).astype(BF16)


def times(value, high, low):
    a, b = halves(value)
    total = lax.dot_general(a, high, NT, preferred_element_type=F32)
    total = total + lax.dot_general(b, high, NT, preferred_element_type=F32)
    return total + lax.dot_general(a, low, NT, preferred_element_type=F32)


def kernel(
    dims,
    v_hbm, r_hbm, f_hbm,
    out,
    v_loc, r_loc, v_all, r_all, p_sum, p_send, p_swap, p_recv, g_send, g_recv, g_own, g_all, s_own, s_all, v_tail, r_tail, factor, f_high, f_low,
    ld_sem, own_sem, r_ssem, r_rsem, x_ssem, v_ssem, v_rsem,
    pw_ssem, pw_rsem, gs_ssem, gs_rsem, ga_ssem, ga_rsem, ps_ssem, ps_rsem, sa_ssem, sa_rsem, o_ssem, o_rsem, o_own,
):
    rows, panel, whole, valid, chunk, slim, extras, step = dims
    per = rows // R
    share = panel // (X * Q)
    half = chunk // 2
    prow, pcol = lax.axis_index("prow"), lax.axis_index("pcol")
    x, yl, z = pcol // Q, lax.rem(pcol // Z, YL), lax.rem(pcol, Z)
    h, k = prow // 2, lax.rem(prow, 2)

    yls = [yl, 1 - yl]
    zs = [z] + [lax.rem(z + dz, Z) for dz in range(1, Z)]
    xs = [x] + [lax.rem(x + dx, X) for dx in range(1, X)]
    prows = [prow, h * 2 + 1 - k, (1 - h) * 2 + k, (1 - h) * 2 + 1 - k]

    def at(d, dx=0):
        dy, dz = ORDER[d // R]
        return prows[d % R], xs[dx] * Q + yls[dy] * Z + zs[dz]

    def send(src, dst, ssem, rsem, to):
        copy = pltpu.make_async_remote_copy(
            src_ref=src, dst_ref=dst, send_sem=ssem, recv_sem=rsem,
            device_id=to, device_id_type=pl.DeviceIdType.MESH,
        )
        copy.start()
        return copy

    def arrived(ref, sem):
        pltpu.make_async_copy(ref, ref, sem).wait()

    def first_of(q):
        return (q * (slim // 128) + sum((q + (Q - 1 - e)) // Q for e in extras)) * 128

    def wide(q):
        return sum((q + (Q - e)) // Q - (q + (Q - 1 - e)) // Q for e in extras) == 1

    def place_q(slot):
        return yls[ORDER[slot][0]] * Z + zs[ORDER[slot][1]]

    def either(q, action, most=chunk):
        @pl.when(wide(q))
        def _():
            action(most)

        @pl.when(jnp.logical_not(wide(q)))
        def _():
            action(most - 128)

    @pl.when(jnp.logical_not(wide(place_q(0))))
    def _():
        v_all[:, :, :, :, slim:] = jnp.zeros((2, Q, 2, per, chunk - slim), BF16)
        r_all[:, :, slim:] = jnp.zeros((2, panel, chunk - slim), BF16)

    barrier = pltpu.get_barrier_semaphore()
    for d in OTHERS:
        pl.semaphore_signal(barrier, inc=1, device_id=at(d), device_id_type=pl.DeviceIdType.MESH)
    for dx in (1, 3):
        pl.semaphore_signal(barrier, inc=1, device_id=at(0, dx), device_id_type=pl.DeviceIdType.MESH)

    load_r = pltpu.make_async_copy(r_hbm.at[:, :, pl.ds(0, whole)], r_loc.at[:, :, pl.ds(0, whole)], ld_sem.at[0])
    load_v = [
        pltpu.make_async_copy(
            v_hbm.at[pl.ds(r * per, per), pl.ds(0, whole)], v_loc.at[r // 2, r % 2, :, pl.ds(0, whole)], ld_sem.at[1 + r])
        for r in (0, 2, 1, 3)
    ]
    load_r.start()
    for load in load_v:
        load.start()
    load_f = pltpu.make_async_copy(f_hbm, factor, ld_sem.at[1 + R])
    load_f.start()
    tails = [
        pltpu.make_async_copy(v_hbm.at[:, pl.ds(whole, valid)], v_tail, ld_sem.at[2 + R]),
        pltpu.make_async_copy(r_hbm.at[:, :, pl.ds(whole, valid)], r_tail, ld_sem.at[3 + R]),
    ]
    for load in tails:
        load.start()

    edge = v_loc.shape[3] - whole
    for load in tails:
        load.wait()
    for r in range(R):
        v_loc[r // 2, r % 2, :, whole:] = jnp.zeros((per, edge), BF16)
        v_loc[r // 2, r % 2, :, whole:whole + valid] = v_tail[r * per:(r + 1) * per, :]
    for p in range(2):
        r_loc[p, :, whole:] = jnp.zeros((share, edge), BF16)
        r_loc[p, :, whole:whole + valid] = r_tail[p]

    pl.semaphore_wait(barrier, GROUP - 1 + 2)

    mine = pl.ds(pl.multiple_of(pcol * share, share), share)

    def columns(slot, count, skip=0):
        return pl.ds(pl.multiple_of(first_of(place_q(slot)) + skip, 128), count)

    load_r.wait()
    def r_mine(count):
        return r_all.at[:, mine, pl.ds(0, count)]

    either(place_q(0), lambda n: pltpu.make_async_copy(r_loc.at[:, :, columns(0, n)], r_mine(n), own_sem.at[0]).start())
    for slot in range(1, Q):
        d = mirror(slot * R)
        either(place_q(d // R), lambda n: send(
            r_loc.at[:, :, columns(d // R, n)], r_mine(n), r_ssem.at[slot], r_rsem.at[slot], at(d)))
    part_width = chunk // PIECES

    def v_sem(slot, number):
        return slot if number is None else Q + slot * PIECES + number

    def v_landing(slot, number, count):
        return v_all.at[0 if number is None else 1, slot, :, :, pl.ds((number or 0) * part_width, count)]

    def v_source(slot, number, count):
        return v_loc.at[:, 0 if number is None else 1, :, columns(slot, count, (number or 0) * part_width)]

    def v_each(q, number, action):
        if number is None:
            either(q, action)
        elif number == PIECES - 1:
            either(q, action, part_width)
        else:
            action(part_width)

    def v_out(numbers):
        for number in numbers:
            for pair in GOING:
                d = SLOT[pair] * R
                slot = mirror(d) // R
                sem = v_sem(slot, number)
                v_each(place_q(d // R), number, lambda n: send(
                    v_source(d // R, number, n), v_landing(slot, number, n), v_ssem.at[sem], v_rsem.at[sem], at(d)))

    def v_arrived(slot, number):
        sem = v_rsem.at[v_sem(slot, number)]
        v_each(place_q(0), number, lambda n: arrived(v_landing(slot, number, n), sem))

    def own_copy(core):
        def start(n):
            pltpu.make_async_copy(
                v_loc.at[:, core, :, columns(0, n)], v_all.at[core, 0, :, :, pl.ds(0, n)], own_sem.at[1 + core]).start()
        either(place_q(0), start)

    def own_copied(core):
        either(place_q(0), lambda n: arrived(v_all.at[core, 0, :, :, pl.ds(0, n)], own_sem.at[1 + core]))

    load_v[0].wait()
    load_v[1].wait()
    v_out([None])
    own_copy(0)
    load_v[2].wait()
    load_v[3].wait()
    v_out(range(AHEAD[0]))
    own_copy(1)

    def piece(slot, dx, cols=None):
        source = pl.ds(pl.multiple_of(at(slot * R, dx)[1] * share, share), share)
        return r_all.at[:, source, :] if cols is None else r_all.at[:, source, cols]

    parts = (pl.ds(0, half), pl.ds(half, half))

    def spread(slot):
        came = r_rsem.at[slot] if slot else own_sem.at[0]
        either(place_q(0), lambda n: arrived(piece(slot, 0, pl.ds(0, n)), came))
        for dx in (1, 3):
            send(piece(slot, 0), piece(slot, 0), x_ssem.at[dx * Q + slot], r_rsem.at[(4 - dx) * Q + slot], at(0, dx))

    def relay(slot):
        for number, dx in enumerate((1, 3)):
            arrived(piece(slot, dx), r_rsem.at[dx * Q + slot])
            part = piece(slot, dx, parts[number])
            send(part, part, x_ssem.at[2 * number * Q + slot], r_rsem.at[(2 + 2 * number) * Q + slot], at(0, 4 - dx))

    lag = 1
    for slot in range(Q + lag):
        if slot < Q:
            spread(slot)
        if slot >= lag:
            relay(slot - lag)

    load_f.wait()
    f_high[...], f_low[...] = halves(factor[...])
    for slot in range(Q):
        for number in range(2):
            arrived(piece(slot, 2, parts[number]), r_rsem.at[(2 + 2 * number) * Q + slot])

    def summed(a, b, m):
        def one(j, total):
            cols = pl.ds(pl.multiple_of(j * step, 128), step)
            return total + lax.dot_general(a(cols), b(cols), NT, preferred_element_type=F32)
        return lax.fori_loop(0, chunk // step, one, jnp.zeros((m, panel), F32))

    part = panel // GROUP
    gram = summed(lambda cols: r_all[0, :, cols], lambda cols: r_all[1, :, cols], panel)
    g_send[...] = gram.reshape(GROUP, part, panel).astype(BF16)

    def owner(d):
        across, far = at(d)
        return lax.rem(far, Q) * R + across

    for d in OTHERS:
        send(g_send.at[owner(d)], g_recv.at[mirror(d)], gs_ssem.at[d], gs_rsem.at[mirror(d)], at(d))
    v_out(range(AHEAD[0], AHEAD[1]))

    sides = (h, 1 - h)

    def place(slot, flip, core):
        return sides[flip] * 2 + core, at(slot * R)[1]

    def turned(slot):
        return mirror(slot * R) // R

    def tall(ref):
        value = ref[...]
        return value.reshape(2 * Q * per, value.shape[-1])

    step_y = lax.rem(h + k, 2)

    def p_out(core):
        send(p_send.at[core, :, 1 - k], p_swap.at[core], pw_ssem.at[core], pw_rsem.at[core], place(0, 0, 1 - k))
        arrived(p_swap.at[core], pw_rsem.at[core])
        p_send[core, :, k] = (p_send[core, :, k].astype(F32) + p_swap[core].astype(F32)).astype(BF16)

        def p_to(slot):
            spot = turned(slot) * 2 + step_y
            send(p_send.at[core, slot, k], p_recv.at[spot], ps_ssem.at[slot * 2 + core], ps_rsem.at[spot],
                 (k * 2 + core, at(slot * R)[1]))

        for slot in DISTANT:
            p_to(slot)
        here = jnp.logical_and(h == core, k == core)

        @pl.when(jnp.logical_not(here))
        def _():
            p_to(0)

        @pl.when(here)
        def _():
            p_recv[0] = p_send[core, 0, core]

    for slot in range(1, Q):
        v_arrived(slot, None)
    own_copied(0)
    for p in range(2):
        total = summed(lambda cols: tall(v_all.at[0, :, :, :, cols]), lambda cols: r_all[p, :, cols], 2 * Q * per)
        p_send[0, :, :, :, p * panel:(p + 1) * panel] = total.astype(BF16).reshape(Q, 2, per, panel)
    p_out(0)
    v_out(range(AHEAD[1], AHEAD[2]))

    for d in OTHERS:
        arrived(g_recv.at[d], gs_rsem.at[d])
    g_own[...] = (jnp.sum(g_recv[1:].astype(F32), axis=0) + g_send[owner(0)].astype(F32)).astype(BF16)
    for d in OTHERS:
        send(g_own, g_all.at[owner(0)], ga_ssem.at[d], ga_rsem.at[mirror(d)], at(d))
    g_all[owner(0)] = g_own[...]
    v_out(range(AHEAD[2], AHEAD[3]))

    def second_half(numbers):
        for number in numbers:
            for slot in range(1, Q):
                v_arrived(slot, number)
            cols = pl.ds(number * part_width, part_width)
            for p in range(2):
                here = slice(p * panel, (p + 1) * panel)
                total = lax.dot_general(
                    tall(v_all.at[1, :, :, :, cols]), r_all[p, :, cols], NT, preferred_element_type=F32)
                if number:
                    total = total + p_sum[:, here]
                if number < PIECES - 1:
                    p_sum[:, here] = total
                else:
                    p_send[1, :, :, :, here] = total.astype(BF16).reshape(Q, 2, per, panel)

    own_copied(1)
    second_half(range(AHEAD[1]))

    def s_place(core, slot, flip):
        return s_all.at[core, slot, sides[flip]]

    def s_out(core):
        @pl.when(k == core)
        def _():
            for spot in range(1, 2 * Q):
                arrived(p_recv.at[spot], ps_rsem.at[spot])

            @pl.when(h != core)
            def _():
                arrived(p_recv.at[0], ps_rsem.at[0])
            product = jnp.sum(p_recv[...].astype(F32), axis=0)
            first = times(product[:, :panel], f_high[0], f_low[0]).astype(BF16)
            second = times(product[:, panel:], f_high[1], f_low[1])
            for d in OTHERS:
                arrived(g_all.at[owner(d)], ga_rsem.at[d])
            gram = g_all[...].reshape(panel, panel)
            second = second - times(jnp.dot(first, gram, preferred_element_type=F32), f_high[1], f_low[1])
            s_own[:, :panel] = first
            s_own[:, panel:] = second.astype(BF16)
            for slot, flip in FAR:
                spot = (turned(slot) * 2 + flip) * 2 + core
                send(s_own, s_all.at[core, turned(slot), h], sa_ssem.at[(slot * 2 + flip) * 2], sa_rsem.at[spot],
                     place(slot, flip, core))
            send(s_own, s_place(core, 0, 0), sa_ssem.at[1], sa_rsem.at[core], place(0, 0, 1 - core))
            s_all[core, 0, h] = s_own[...]

    def s_shared(core):
        @pl.when(k == core)
        def _():
            for slot, flip in FAR:
                spot = (slot * 2 + flip) * 2 + core
                arrived(s_place(core, slot, flip), sa_rsem.at[spot])
                send(s_place(core, slot, flip), s_place(core, slot, flip), sa_ssem.at[(slot * 2 + flip) * 2 + 1],
                     sa_rsem.at[spot], place(0, 0, 1 - core))

        @pl.when(k != core)
        def _():
            for slot, flip in FAR + [(0, 0)]:
                arrived(s_place(core, slot, flip), sa_rsem.at[(slot * 2 + flip) * 2 + core])

    base = first_of(place_q(0))
    width = chunk // 6

    def results(core, first, stop):
        def update(j):
            here = pl.ds(pl.multiple_of(j * width, 128), width)
            change = jnp.dot(tall(s_all.at[core, :, :, :, pl.ds(0, panel)]), r_all[0, :, here], preferred_element_type=F32)
            change = change + jnp.dot(
                tall(s_all.at[core, :, :, :, pl.ds(panel, panel)]), r_all[1, :, here], preferred_element_type=F32)
            fresh = (tall(v_all.at[core, :, :, :, here]).astype(F32) - change).astype(BF16)
            v_all[core, :, :, :, here] = fresh.reshape(Q, 2, per, width)

        def leave(j, count):
            there = pl.ds(pl.multiple_of(base + j * width, 128), count)
            here = pl.ds(pl.multiple_of(j * width, 128), count)
            for slot, flip in FAR:
                send(v_all.at[core, slot, sides[flip], :, here], out.at[prow, :, there],
                     o_ssem.at[(slot * 2 + flip) * 2 + core], o_rsem.at[(turned(slot) * 2 + flip) * 2 + k],
                     place(slot, flip, core))

            @pl.when(k == core)
            def _():
                pltpu.make_async_copy(v_all.at[core, 0, h, :, here], out.at[prow, :, there], o_own.at[0]).start()

            @pl.when(k != core)
            def _():
                send(v_all.at[core, 0, h, :, here], out.at[prow, :, there], o_ssem.at[core], o_rsem.at[k],
                     place(0, 0, core))

        last = chunk // width - 1

        @pl.loop(first, min(stop, last))
        def _(j):
            update(j)
            leave(j, width)
        if stop > last:
            update(last)
            either(place_q(0), lambda n: leave(last, n), width)

    s_out(0)
    second_half(range(AHEAD[1], PIECES))
    p_out(1)
    s_shared(0)
    results(0, 0, 3)
    s_out(1)
    results(0, 3, 6)
    s_shared(1)
    results(1, 0, 6)

    for slot in range(Q):
        if slot:
            q = place_q(turned(slot))
            either(q, lambda n: arrived(piece(slot, 0, pl.ds(0, n)), r_ssem.at[slot]))
            for number in (None, *range(PIECES)):
                sem = v_ssem.at[v_sem(slot, number)]
                v_each(q, number, lambda n: arrived(v_landing(slot, number, n), sem))
        for dx in (1, 3):
            arrived(piece(slot, 0), x_ssem.at[dx * Q + slot])
        for number in range(2):
            arrived(piece(slot, 0, parts[number]), x_ssem.at[2 * number * Q + slot])
    def out_rows(n):
        return out.at[0, :, pl.ds(0, n)]

    either(place_q(0), lambda n: arrived(out_rows(n), o_own.at[0]))
    for d in OTHERS:
        arrived(g_own, gs_ssem.at[d])
        arrived(g_own, ga_ssem.at[d])
        arrived(s_own, sa_ssem.at[d])

    def ended(spot):
        either(place_q(0), lambda n: arrived(out_rows(n), o_ssem.at[spot]))

    def landed(slot, flip, core):
        q = place_q(slot)

        def wait(n):
            there = pl.ds(pl.multiple_of(first_of(q), 128), n)
            arrived(out.at[place(slot, flip, core)[0], :, there], o_rsem.at[(slot * 2 + flip) * 2 + core])
        either(q, wait)

    for core in range(2):
        arrived(p_swap.at[core], pw_ssem.at[core])
        for slot in DISTANT:
            arrived(s_own, ps_ssem.at[slot * 2 + core])

        @pl.when(jnp.logical_not(jnp.logical_and(h == core, k == core)))
        def _():
            arrived(s_own, ps_ssem.at[core])

    ended(1 - k)
    landed(0, 0, 1 - k)
    for slot, flip in FAR:
        for core in range(2):
            ended((slot * 2 + flip) * 2 + core)
            landed(slot, flip, core)


def joined(width, held, out, line, out_sem):
    stores = []
    rows = held.shape[1]
    for r in sorted(range(R), key=lambda r: r * width % 128):
        first, shift = r * width // 128 * 128, r * width % 128
        end = (r + 1) * width // 128 * 128
        if shift == 0:
            source = held.at[r, :, pl.ds(0, end - first)]
        else:
            count = (end - first) // 128
            lane = lax.broadcasted_iota(jnp.int32, (rows, 128), 1)
            keep = held[r - 1, :, pl.ds(first - (r - 1) * width // 128 * 128, 128)].astype(F32)
            turned = pltpu.roll(held[r, :, :128].astype(F32), shift, 1)
            line[r // 2, :, :128] = jnp.where(lane < shift, keep, turned).astype(BF16)
            width_step = 13 * 128
            for a in range(128, count * 128, width_step):
                n = min(width_step, count * 128 - a)
                wide = held[r, :, a - 128:a + n].astype(F32)
                line[r // 2, :, a:a + n] = pltpu.roll(wide, shift, 1)[:, 128:].astype(BF16)
            source = line.at[r // 2]
        store = pltpu.make_async_copy(source, out.at[:, pl.ds(first, end - first)], out_sem.at[r])
        store.start()
        stores.append(store)
    for store in stores:
        store.wait()


def body(vectors, reflectors, panel_factor):
    rows, width = vectors.shape
    panel = panel_factor.shape[1]
    share = reflectors.shape[1]
    tiles = pl.cdiv(width, 128)
    chunk = pl.cdiv(tiles, Q) * 128
    whole = (tiles - 1) * 128
    slim = tiles // Q * 128
    extras = tuple(number * Q // (tiles % Q) for number in range(tiles % Q))
    dims = (rows, panel, whole, width - whole, chunk, slim, extras, chunk // 3)
    per = rows // R
    any_spec = pl.BlockSpec(memory_space=pl.ANY)
    dma = pltpu.SemaphoreType.DMA
    part = panel // GROUP
    gathered = pl.pallas_call(
        functools.partial(kernel, dims),
        out_shape=pltpu.VMEM((R, per, tiles * 128), BF16),
        in_specs=[
            any_spec, any_spec,
            any_spec,
        ],
        out_specs=pl.BlockSpec(memory_space=pltpu.VMEM),
        scratch_shapes=[
            pltpu.VMEM((2, 2, per, tiles * 128), BF16),
            pltpu.VMEM((2, share, tiles * 128), BF16),
            pltpu.VMEM((2, Q, 2, per, chunk), BF16),
            pltpu.VMEM((2, panel, chunk), BF16),
            pltpu.VMEM((rows * Q // 2, 2 * panel), F32),
            pltpu.VMEM((2, Q, 2, per, 2 * panel), BF16),
            pltpu.VMEM((2, Q, per, 2 * panel), BF16),
            pltpu.VMEM((2 * Q, per, 2 * panel), BF16),
            pltpu.VMEM((GROUP, part, panel), BF16),
            pltpu.VMEM((GROUP, part, panel), BF16),
            pltpu.VMEM((part, panel), BF16),
            pltpu.VMEM((GROUP, part, panel), BF16),
            pltpu.VMEM((per, 2 * panel), BF16),
            pltpu.VMEM((2, Q, 2, per, 2 * panel), BF16),
            pltpu.VMEM((rows, width - whole), BF16),
            pltpu.VMEM((2, share, width - whole), BF16),
            pltpu.VMEM((2, panel, panel), F32),
            pltpu.VMEM((2, panel, panel), BF16),
            pltpu.VMEM((2, panel, panel), BF16),
            dma((4 + R,)), dma((3,)), dma((Q,)), dma(((X + 1) * Q,)), dma((X * Q,)), dma((Q + Q * PIECES,)), dma((Q + Q * PIECES,)),
            dma((2,)), dma((2,)),
            dma((GROUP,)), dma((GROUP,)), dma((GROUP,)), dma((GROUP,)), dma((2 * Q,)), dma((2 * Q,)),
            dma((GROUP,)), dma((GROUP,)), dma((GROUP,)), dma((GROUP,)), dma((1,)),
        ],
        compiler_params=pltpu.CompilerParams(
            collective_id=0, has_side_effects=True, vmem_limit_bytes=62700000
        ),
        name="back_transform",
    )(vectors, reflectors, panel_factor)
    line = R * width // 128 * 128 - (R - 1) * width // 128 * 128
    rows_out = pl.pallas_call(
        functools.partial(joined, width),
        out_shape=jax.ShapeDtypeStruct((per, R * width), BF16),
        in_specs=[pl.BlockSpec(memory_space=pltpu.VMEM)],
        out_specs=any_spec,
        scratch_shapes=[pltpu.VMEM((2, per, line), BF16), dma((R,))],
        compiler_params=pltpu.CompilerParams(vmem_limit_bytes=16 * 1024 * 1024),
        name="joined",
    )(gathered)
    return rows_out[None]


def solution(mesh):
    placed = (P("pcol", "prow"), P(None, "pcol", "prow"), P())
    return jax.shard_map(
        body, mesh=mesh, in_specs=placed, out_specs=P("pcol", "prow", None), check_vma=False
    )
```

```python
import functools

import jax
import jax.numpy as jnp
from jax import lax
from jax.experimental import pallas as pl
from jax.experimental.pallas import tpu as pltpu
from jax.sharding import PartitionSpec as P

X, YL, Z, R = 4, 2, 4, 4
Q = YL * Z
GROUP = Q * R
ORDER = ((0, 0), (1, 0), (1, 1), (1, 3), (0, 2), (1, 2), (0, 1), (0, 3))
SLOT = {pair: number for number, pair in enumerate(ORDER)}
PAIRS = [(slot, flip) for slot in range(Q) for flip in range(2)]
PIECES, AHEAD = 5, (2, 3, 4, 5)
GOING = ((0, 1), (0, 3), (1, 1), (1, 3), (1, 0), (0, 2), (1, 2))


def hops(d):
    dy, dz = ORDER[d // R]
    return min(dz, Z - dz) + (1 if dy else d % R // 2 * 2)


OTHERS = sorted(range(1, GROUP), key=lambda d: -hops(d))

FAR = sorted(PAIRS[1:], key=lambda pair: -hops(pair[0] * R + pair[1] * 2))
DISTANT = sorted(range(1, Q), key=lambda slot: -hops(slot * R))
BF16, F32 = jnp.bfloat16, jnp.float32
NT = (((1,), (1,)), ((), ()))


def mirror(d):
    dy, dz = ORDER[d // R]
    return SLOT[dy, (4 - dz) % 4] * R + d % R


def halves(value):
    high = value.astype(BF16)
    return high, (value - high.astype(F32)).astype(BF16)


def times(value, high, low):
    a, b = halves(value)
    total = lax.dot_general(a, high, NT, preferred_element_type=F32)
    total = total + lax.dot_general(b, high, NT, preferred_element_type=F32)
    return total + lax.dot_general(a, low, NT, preferred_element_type=F32)


def kernel(
    dims,
    v_hbm, r_hbm, f_hbm,
    out,
    v_loc, r_loc, v_all, r_all, p_sum, p_send, p_swap, p_recv, g_send, g_recv, g_own, g_all, s_own, s_all, v_tail, r_tail, factor, f_high, f_low,
    ld_sem, own_sem, r_ssem, r_rsem, x_ssem, v_ssem, v_rsem,
    pw_ssem, pw_rsem, gs_ssem, gs_rsem, ga_ssem, ga_rsem, ps_ssem, ps_rsem, sa_ssem, sa_rsem, o_ssem, o_rsem, o_own,
):
    rows, panel, whole, valid, chunk, slim, extras, step = dims
    per = rows // R
    share = panel // (X * Q)
    half = chunk // 2
    prow, pcol = lax.axis_index("prow"), lax.axis_index("pcol")
    x, yl, z = pcol // Q, lax.rem(pcol // Z, YL), lax.rem(pcol, Z)
    h, k = prow // 2, lax.rem(prow, 2)

    yls = [yl, 1 - yl]
    zs = [z] + [lax.rem(z + dz, Z) for dz in range(1, Z)]
    xs = [x] + [lax.rem(x + dx, X) for dx in range(1, X)]
    prows = [prow, h * 2 + 1 - k, (1 - h) * 2 + k, (1 - h) * 2 + 1 - k]

    def at(d, dx=0):
        dy, dz = ORDER[d // R]
        return prows[d % R], xs[dx] * Q + yls[dy] * Z + zs[dz]

    def send(src, dst, ssem, rsem, to):
        copy = pltpu.make_async_remote_copy(
            src_ref=src, dst_ref=dst, send_sem=ssem, recv_sem=rsem,
            device_id=to, device_id_type=pl.DeviceIdType.MESH,
        )
        copy.start()
        return copy

    def arrived(ref, sem):
        pltpu.make_async_copy(ref, ref, sem).wait()

    def first_of(q):
        return (q * (slim // 128) + sum((q + (Q - 1 - e)) // Q for e in extras)) * 128

    def wide(q):
        return sum((q + (Q - e)) // Q - (q + (Q - 1 - e)) // Q for e in extras) == 1

    def place_q(slot):
        return yls[ORDER[slot][0]] * Z + zs[ORDER[slot][1]]

    def either(q, action, most=chunk):
        @pl.when(wide(q))
        def _():
            action(most)

        @pl.when(jnp.logical_not(wide(q)))
        def _():
            action(most - 128)

    @pl.when(jnp.logical_not(wide(place_q(0))))
    def _():
        v_all[:, :, :, :, slim:] = jnp.zeros((2, Q, 2, per, chunk - slim), BF16)
        r_all[:, :, slim:] = jnp.zeros((2, panel, chunk - slim), BF16)

    barrier = pltpu.get_barrier_semaphore()
    for d in OTHERS:
        pl.semaphore_signal(barrier, inc=1, device_id=at(d), device_id_type=pl.DeviceIdType.MESH)
    for dx in (1, 3):
        pl.semaphore_signal(barrier, inc=1, device_id=at(0, dx), device_id_type=pl.DeviceIdType.MESH)

    load_r = pltpu.make_async_copy(r_hbm.at[:, :, pl.ds(0, whole)], r_loc.at[:, :, pl.ds(0, whole)], ld_sem.at[0])
    load_v = [
        pltpu.make_async_copy(
            v_hbm.at[pl.ds(r * per, per), pl.ds(0, whole)], v_loc.at[r // 2, r % 2, :, pl.ds(0, whole)], ld_sem.at[1 + r])
        for r in (0, 2, 1, 3)
    ]
    load_r.start()
    for load in load_v:
        load.start()
    load_f = pltpu.make_async_copy(f_hbm, factor, ld_sem.at[1 + R])
    load_f.start()
    tails = [
        pltpu.make_async_copy(v_hbm.at[:, pl.ds(whole, valid)], v_tail, ld_sem.at[2 + R]),
        pltpu.make_async_copy(r_hbm.at[:, :, pl.ds(whole, valid)], r_tail, ld_sem.at[3 + R]),
    ]
    for load in tails:
        load.start()

    edge = v_loc.shape[3] - whole
    for load in tails:
        load.wait()
    for r in range(R):
        v_loc[r // 2, r % 2, :, whole:] = jnp.zeros((per, edge), BF16)
        v_loc[r // 2, r % 2, :, whole:whole + valid] = v_tail[r * per:(r + 1) * per, :]
    for p in range(2):
        r_loc[p, :, whole:] = jnp.zeros((share, edge), BF16)
        r_loc[p, :, whole:whole + valid] = r_tail[p]

    pl.semaphore_wait(barrier, GROUP - 1 + 2)

    mine = pl.ds(pl.multiple_of(pcol * share, share), share)

    def columns(slot, count, skip=0):
        return pl.ds(pl.multiple_of(first_of(place_q(slot)) + skip, 128), count)

    load_r.wait()
    def r_mine(count):
        return r_all.at[:, mine, pl.ds(0, count)]

    either(place_q(0), lambda n: pltpu.make_async_copy(r_loc.at[:, :, columns(0, n)], r_mine(n), own_sem.at[0]).start())
    for slot in range(1, Q):
        d = mirror(slot * R)
        either(place_q(d // R), lambda n: send(
            r_loc.at[:, :, columns(d // R, n)], r_mine(n), r_ssem.at[slot], r_rsem.at[slot], at(d)))
    part_width = chunk // PIECES

    def v_sem(slot, number):
        return slot if number is None else Q + slot * PIECES + number

    def v_landing(slot, number, count):
        return v_all.at[0 if number is None else 1, slot, :, :, pl.ds((number or 0) * part_width, count)]

    def v_source(slot, number, count):
        return v_loc.at[:, 0 if number is None else 1, :, columns(slot, count, (number or 0) * part_width)]

    def v_each(q, number, action):
        if number is None:
            either(q, action)
        elif number == PIECES - 1:
            either(q, action, part_width)
        else:
            action(part_width)

    def v_out(numbers):
        for number in numbers:
            for pair in GOING:
                d = SLOT[pair] * R
                slot = mirror(d) // R
                sem = v_sem(slot, number)
                v_each(place_q(d // R), number, lambda n: send(
                    v_source(d // R, number, n), v_landing(slot, number, n), v_ssem.at[sem], v_rsem.at[sem], at(d)))

    def v_arrived(slot, number):
        sem = v_rsem.at[v_sem(slot, number)]
        v_each(place_q(0), number, lambda n: arrived(v_landing(slot, number, n), sem))

    def own_copy(core):
        def start(n):
            pltpu.make_async_copy(
                v_loc.at[:, core, :, columns(0, n)], v_all.at[core, 0, :, :, pl.ds(0, n)], own_sem.at[1 + core]).start()
        either(place_q(0), start)

    def own_copied(core):
        either(place_q(0), lambda n: arrived(v_all.at[core, 0, :, :, pl.ds(0, n)], own_sem.at[1 + core]))

    load_v[0].wait()
    load_v[1].wait()
    v_out([None])
    own_copy(0)
    load_v[2].wait()
    load_v[3].wait()
    v_out(range(AHEAD[0]))
    own_copy(1)

    def piece(slot, dx, cols=None):
        source = pl.ds(pl.multiple_of(at(slot * R, dx)[1] * share, share), share)
        return r_all.at[:, source, :] if cols is None else r_all.at[:, source, cols]

    parts = (pl.ds(0, half), pl.ds(half, half))

    def spread(slot):
        came = r_rsem.at[slot] if slot else own_sem.at[0]
        either(place_q(0), lambda n: arrived(piece(slot, 0, pl.ds(0, n)), came))
        for dx in (1, 3):
            send(piece(slot, 0), piece(slot, 0), x_ssem.at[dx * Q + slot], r_rsem.at[(4 - dx) * Q + slot], at(0, dx))

    def relay(slot):
        for number, dx in enumerate((1, 3)):
            arrived(piece(slot, dx), r_rsem.at[dx * Q + slot])
            part = piece(slot, dx, parts[number])
            send(part, part, x_ssem.at[2 * number * Q + slot], r_rsem.at[(2 + 2 * number) * Q + slot], at(0, 4 - dx))

    lag = 1
    for slot in range(Q + lag):
        if slot < Q:
            spread(slot)
        if slot >= lag:
            relay(slot - lag)

    load_f.wait()
    f_high[...], f_low[...] = halves(factor[...])
    for slot in range(Q):
        for number in range(2):
            arrived(piece(slot, 2, parts[number]), r_rsem.at[(2 + 2 * number) * Q + slot])

    def summed(a, b, m):
        def one(j, total):
            cols = pl.ds(pl.multiple_of(j * step, 128), step)
            return total + lax.dot_general(a(cols), b(cols), NT, preferred_element_type=F32)
        return lax.fori_loop(0, chunk // step, one, jnp.zeros((m, panel), F32))

    part = panel // GROUP
    gram = summed(lambda cols: r_all[0, :, cols], lambda cols: r_all[1, :, cols], panel)
    g_send[...] = gram.reshape(GROUP, part, panel).astype(BF16)

    def owner(d):
        across, far = at(d)
        return lax.rem(far, Q) * R + across

    for d in OTHERS:
        send(g_send.at[owner(d)], g_recv.at[mirror(d)], gs_ssem.at[d], gs_rsem.at[mirror(d)], at(d))
    v_out(range(AHEAD[0], AHEAD[1]))

    sides = (h, 1 - h)

    def place(slot, flip, core):
        return sides[flip] * 2 + core, at(slot * R)[1]

    def turned(slot):
        return mirror(slot * R) // R

    def tall(ref):
        value = ref[...]
        return value.reshape(2 * Q * per, value.shape[-1])

    step_y = lax.rem(h + k, 2)

    def p_out(core):
        send(p_send.at[core, :, 1 - k], p_swap.at[core], pw_ssem.at[core], pw_rsem.at[core], place(0, 0, 1 - k))
        arrived(p_swap.at[core], pw_rsem.at[core])
        p_send[core, :, k] = (p_send[core, :, k].astype(F32) + p_swap[core].astype(F32)).astype(BF16)

        def p_to(slot):
            spot = turned(slot) * 2 + step_y
            send(p_send.at[core, slot, k], p_recv.at[spot], ps_ssem.at[slot * 2 + core], ps_rsem.at[spot],
                 (k * 2 + core, at(slot * R)[1]))

        for slot in DISTANT:
            p_to(slot)
        here = jnp.logical_and(h == core, k == core)

        @pl.when(jnp.logical_not(here))
        def _():
            p_to(0)

        @pl.when(here)
        def _():
            p_recv[0] = p_send[core, 0, core]

    for slot in range(1, Q):
        v_arrived(slot, None)
    own_copied(0)
    for p in range(2):
        total = summed(lambda cols: tall(v_all.at[0, :, :, :, cols]), lambda cols: r_all[p, :, cols], 2 * Q * per)
        p_send[0, :, :, :, p * panel:(p + 1) * panel] = total.astype(BF16).reshape(Q, 2, per, panel)
    p_out(0)
    v_out(range(AHEAD[1], AHEAD[2]))

    for d in OTHERS:
        arrived(g_recv.at[d], gs_rsem.at[d])
    g_own[...] = (jnp.sum(g_recv[1:].astype(F32), axis=0) + g_send[owner(0)].astype(F32)).astype(BF16)
    for d in OTHERS:
        send(g_own, g_all.at[owner(0)], ga_ssem.at[d], ga_rsem.at[mirror(d)], at(d))
    g_all[owner(0)] = g_own[...]
    v_out(range(AHEAD[2], AHEAD[3]))

    def second_half(numbers):
        for number in numbers:
            for slot in range(1, Q):
                v_arrived(slot, number)
            cols = pl.ds(number * part_width, part_width)
            for p in range(2):
                here = slice(p * panel, (p + 1) * panel)
                total = lax.dot_general(
                    tall(v_all.at[1, :, :, :, cols]), r_all[p, :, cols], NT, preferred_element_type=F32)
                if number:
                    total = total + p_sum[:, here]
                if number < PIECES - 1:
                    p_sum[:, here] = total
                else:
                    p_send[1, :, :, :, here] = total.astype(BF16).reshape(Q, 2, per, panel)

    own_copied(1)
    second_half(range(AHEAD[1]))

    def s_place(core, slot, flip):
        return s_all.at[core, slot, sides[flip]]

    def s_out(core):
        @pl.when(k == core)
        def _():
            for spot in range(1, 2 * Q):
                arrived(p_recv.at[spot], ps_rsem.at[spot])

            @pl.when(h != core)
            def _():
                arrived(p_recv.at[0], ps_rsem.at[0])
            product = jnp.sum(p_recv[...].astype(F32), axis=0)
            first = times(product[:, :panel], f_high[0], f_low[0]).astype(BF16)
            second = times(product[:, panel:], f_high[1], f_low[1])
            for d in OTHERS:
                arrived(g_all.at[owner(d)], ga_rsem.at[d])
            gram = g_all[...].reshape(panel, panel)
            second = second - times(jnp.dot(first, gram, preferred_element_type=F32), f_high[1], f_low[1])
            s_own[:, :panel] = first
            s_own[:, panel:] = second.astype(BF16)
            for slot, flip in FAR:
                spot = (turned(slot) * 2 + flip) * 2 + core
                send(s_own, s_all.at[core, turned(slot), h], sa_ssem.at[(slot * 2 + flip) * 2], sa_rsem.at[spot],
                     place(slot, flip, core))
            send(s_own, s_place(core, 0, 0), sa_ssem.at[1], sa_rsem.at[core], place(0, 0, 1 - core))
            s_all[core, 0, h] = s_own[...]

    def s_shared(core):
        @pl.when(k == core)
        def _():
            for slot, flip in FAR:
                spot = (slot * 2 + flip) * 2 + core
                arrived(s_place(core, slot, flip), sa_rsem.at[spot])
                send(s_place(core, slot, flip), s_place(core, slot, flip), sa_ssem.at[(slot * 2 + flip) * 2 + 1],
                     sa_rsem.at[spot], place(0, 0, 1 - core))

        @pl.when(k != core)
        def _():
            for slot, flip in FAR + [(0, 0)]:
                arrived(s_place(core, slot, flip), sa_rsem.at[(slot * 2 + flip) * 2 + core])

    base = first_of(place_q(0))
    width = chunk // 6

    def results(core, first, stop):
        def update(j):
            here = pl.ds(pl.multiple_of(j * width, 128), width)
            change = jnp.dot(tall(s_all.at[core, :, :, :, pl.ds(0, panel)]), r_all[0, :, here], preferred_element_type=F32)
            change = change + jnp.dot(
                tall(s_all.at[core, :, :, :, pl.ds(panel, panel)]), r_all[1, :, here], preferred_element_type=F32)
            fresh = (tall(v_all.at[core, :, :, :, here]).astype(F32) - change).astype(BF16)
            v_all[core, :, :, :, here] = fresh.reshape(Q, 2, per, width)

        def leave(j, count):
            there = pl.ds(pl.multiple_of(base + j * width, 128), count)
            here = pl.ds(pl.multiple_of(j * width, 128), count)
            for slot, flip in FAR:
                send(v_all.at[core, slot, sides[flip], :, here], out.at[prow, :, there],
                     o_ssem.at[(slot * 2 + flip) * 2 + core], o_rsem.at[(turned(slot) * 2 + flip) * 2 + k],
                     place(slot, flip, core))

            @pl.when(k == core)
            def _():
                pltpu.make_async_copy(v_all.at[core, 0, h, :, here], out.at[prow, :, there], o_own.at[0]).start()

            @pl.when(k != core)
            def _():
                send(v_all.at[core, 0, h, :, here], out.at[prow, :, there], o_ssem.at[core], o_rsem.at[k],
                     place(0, 0, core))

        last = chunk // width - 1

        @pl.loop(first, min(stop, last))
        def _(j):
            update(j)
            leave(j, width)
        if stop > last:
            update(last)
            either(place_q(0), lambda n: leave(last, n), width)

    s_out(0)
    second_half(range(AHEAD[1], PIECES))
    p_out(1)
    s_shared(0)
    results(0, 0, 2)
    s_out(1)
    results(0, 2, 6)
    s_shared(1)
    results(1, 0, 6)

    for slot in range(Q):
        if slot:
            q = place_q(turned(slot))
            either(q, lambda n: arrived(piece(slot, 0, pl.ds(0, n)), r_ssem.at[slot]))
            for number in (None, *range(PIECES)):
                sem = v_ssem.at[v_sem(slot, number)]
                v_each(q, number, lambda n: arrived(v_landing(slot, number, n), sem))
        for dx in (1, 3):
            arrived(piece(slot, 0), x_ssem.at[dx * Q + slot])
        for number in range(2):
            arrived(piece(slot, 0, parts[number]), x_ssem.at[2 * number * Q + slot])
    def out_rows(n):
        return out.at[0, :, pl.ds(0, n)]

    either(place_q(0), lambda n: arrived(out_rows(n), o_own.at[0]))
    for d in OTHERS:
        arrived(g_own, gs_ssem.at[d])
        arrived(g_own, ga_ssem.at[d])
        arrived(s_own, sa_ssem.at[d])

    def ended(spot):
        either(place_q(0), lambda n: arrived(out_rows(n), o_ssem.at[spot]))

    def landed(slot, flip, core):
        q = place_q(slot)

        def wait(n):
            there = pl.ds(pl.multiple_of(first_of(q), 128), n)
            arrived(out.at[place(slot, flip, core)[0], :, there], o_rsem.at[(slot * 2 + flip) * 2 + core])
        either(q, wait)

    for core in range(2):
        arrived(p_swap.at[core], pw_ssem.at[core])
        for slot in DISTANT:
            arrived(s_own, ps_ssem.at[slot * 2 + core])

        @pl.when(jnp.logical_not(jnp.logical_and(h == core, k == core)))
        def _():
            arrived(s_own, ps_ssem.at[core])

    ended(1 - k)
    landed(0, 0, 1 - k)
    for slot, flip in FAR:
        for core in range(2):
            ended((slot * 2 + flip) * 2 + core)
            landed(slot, flip, core)


def joined(width, held, out, line, out_sem):
    stores = []
    rows = held.shape[1]
    for r in sorted(range(R), key=lambda r: r * width % 128):
        first, shift = r * width // 128 * 128, r * width % 128
        end = (r + 1) * width // 128 * 128
        if shift == 0:
            source = held.at[r, :, pl.ds(0, end - first)]
        else:
            count = (end - first) // 128
            lane = lax.broadcasted_iota(jnp.int32, (rows, 128), 1)
            keep = held[r - 1, :, pl.ds(first - (r - 1) * width // 128 * 128, 128)].astype(F32)
            turned = pltpu.roll(held[r, :, :128].astype(F32), shift, 1)
            line[r // 2, :, :128] = jnp.where(lane < shift, keep, turned).astype(BF16)
            width_step = 13 * 128
            for a in range(128, count * 128, width_step):
                n = min(width_step, count * 128 - a)
                wide = held[r, :, a - 128:a + n].astype(F32)
                line[r // 2, :, a:a + n] = pltpu.roll(wide, shift, 1)[:, 128:].astype(BF16)
            source = line.at[r // 2]
        store = pltpu.make_async_copy(source, out.at[:, pl.ds(first, end - first)], out_sem.at[r])
        store.start()
        stores.append(store)
    for store in stores:
        store.wait()


def body(vectors, reflectors, panel_factor):
    rows, width = vectors.shape
    panel = panel_factor.shape[1]
    share = reflectors.shape[1]
    tiles = pl.cdiv(width, 128)
    chunk = pl.cdiv(tiles, Q) * 128
    whole = (tiles - 1) * 128
    slim = tiles // Q * 128
    extras = tuple(number * Q // (tiles % Q) for number in range(tiles % Q))
    dims = (rows, panel, whole, width - whole, chunk, slim, extras, chunk // 3)
    per = rows // R
    any_spec = pl.BlockSpec(memory_space=pl.ANY)
    dma = pltpu.SemaphoreType.DMA
    part = panel // GROUP
    gathered = pl.pallas_call(
        functools.partial(kernel, dims),
        out_shape=pltpu.VMEM((R, per, tiles * 128), BF16),
        in_specs=[
            any_spec, any_spec,
            any_spec,
        ],
        out_specs=pl.BlockSpec(memory_space=pltpu.VMEM),
        scratch_shapes=[
            pltpu.VMEM((2, 2, per, tiles * 128), BF16),
            pltpu.VMEM((2, share, tiles * 128), BF16),
            pltpu.VMEM((2, Q, 2, per, chunk), BF16),
            pltpu.VMEM((2, panel, chunk), BF16),
            pltpu.VMEM((rows * Q // 2, 2 * panel), F32),
            pltpu.VMEM((2, Q, 2, per, 2 * panel), BF16),
            pltpu.VMEM((2, Q, per, 2 * panel), BF16),
            pltpu.VMEM((2 * Q, per, 2 * panel), BF16),
            pltpu.VMEM((GROUP, part, panel), BF16),
            pltpu.VMEM((GROUP, part, panel), BF16),
            pltpu.VMEM((part, panel), BF16),
            pltpu.VMEM((GROUP, part, panel), BF16),
            pltpu.VMEM((per, 2 * panel), BF16),
            pltpu.VMEM((2, Q, 2, per, 2 * panel), BF16),
            pltpu.VMEM((rows, width - whole), BF16),
            pltpu.VMEM((2, share, width - whole), BF16),
            pltpu.VMEM((2, panel, panel), F32),
            pltpu.VMEM((2, panel, panel), BF16),
            pltpu.VMEM((2, panel, panel), BF16),
            dma((4 + R,)), dma((3,)), dma((Q,)), dma(((X + 1) * Q,)), dma((X * Q,)), dma((Q + Q * PIECES,)), dma((Q + Q * PIECES,)),
            dma((2,)), dma((2,)),
            dma((GROUP,)), dma((GROUP,)), dma((GROUP,)), dma((GROUP,)), dma((2 * Q,)), dma((2 * Q,)),
            dma((GROUP,)), dma((GROUP,)), dma((GROUP,)), dma((GROUP,)), dma((1,)),
        ],
        compiler_params=pltpu.CompilerParams(
            collective_id=0, has_side_effects=True, vmem_limit_bytes=62700000
        ),
        name="back_transform",
    )(vectors, reflectors, panel_factor)
    line = R * width // 128 * 128 - (R - 1) * width // 128 * 128
    rows_out = pl.pallas_call(
        functools.partial(joined, width),
        out_shape=jax.ShapeDtypeStruct((per, R * width), BF16),
        in_specs=[pl.BlockSpec(memory_space=pltpu.VMEM)],
        out_specs=any_spec,
        scratch_shapes=[pltpu.VMEM((2, per, line), BF16), dma((R,))],
        compiler_params=pltpu.CompilerParams(vmem_limit_bytes=16 * 1024 * 1024),
        name="joined",
    )(gathered)
    return rows_out[None]


def solution(mesh):
    placed = (P("pcol", "prow"), P(None, "pcol", "prow"), P())
    return jax.shard_map(
        body, mesh=mesh, in_specs=placed, out_specs=P("pcol", "prow", None), check_vma=False
    )
```

```python
import functools

import jax
import jax.numpy as jnp
from jax import lax
from jax.experimental import pallas as pl
from jax.experimental.pallas import tpu as pltpu
from jax.sharding import PartitionSpec as P

X, YL, Z, R = 4, 2, 4, 4
Q = YL * Z
GROUP = Q * R
ORDER = ((0, 0), (1, 0), (1, 1), (1, 3), (0, 2), (1, 2), (0, 1), (0, 3))
SLOT = {pair: number for number, pair in enumerate(ORDER)}
PAIRS = [(slot, flip) for slot in range(Q) for flip in range(2)]
PIECES, AHEAD = 5, (2, 3, 4, 5)
GOING = ((0, 1), (0, 3), (1, 1), (1, 3), (1, 0), (0, 2), (1, 2))


def hops(d):
    dy, dz = ORDER[d // R]
    return min(dz, Z - dz) + (1 if dy else d % R // 2 * 2)


OTHERS = sorted(range(1, GROUP), key=lambda d: -hops(d))

FAR = sorted(PAIRS[1:], key=lambda pair: -hops(pair[0] * R + pair[1] * 2))
DISTANT = sorted(range(1, Q), key=lambda slot: -hops(slot * R))
BF16, F32 = jnp.bfloat16, jnp.float32
NT = (((1,), (1,)), ((), ()))


def mirror(d):
    dy, dz = ORDER[d // R]
    return SLOT[dy, (4 - dz) % 4] * R + d % R


def halves(value):
    high = value.astype(BF16)
    return high, (value - high.astype(F32)).astype(BF16)


def times(value, high, low):
    a, b = halves(value)
    total = lax.dot_general(a, high, NT, preferred_element_type=F32)
    total = total + lax.dot_general(b, high, NT, preferred_element_type=F32)
    return total + lax.dot_general(a, low, NT, preferred_element_type=F32)


def kernel(
    dims,
    v_hbm, r_hbm, f_hbm,
    out,
    v_loc, r_loc, v_all, r_all, p_sum, p_send, p_swap, p_recv, g_send, g_recv, g_own, g_all, s_own, s_all, v_tail, r_tail, factor, f_high, f_low,
    ld_sem, own_sem, r_ssem, r_rsem, x_ssem, v_ssem, v_rsem,
    pw_ssem, pw_rsem, gs_ssem, gs_rsem, ga_ssem, ga_rsem, ps_ssem, ps_rsem, sa_ssem, sa_rsem, o_ssem, o_rsem, o_own,
):
    rows, panel, whole, valid, chunk, slim, extras, step = dims
    per = rows // R
    share = panel // (X * Q)
    half = chunk // 2
    prow, pcol = lax.axis_index("prow"), lax.axis_index("pcol")
    x, yl, z = pcol // Q, lax.rem(pcol // Z, YL), lax.rem(pcol, Z)
    h, k = prow // 2, lax.rem(prow, 2)

    yls = [yl, 1 - yl]
    zs = [z] + [lax.rem(z + dz, Z) for dz in range(1, Z)]
    xs = [x] + [lax.rem(x + dx, X) for dx in range(1, X)]
    prows = [prow, h * 2 + 1 - k, (1 - h) * 2 + k, (1 - h) * 2 + 1 - k]

    def at(d, dx=0):
        dy, dz = ORDER[d // R]
        return prows[d % R], xs[dx] * Q + yls[dy] * Z + zs[dz]

    def send(src, dst, ssem, rsem, to):
        copy = pltpu.make_async_remote_copy(
            src_ref=src, dst_ref=dst, send_sem=ssem, recv_sem=rsem,
            device_id=to, device_id_type=pl.DeviceIdType.MESH,
        )
        copy.start()
        return copy

    def arrived(ref, sem):
        pltpu.make_async_copy(ref, ref, sem).wait()

    def first_of(q):
        return (q * (slim // 128) + sum((q + (Q - 1 - e)) // Q for e in extras)) * 128

    def wide(q):
        return sum((q + (Q - e)) // Q - (q + (Q - 1 - e)) // Q for e in extras) == 1

    def place_q(slot):
        return yls[ORDER[slot][0]] * Z + zs[ORDER[slot][1]]

    def either(q, action, most=chunk):
        @pl.when(wide(q))
        def _():
            action(most)

        @pl.when(jnp.logical_not(wide(q)))
        def _():
            action(most - 128)

    @pl.when(jnp.logical_not(wide(place_q(0))))
    def _():
        v_all[:, :, :, :, slim:] = jnp.zeros((2, Q, 2, per, chunk - slim), BF16)
        r_all[:, :, slim:] = jnp.zeros((2, panel, chunk - slim), BF16)

    barrier = pltpu.get_barrier_semaphore()
    for d in OTHERS:
        pl.semaphore_signal(barrier, inc=1, device_id=at(d), device_id_type=pl.DeviceIdType.MESH)
    for dx in (1, 3):
        pl.semaphore_signal(barrier, inc=1, device_id=at(0, dx), device_id_type=pl.DeviceIdType.MESH)

    load_r = pltpu.make_async_copy(r_hbm.at[:, :, pl.ds(0, whole)], r_loc.at[:, :, pl.ds(0, whole)], ld_sem.at[0])
    load_v = [
        pltpu.make_async_copy(
            v_hbm.at[pl.ds(r * per, per), pl.ds(0, whole)], v_loc.at[r // 2, r % 2, :, pl.ds(0, whole)], ld_sem.at[1 + r])
        for r in (0, 2, 1, 3)
    ]
    load_r.start()
    for load in load_v:
        load.start()
    load_f = pltpu.make_async_copy(f_hbm, factor, ld_sem.at[1 + R])
    load_f.start()
    tails = [
        pltpu.make_async_copy(v_hbm.at[:, pl.ds(whole, valid)], v_tail, ld_sem.at[2 + R]),
        pltpu.make_async_copy(r_hbm.at[:, :, pl.ds(whole, valid)], r_tail, ld_sem.at[3 + R]),
    ]
    for load in tails:
        load.start()

    edge = v_loc.shape[3] - whole
    for load in tails:
        load.wait()
    for r in range(R):
        v_loc[r // 2, r % 2, :, whole:] = jnp.zeros((per, edge), BF16)
        v_loc[r // 2, r % 2, :, whole:whole + valid] = v_tail[r * per:(r + 1) * per, :]
    for p in range(2):
        r_loc[p, :, whole:] = jnp.zeros((share, edge), BF16)
        r_loc[p, :, whole:whole + valid] = r_tail[p]

    pl.semaphore_wait(barrier, GROUP - 1 + 2)

    mine = pl.ds(pl.multiple_of(pcol * share, share), share)

    def columns(slot, count, skip=0):
        return pl.ds(pl.multiple_of(first_of(place_q(slot)) + skip, 128), count)

    load_r.wait()
    def r_mine(count):
        return r_all.at[:, mine, pl.ds(0, count)]

    either(place_q(0), lambda n: pltpu.make_async_copy(r_loc.at[:, :, columns(0, n)], r_mine(n), own_sem.at[0]).start())
    for slot in range(1, Q):
        d = mirror(slot * R)
        either(place_q(d // R), lambda n: send(
            r_loc.at[:, :, columns(d // R, n)], r_mine(n), r_ssem.at[slot], r_rsem.at[slot], at(d)))
    part_width = chunk // PIECES

    def v_sem(slot, number):
        return slot if number is None else Q + slot * PIECES + number

    def v_landing(slot, number, count):
        return v_all.at[0 if number is None else 1, slot, :, :, pl.ds((number or 0) * part_width, count)]

    def v_source(slot, number, count):
        return v_loc.at[:, 0 if number is None else 1, :, columns(slot, count, (number or 0) * part_width)]

    def v_each(q, number, action):
        if number is None:
            either(q, action)
        elif number == PIECES - 1:
            either(q, action, part_width)
        else:
            action(part_width)

    def v_out(numbers):
        for number in numbers:
            for pair in GOING:
                d = SLOT[pair] * R
                slot = mirror(d) // R
                sem = v_sem(slot, number)
                v_each(place_q(d // R), number, lambda n: send(
                    v_source(d // R, number, n), v_landing(slot, number, n), v_ssem.at[sem], v_rsem.at[sem], at(d)))

    def v_arrived(slot, number):
        sem = v_rsem.at[v_sem(slot, number)]
        v_each(place_q(0), number, lambda n: arrived(v_landing(slot, number, n), sem))

    def own_copy(core):
        def start(n):
            pltpu.make_async_copy(
                v_loc.at[:, core, :, columns(0, n)], v_all.at[core, 0, :, :, pl.ds(0, n)], own_sem.at[1 + core]).start()
        either(place_q(0), start)

    def own_copied(core):
        either(place_q(0), lambda n: arrived(v_all.at[core, 0, :, :, pl.ds(0, n)], own_sem.at[1 + core]))

    load_v[0].wait()
    load_v[1].wait()
    v_out([None])
    own_copy(0)
    load_v[2].wait()
    load_v[3].wait()
    v_out(range(AHEAD[0]))
    own_copy(1)

    def piece(slot, dx, cols=None):
        source = pl.ds(pl.multiple_of(at(slot * R, dx)[1] * share, share), share)
        return r_all.at[:, source, :] if cols is None else r_all.at[:, source, cols]

    parts = (pl.ds(0, half), pl.ds(half, half))

    def spread(slot):
        came = r_rsem.at[slot] if slot else own_sem.at[0]
        either(place_q(0), lambda n: arrived(piece(slot, 0, pl.ds(0, n)), came))
        for dx in (1, 3):
            send(piece(slot, 0), piece(slot, 0), x_ssem.at[dx * Q + slot], r_rsem.at[(4 - dx) * Q + slot], at(0, dx))

    def relay(slot):
        for number, dx in enumerate((1, 3)):
            arrived(piece(slot, dx), r_rsem.at[dx * Q + slot])
            part = piece(slot, dx, parts[number])
            send(part, part, x_ssem.at[2 * number * Q + slot], r_rsem.at[(2 + 2 * number) * Q + slot], at(0, 4 - dx))

    lag = 1
    for slot in range(Q + lag):
        if slot < Q:
            spread(slot)
        if slot >= lag:
            relay(slot - lag)

    load_f.wait()
    f_high[...], f_low[...] = halves(factor[...])
    for slot in range(Q):
        for number in range(2):
            arrived(piece(slot, 2, parts[number]), r_rsem.at[(2 + 2 * number) * Q + slot])

    def summed(a, b, m):
        def one(j, total):
            cols = pl.ds(pl.multiple_of(j * step, 128), step)
            return total + lax.dot_general(a(cols), b(cols), NT, preferred_element_type=F32)
        return lax.fori_loop(0, chunk // step, one, jnp.zeros((m, panel), F32))

    part = panel // GROUP
    gram = summed(lambda cols: r_all[0, :, cols], lambda cols: r_all[1, :, cols], panel)
    g_send[...] = gram.reshape(GROUP, part, panel).astype(BF16)

    def owner(d):
        across, far = at(d)
        return lax.rem(far, Q) * R + across

    for d in OTHERS:
        send(g_send.at[owner(d)], g_recv.at[mirror(d)], gs_ssem.at[d], gs_rsem.at[mirror(d)], at(d))
    v_out(range(AHEAD[0], AHEAD[1]))

    sides = (h, 1 - h)

    def place(slot, flip, core):
        return sides[flip] * 2 + core, at(slot * R)[1]

    def turned(slot):
        return mirror(slot * R) // R

    def tall(ref):
        value = ref[...]
        return value.reshape(2 * Q * per, value.shape[-1])

    step_y = lax.rem(h + k, 2)

    def p_out(core):
        send(p_send.at[core, :, 1 - k], p_swap.at[core], pw_ssem.at[core], pw_rsem.at[core], place(0, 0, 1 - k))
        arrived(p_swap.at[core], pw_rsem.at[core])
        p_send[core, :, k] = (p_send[core, :, k].astype(F32) + p_swap[core].astype(F32)).astype(BF16)

        def p_to(slot):
            spot = turned(slot) * 2 + step_y
            send(p_send.at[core, slot, k], p_recv.at[spot], ps_ssem.at[slot * 2 + core], ps_rsem.at[spot],
                 (k * 2 + core, at(slot * R)[1]))

        for slot in DISTANT:
            p_to(slot)
        here = jnp.logical_and(h == core, k == core)

        @pl.when(jnp.logical_not(here))
        def _():
            p_to(0)

        @pl.when(here)
        def _():
            p_recv[0] = p_send[core, 0, core]

    for slot in range(1, Q):
        v_arrived(slot, None)
    own_copied(0)
    for p in range(2):
        total = summed(lambda cols: tall(v_all.at[0, :, :, :, cols]), lambda cols: r_all[p, :, cols], 2 * Q * per)
        p_send[0, :, :, :, p * panel:(p + 1) * panel] = total.astype(BF16).reshape(Q, 2, per, panel)
    p_out(0)
    v_out(range(AHEAD[1], AHEAD[2]))

    for d in OTHERS:
        arrived(g_recv.at[d], gs_rsem.at[d])
    g_own[...] = (jnp.sum(g_recv[1:].astype(F32), axis=0) + g_send[owner(0)].astype(F32)).astype(BF16)
    for d in OTHERS:
        send(g_own, g_all.at[owner(0)], ga_ssem.at[d], ga_rsem.at[mirror(d)], at(d))
    g_all[owner(0)] = g_own[...]
    v_out(range(AHEAD[2], AHEAD[3]))

    def second_half(numbers):
        for number in numbers:
            for slot in range(1, Q):
                v_arrived(slot, number)
            cols = pl.ds(number * part_width, part_width)
            for p in range(2):
                here = slice(p * panel, (p + 1) * panel)
                total = lax.dot_general(
                    tall(v_all.at[1, :, :, :, cols]), r_all[p, :, cols], NT, preferred_element_type=F32)
                if number:
                    total = total + p_sum[:, here]
                if number < PIECES - 1:
                    p_sum[:, here] = total
                else:
                    p_send[1, :, :, :, here] = total.astype(BF16).reshape(Q, 2, per, panel)

    own_copied(1)
    second_half(range(AHEAD[1]))

    def s_place(core, slot, flip):
        return s_all.at[core, slot, sides[flip]]

    def s_out(core):
        @pl.when(k == core)
        def _():
            for spot in range(1, 2 * Q):
                arrived(p_recv.at[spot], ps_rsem.at[spot])

            @pl.when(h != core)
            def _():
                arrived(p_recv.at[0], ps_rsem.at[0])
            product = jnp.sum(p_recv[...].astype(F32), axis=0)
            first = times(product[:, :panel], f_high[0], f_low[0]).astype(BF16)
            second = times(product[:, panel:], f_high[1], f_low[1])
            for d in OTHERS:
                arrived(g_all.at[owner(d)], ga_rsem.at[d])
            gram = g_all[...].reshape(panel, panel)
            second = second - times(jnp.dot(first, gram, preferred_element_type=F32), f_high[1], f_low[1])
            s_own[:, :panel] = first
            s_own[:, panel:] = second.astype(BF16)
            for slot, flip in FAR:
                spot = (turned(slot) * 2 + flip) * 2 + core
                send(s_own, s_all.at[core, turned(slot), h], sa_ssem.at[(slot * 2 + flip) * 2], sa_rsem.at[spot],
                     place(slot, flip, core))
            send(s_own, s_place(core, 0, 0), sa_ssem.at[1], sa_rsem.at[core], place(0, 0, 1 - core))
            s_all[core, 0, h] = s_own[...]

    def s_shared(core):
        @pl.when(k == core)
        def _():
            for slot, flip in FAR:
                spot = (slot * 2 + flip) * 2 + core
                arrived(s_place(core, slot, flip), sa_rsem.at[spot])
                send(s_place(core, slot, flip), s_place(core, slot, flip), sa_ssem.at[(slot * 2 + flip) * 2 + 1],
                     sa_rsem.at[spot], place(0, 0, 1 - core))

        @pl.when(k != core)
        def _():
            for slot, flip in FAR + [(0, 0)]:
                arrived(s_place(core, slot, flip), sa_rsem.at[(slot * 2 + flip) * 2 + core])

    base = first_of(place_q(0))
    width = chunk // 6

    def results(core, first, stop):
        def update(j):
            here = pl.ds(pl.multiple_of(j * width, 128), width)
            change = jnp.dot(tall(s_all.at[core, :, :, :, pl.ds(0, panel)]), r_all[0, :, here], preferred_element_type=F32)
            change = change + jnp.dot(
                tall(s_all.at[core, :, :, :, pl.ds(panel, panel)]), r_all[1, :, here], preferred_element_type=F32)
            fresh = (tall(v_all.at[core, :, :, :, here]).astype(F32) - change).astype(BF16)
            v_all[core, :, :, :, here] = fresh.reshape(Q, 2, per, width)

        def leave(j, count):
            there = pl.ds(pl.multiple_of(base + j * width, 128), count)
            here = pl.ds(pl.multiple_of(j * width, 128), count)
            for slot, flip in FAR:
                send(v_all.at[core, slot, sides[flip], :, here], out.at[prow, :, there],
                     o_ssem.at[(slot * 2 + flip) * 2 + core], o_rsem.at[(turned(slot) * 2 + flip) * 2 + k],
                     place(slot, flip, core))

            @pl.when(k == core)
            def _():
                pltpu.make_async_copy(v_all.at[core, 0, h, :, here], out.at[prow, :, there], o_own.at[0]).start()

            @pl.when(k != core)
            def _():
                send(v_all.at[core, 0, h, :, here], out.at[prow, :, there], o_ssem.at[core], o_rsem.at[k],
                     place(0, 0, core))

        last = chunk // width - 1

        @pl.loop(first, min(stop, last))
        def _(j):
            update(j)
            leave(j, width)
        if stop > last:
            update(last)
            either(place_q(0), lambda n: leave(last, n), width)

    s_out(0)
    second_half(range(AHEAD[1], PIECES))
    p_out(1)
    s_shared(0)
    results(0, 0, 1)
    s_out(1)
    results(0, 1, 6)
    s_shared(1)
    results(1, 0, 6)

    for slot in range(Q):
        if slot:
            q = place_q(turned(slot))
            either(q, lambda n: arrived(piece(slot, 0, pl.ds(0, n)), r_ssem.at[slot]))
            for number in (None, *range(PIECES)):
                sem = v_ssem.at[v_sem(slot, number)]
                v_each(q, number, lambda n: arrived(v_landing(slot, number, n), sem))
        for dx in (1, 3):
            arrived(piece(slot, 0), x_ssem.at[dx * Q + slot])
        for number in range(2):
            arrived(piece(slot, 0, parts[number]), x_ssem.at[2 * number * Q + slot])
    def out_rows(n):
        return out.at[0, :, pl.ds(0, n)]

    either(place_q(0), lambda n: arrived(out_rows(n), o_own.at[0]))
    for d in OTHERS:
        arrived(g_own, gs_ssem.at[d])
        arrived(g_own, ga_ssem.at[d])
        arrived(s_own, sa_ssem.at[d])

    def ended(spot):
        either(place_q(0), lambda n: arrived(out_rows(n), o_ssem.at[spot]))

    def landed(slot, flip, core):
        q = place_q(slot)

        def wait(n):
            there = pl.ds(pl.multiple_of(first_of(q), 128), n)
            arrived(out.at[place(slot, flip, core)[0], :, there], o_rsem.at[(slot * 2 + flip) * 2 + core])
        either(q, wait)

    for core in range(2):
        arrived(p_swap.at[core], pw_ssem.at[core])
        for slot in DISTANT:
            arrived(s_own, ps_ssem.at[slot * 2 + core])

        @pl.when(jnp.logical_not(jnp.logical_and(h == core, k == core)))
        def _():
            arrived(s_own, ps_ssem.at[core])

    ended(1 - k)
    landed(0, 0, 1 - k)
    for slot, flip in FAR:
        for core in range(2):
            ended((slot * 2 + flip) * 2 + core)
            landed(slot, flip, core)


def joined(width, held, out, line, out_sem):
    stores = []
    rows = held.shape[1]
    for r in sorted(range(R), key=lambda r: r * width % 128):
        first, shift = r * width // 128 * 128, r * width % 128
        end = (r + 1) * width // 128 * 128
        if shift == 0:
            source = held.at[r, :, pl.ds(0, end - first)]
        else:
            count = (end - first) // 128
            lane = lax.broadcasted_iota(jnp.int32, (rows, 128), 1)
            keep = held[r - 1, :, pl.ds(first - (r - 1) * width // 128 * 128, 128)].astype(F32)
            turned = pltpu.roll(held[r, :, :128].astype(F32), shift, 1)
            line[r // 2, :, :128] = jnp.where(lane < shift, keep, turned).astype(BF16)
            width_step = 13 * 128
            for a in range(128, count * 128, width_step):
                n = min(width_step, count * 128 - a)
                wide = held[r, :, a - 128:a + n].astype(F32)
                line[r // 2, :, a:a + n] = pltpu.roll(wide, shift, 1)[:, 128:].astype(BF16)
            source = line.at[r // 2]
        store = pltpu.make_async_copy(source, out.at[:, pl.ds(first, end - first)], out_sem.at[r])
        store.start()
        stores.append(store)
    for store in stores:
        store.wait()


def body(vectors, reflectors, panel_factor):
    rows, width = vectors.shape
    panel = panel_factor.shape[1]
    share = reflectors.shape[1]
    tiles = pl.cdiv(width, 128)
    chunk = pl.cdiv(tiles, Q) * 128
    whole = (tiles - 1) * 128
    slim = tiles // Q * 128
    extras = tuple(number * Q // (tiles % Q) for number in range(tiles % Q))
    dims = (rows, panel, whole, width - whole, chunk, slim, extras, chunk // 3)
    per = rows // R
    any_spec = pl.BlockSpec(memory_space=pl.ANY)
    dma = pltpu.SemaphoreType.DMA
    part = panel // GROUP
    gathered = pl.pallas_call(
        functools.partial(kernel, dims),
        out_shape=pltpu.VMEM((R, per, tiles * 128), BF16),
        in_specs=[
            any_spec, any_spec,
            any_spec,
        ],
        out_specs=pl.BlockSpec(memory_space=pltpu.VMEM),
        scratch_shapes=[
            pltpu.VMEM((2, 2, per, tiles * 128), BF16),
            pltpu.VMEM((2, share, tiles * 128), BF16),
            pltpu.VMEM((2, Q, 2, per, chunk), BF16),
            pltpu.VMEM((2, panel, chunk), BF16),
            pltpu.VMEM((rows * Q // 2, 2 * panel), F32),
            pltpu.VMEM((2, Q, 2, per, 2 * panel), BF16),
            pltpu.VMEM((2, Q, per, 2 * panel), BF16),
            pltpu.VMEM((2 * Q, per, 2 * panel), BF16),
            pltpu.VMEM((GROUP, part, panel), BF16),
            pltpu.VMEM((GROUP, part, panel), BF16),
            pltpu.VMEM((part, panel), BF16),
            pltpu.VMEM((GROUP, part, panel), BF16),
            pltpu.VMEM((per, 2 * panel), BF16),
            pltpu.VMEM((2, Q, 2, per, 2 * panel), BF16),
            pltpu.VMEM((rows, width - whole), BF16),
            pltpu.VMEM((2, share, width - whole), BF16),
            pltpu.VMEM((2, panel, panel), F32),
            pltpu.VMEM((2, panel, panel), BF16),
            pltpu.VMEM((2, panel, panel), BF16),
            dma((4 + R,)), dma((3,)), dma((Q,)), dma(((X + 1) * Q,)), dma((X * Q,)), dma((Q + Q * PIECES,)), dma((Q + Q * PIECES,)),
            dma((2,)), dma((2,)),
            dma((GROUP,)), dma((GROUP,)), dma((GROUP,)), dma((GROUP,)), dma((2 * Q,)), dma((2 * Q,)),
            dma((GROUP,)), dma((GROUP,)), dma((GROUP,)), dma((GROUP,)), dma((1,)),
        ],
        compiler_params=pltpu.CompilerParams(
            collective_id=0, has_side_effects=True, vmem_limit_bytes=62700000
        ),
        name="back_transform",
    )(vectors, reflectors, panel_factor)
    line = R * width // 128 * 128 - (R - 1) * width // 128 * 128
    rows_out = pl.pallas_call(
        functools.partial(joined, width),
        out_shape=jax.ShapeDtypeStruct((per, R * width), BF16),
        in_specs=[pl.BlockSpec(memory_space=pltpu.VMEM)],
        out_specs=any_spec,
        scratch_shapes=[pltpu.VMEM((2, per, line), BF16), dma((R,))],
        compiler_params=pltpu.CompilerParams(vmem_limit_bytes=16 * 1024 * 1024),
        name="joined",
    )(gathered)
    return rows_out[None]


def solution(mesh):
    placed = (P("pcol", "prow"), P(None, "pcol", "prow"), P())
    return jax.shard_map(
        body, mesh=mesh, in_specs=placed, out_specs=P("pcol", "prow", None), check_vma=False
    )
```
